128 devices in a mesh: sx: 8 (over x, core), sy: 8 (over z, y_hi), dp: 2 (over y_lo).
Axes of the slice: x: 4, y: 4 (y_hi: 2, y_lo: 2; y = y_hi * 2 + y_lo), z: 4, core: 2. Of those that a mesh axis runs over, the one named last changes fastest.
Arguments:
- tokens: bfloat16 [2, 32768, 1280], P('dp', ('sx', 'sy')), may hold values from -6 to 6
- lengths: int32 [2, 256], P('dp'), may hold values from 1 to 512, 32768 in all within a row
- ln_gain: float32 [1280], replicated, may hold values from 0.1 to 1.9
- w_qkv: bfloat16 [1280, 3840], P('dp'), may hold values from -4 to 4, as said below
- w_out: bfloat16 [1280, 1280], P('dp'), may hold values from -0.15625 to 0.15625
Outputs:
- hidden: bfloat16 [2, 32768, 1280], P('dp', ('sx', 'sy'))
- pooled: float32 [2, 256, 1280], P('dp')
The draws below stay inside these ranges and needn't reach their ends.
Inputs may be any that keep to these rules, and one draw needn't show every extreme that they name: The 256 lengths of a row sum to 32768; images are packed end to end in order. `w_qkv`: columns are queries, then keys, then values, each of 16 heads of 80 columns.
All inputs are finite; a program needn't handle non-finite values.
Results may differ from the reference program's by a relative error of at most 0.0051.
Values may be sent and summed in bfloat16 or wider, within the bound.
No kernel may reach another device: no remote copies, remote signals or barrier semaphores. Data moves between devices by JAX's collectives and lax.ppermute only.
A program may use at most 128 MiB of HBM per device.

```python
import math
import jax
import jax.numpy as jnp
import numpy as np
from jax import lax

D = 1280
HEADS = 16
MAXLEN = 512
ROWS = 2
SEQ = 32768
IMAGES = 256


def draw_w_qkv(key, part):
    first = jax.random.fold_in(jax.random.fold_in(key, 11), 0)
    base = jax.random.normal(first, (D, 3 * D), jnp.float32) * D ** (-0.5)
    return jnp.clip(base, -4.0, 4.0).astype(jnp.bfloat16)


def block_levels(rng, dims, pieces, least, largest):
    def one(position, shards_of):
        steps = jax.random.uniform(jax.random.fold_in(jax.random.fold_in(rng, 6), position), (shards_of,), jnp.float32, least / len(pieces), largest / len(pieces))
        return jnp.repeat(jnp.exp(steps), dims[position] // shards_of).reshape((-1,) + (1,) * (len(dims) - position - 1))

    loudness = one(*pieces[0])
    for cut in pieces[1:]:
        loudness = loudness * one(*cut)
    return loudness


def split_up(number_of, total, limit, lean):
    portions = [(1 << 20) // math.isqrt(standing ** lean) + 1 for standing in range(2, number_of + 1)]
    spare, given = total - limit - (number_of - 1), [1] * (number_of - 1)
    while spare > 0:
        candidates = [i for i in range(number_of - 1) if given[i] < limit]
        whole, remaining = sum([portions[i] for i in candidates]), spare
        for i in candidates:
            extra = min(limit - given[i], max(1, remaining * portions[i] // whole), spare)
            given[i] = given[i] + extra
            spare = spare - extra
    return np.array([limit] + given)


def ragged_sizes(stream_key, number_of, total, limit, lean):
    if number_of == 2:
        one = jax.random.randint(stream_key, (), max(1, total - limit), min(limit, total - 1) + 1)
        return jnp.stack([one, total - one])
    sizes = jnp.asarray(split_up(number_of, total, limit, lean), jnp.int32)
    twos = (number_of - 1) // 2
    donor, taker = sizes[1:1 + 2 * twos:2], sizes[2:2 + 2 * twos:2]
    room = jnp.minimum(donor - 1, limit - taker)
    passed = jax.random.randint(jax.random.fold_in(stream_key, 1), (twos,), 0, 1 << 20) % (room + 1)
    sizes = sizes.at[1:1 + 2 * twos:2].set(donor - passed).at[2:2 + 2 * twos:2].set(taker + passed)
    return sizes[jax.random.permutation(jax.random.fold_in(stream_key, 2), number_of)]


def gaussian(stream_key, shape, scale, bound, cuts=(), held_as=jnp.bfloat16):
    result = scale * jax.random.normal(stream_key, shape, jnp.float32)
    if cuts:
        result = result * block_levels(stream_key, shape, cuts, -0.22, 0.18)
    return jnp.clip(result, -bound, bound).astype(held_as)


def setup_inputs(seed: int = 0) -> dict:
    splits = jax.random.split(jax.random.key(seed), 6)
    tokens = gaussian(splits[0], (ROWS, SEQ, D), 1.0, 6.0, ((0, 2), (1, 64)))
    lengths = jax.vmap(lambda own: ragged_sizes(own, IMAGES, SEQ, MAXLEN, 2))(jax.random.split(splits[1], ROWS)).reshape((ROWS, IMAGES)).astype(jnp.int32)
    ln_gain = jnp.clip(1.0 + 0.18 * jax.random.normal(splits[2], (D,), jnp.float32), 0.1, 1.9)
    w_qkv = draw_w_qkv(jax.random.fold_in(splits[5], 71), 0)
    w_out = gaussian(splits[4], (D, D), D ** -0.5, 0.15625, ((0, 2),))
    return {"tokens": tokens, "lengths": lengths, "ln_gain": ln_gain, "w_qkv": w_qkv, "w_out": w_out}


def image_ids(lengths, positions, total):
    offsets = jnp.cumsum(lengths) - lengths
    counted = lax.optimization_barrier(jnp.sum((offsets[None, :] <= positions[:, None]).astype(jnp.int32), axis=1)) - 1
    inside = (positions >= 0) & (positions < total)
    return jnp.where(inside, counted, -1).astype(jnp.int32)

def normalize(rows, ln_gain):
    values = rows.astype(jnp.float32)
    center = values - lax.optimization_barrier(jnp.mean(values, axis=-1, keepdims=True))
    spread = lax.optimization_barrier(jnp.mean(center * center, axis=-1, keepdims=True))
    return (center * lax.rsqrt(spread + 1e-05) * ln_gain).astype(jnp.bfloat16)

def attend(queries, keys, values, q_ids, k_ids, margin):
    length = queries.shape[0]
    heads = queries.shape[1]
    block = min(512, length)
    window = block + 2 * margin
    scale = queries.shape[2] ** (-0.5)

    def one_block(index):
        start = (index * block).astype(jnp.int32)
        q_blk = lax.dynamic_slice_in_dim(queries, start, block, 0)
        k_blk = lax.dynamic_slice_in_dim(keys, start, window, 0)
        v_blk = lax.dynamic_slice_in_dim(values, start, window, 0)
        q_lab = lax.dynamic_slice_in_dim(q_ids, start, block, 0)
        k_lab = lax.dynamic_slice_in_dim(k_ids, start, window, 0)
        allowed = q_lab[:, None] == k_lab[None, :]

        def one_head(head):
            q_head = lax.dynamic_index_in_dim(q_blk, head, 1, keepdims=False)
            k_head = lax.dynamic_index_in_dim(k_blk, head, 1, keepdims=False)
            v_head = lax.dynamic_index_in_dim(v_blk, head, 1, keepdims=False)
            scores = jnp.dot(q_head, k_head.T, preferred_element_type=jnp.float32) * scale
            scores = jnp.where(allowed, scores, -1e+30)
            top = lax.optimization_barrier(jnp.max(scores, axis=1, keepdims=True))
            weights = jnp.exp(scores - top)
            probs = (weights / lax.optimization_barrier(jnp.sum(weights, axis=1, keepdims=True))).astype(jnp.bfloat16)
            return jnp.dot(probs, v_head, preferred_element_type=jnp.float32).astype(jnp.bfloat16)
        outcome = lax.map(one_head, jnp.arange(heads, dtype=jnp.int32))
        return jnp.transpose(outcome, (1, 0, 2))
    blocks = lax.map(one_block, jnp.arange(length // block, dtype=jnp.int32))
    return blocks.reshape(length, heads, -1)

def reference(tokens, lengths, ln_gain, w_qkv, w_out):
    total = tokens.shape[1]
    width = tokens.shape[2]
    size = width // HEADS
    positions = jnp.arange(total, dtype=jnp.int32)
    extended = jnp.arange(total + 2 * MAXLEN, dtype=jnp.int32) - MAXLEN

    def one_row(pair):
        row, lens = pair
        normed = normalize(row, ln_gain)
        qkv = jnp.dot(normed, w_qkv, preferred_element_type=jnp.float32).astype(jnp.bfloat16)
        qkv = qkv.reshape(total, 3, HEADS, size)
        own_ids = image_ids(lens, positions, total)
        far_ids = image_ids(lens, extended, total)
        padding = jnp.zeros((MAXLEN, 3, HEADS, size), jnp.bfloat16)
        padded = jnp.concatenate([padding, qkv, padding], axis=0)
        context = attend(qkv[:, 0], padded[:, 1], padded[:, 2], own_ids, far_ids, MAXLEN)
        mixed = jnp.dot(context.reshape(total, width), w_out, preferred_element_type=jnp.float32)
        hidden = (row.astype(jnp.float32) + mixed).astype(jnp.bfloat16)
        onehot = (jnp.arange(IMAGES, dtype=jnp.int32)[:, None] == own_ids[None, :]).astype(jnp.bfloat16)
        sums = jnp.dot(onehot, hidden, preferred_element_type=jnp.float32)
        pooled = sums / lens.astype(jnp.float32)[:, None]
        return (hidden, pooled)
    hidden, pooled = lax.map(one_row, (tokens, lengths))
    return (hidden, pooled)
```

```python
import itertools

import jax
import jax.numpy as jnp
from jax import lax
from jax.experimental import pallas as pl
from jax.experimental.pallas import tpu as pltpu
from jax.sharding import Mesh
from jax.sharding import PartitionSpec as P

HEADS = 16
SIZE = 80
D = HEADS * SIZE
LOCAL = 512
WIN = 2 * LOCAL
PAD = WIN + 256
QB = 256
IMAGES = 256
WIDTHS = (256, 384, 512, 640, 768, 896, 1024)
HALF = D // 2
KR = 160
CG = 640
TOKEN_AXES = ("x", "co", "z", "yh")
ALL_AXES = TOKEN_AXES + ("dp",)
LOG2E = 1.4426950408889634


def permutation(move):
    def index(x, co, z, y):
        return ((x * 2 + co) * 8 + (z * 2 + y // 2)) * 2 + y % 2

    places = itertools.product(range(4), range(2), range(4), range(4))
    return [(index(*place), index(*move(*place))) for place in places]


Y_UP = permutation(lambda x, co, z, y: (x, co, z, (y + 1) % 4))
Y_DOWN = permutation(lambda x, co, z, y: (x, co, z, (y - 1) % 4))
X_UP = permutation(lambda x, co, z, y: ((x + 1) % 4, co, z, y))
X_DOWN = permutation(lambda x, co, z, y: ((x - 1) % 4, co, z, y))
Z_UP = permutation(lambda x, co, z, y: (x, co, (z + 1) % 4, y))
Z_DOWN = permutation(lambda x, co, z, y: (x, co, (z - 1) % 4, y))
CORE = permutation(lambda x, co, z, y: (x, 1 - co, z, y))


def moved(piece, pairs):
    return lax.ppermute(piece, ALL_AXES, pairs)


def first_pieces(w_qkv, w_out):
    x, co, z = (lax.axis_index(a) for a in ("x", "co", "z"))
    pieces = []
    for side in range(2):
        a = lax.dynamic_slice(w_qkv, (x * KR, (co * 2 + side) * CG), (KR, CG))
        b = lax.dynamic_slice(w_qkv, (z * KR, (4 + side) * CG), (KR, CG))
        c = lax.dynamic_slice(w_out, (z * KR, side * CG), (KR, CG))
        pieces.append(jnp.stack([a, jnp.where(co == 0, b, c)]))
    return pieces


def attention_kernel(
    place_ref, ends_ref, own_ref, prev_ref, gain_ref, wqkv_ref, wout_ref, mine_ref, other_ref,
    spans_ref, image_ref, lens_ref,
    hprev_ref, hown_ref, pooled_ref,
    x_ref, w_ref, wo_ref, q_ref, k_ref, vt_ref, ctx_ref, bias_ref, hid_ref, sem,
):
    x, z, co, dp = (place_ref[i] for i in range(4))
    lo = ends_ref[0, LOCAL]
    hi = jnp.where(ends_ref[1, WIN - 1] == WIN, WIN, ends_ref[0, WIN - 1])
    base = (lo // 128) * 128
    blocks = (hi - base + QB - 1) // QB

    copies = [
        pltpu.make_async_copy(prev_ref, x_ref.at[pl.ds(0, LOCAL)], sem.at[0]),
        pltpu.make_async_copy(own_ref, x_ref.at[pl.ds(LOCAL, LOCAL)], sem.at[0]),
        pltpu.make_async_copy(wqkv_ref, w_ref.at[pl.ds(dp * HALF, HALF)], sem.at[1]),
        pltpu.make_async_copy(wout_ref, wo_ref.at[pl.ds(dp * HALF, HALF)], sem.at[1]),
    ]
    far = (1 - dp) * HALF
    order = (
        [(0, x, 0), (0, x, 1), (1, z, 0), (1, z, 1)]
        + [(0, (x + 3) % 4, 0), (0, (x + 3) % 4, 1), (0, (x + 1) % 4, 0), (0, (x + 1) % 4, 1)]
        + [(1, (z + 3) % 4, 0), (1, (z + 3) % 4, 1), (1, (z + 1) % 4, 0), (1, (z + 1) % 4, 1)]
        + [(0, (x + 2) % 4, 0), (0, (x + 2) % 4, 1), (1, (z + 2) % 4, 0), (1, (z + 2) % 4, 1)]
    )
    for c in copies:
        c.start()
    for source, core in ((mine_ref, co), (other_ref, 1 - co)):
        for slot, (part, row, side) in enumerate(order):
            rows = pl.ds(pl.multiple_of(far + row * KR, 16), KR)
            if part == 0:
                cols = pl.ds(pl.multiple_of((core * 2 + side) * CG, 128), CG)
                pltpu.make_async_copy(source.at[slot], w_ref.at[rows, cols], sem.at[1]).start()
            else:

                @pl.when(core == 0)
                def _(source=source, slot=slot, rows=rows, side=side):
                    cols = pl.ds((4 + side) * CG, CG)
                    pltpu.make_async_copy(source.at[slot], w_ref.at[rows, cols], sem.at[1]).start()

                @pl.when(core == 1)
                def _(source=source, slot=slot, rows=rows, side=side):
                    cols = pl.ds(side * CG, CG)
                    pltpu.make_async_copy(source.at[slot], wo_ref.at[rows, cols], sem.at[1]).start()

    x_ref[WIN:, :] = jnp.zeros((PAD - WIN, D), jnp.bfloat16)
    k_ref[...] = jnp.zeros_like(k_ref)
    vt_ref[...] = jnp.zeros_like(vt_ref)
    hid_ref[...] = jnp.zeros_like(hid_ref)
    copies[0].wait()
    copies[1].wait()
    copies[2].wait()
    copies[3].wait()
    for source in (mine_ref, other_ref):
        for slot in range(16):
            pltpu.make_async_copy(
                source.at[slot], w_ref.at[pl.ds(0, KR), pl.ds(0, CG)], sem.at[1]
            ).wait()

    def project(j, carry):
        row0 = pl.multiple_of(base + j * QB, 128)
        rows = pl.ds(row0, QB)
        values = x_ref[rows, :].astype(jnp.float32)
        center = values - jnp.mean(values, axis=1, keepdims=True)
        spread = jnp.mean(center * center, axis=1, keepdims=True)
        normed = (center * lax.rsqrt(spread + 1e-05) * gain_ref[...]).astype(jnp.bfloat16)
        q = jnp.dot(normed, w_ref[:, 0:D], preferred_element_type=jnp.float32)
        q_ref[rows, :] = (q * (LOG2E * SIZE**-0.5)).astype(jnp.bfloat16)
        k = jnp.dot(normed, w_ref[:, D : 2 * D], preferred_element_type=jnp.float32)
        k_ref[rows, :] = k.astype(jnp.bfloat16)
        v = jnp.dot(normed, w_ref[:, 2 * D : 3 * D], preferred_element_type=jnp.float32)
        vt_ref[:, rows] = v.T.astype(jnp.bfloat16)
        return carry

    lax.fori_loop(0, blocks, project, 0)

    def attend(j, carry):
        row0 = pl.multiple_of(base + j * QB, 128)
        rows = pl.ds(row0, QB)
        least = ends_ref[0, jnp.maximum(row0, lo)]
        most = ends_ref[1, jnp.minimum(row0 + QB, hi) - 1]
        k0 = pl.multiple_of((least // 128) * 128, 128)
        need = most - k0
        start = spans_ref[0:1, rows]
        end = spans_ref[1:2, rows]
        for i, width in enumerate(WIDTHS):
            above = WIDTHS[i - 1] if i else 0

            @pl.when((need > above) & (need <= width))
            def _(width=width):
                keys = pl.ds(k0, width)
                at = lax.broadcasted_iota(jnp.int32, (width, QB), 0) + k0
                bias_ref[0:width, :] = jnp.where((at >= start) & (at < end), 0.0, -1e30)

                def one_head(h, inner):
                    w0 = pl.multiple_of(jnp.minimum((h * SIZE) // 128 * 128, D - 256), 128)
                    window = pl.ds(w0, 256)
                    lane = lax.broadcasted_iota(jnp.int32, (QB, 256), 1) + (w0 - h * SIZE)
                    q = jnp.where((lane >= 0) & (lane < SIZE), q_ref[rows, window], 0)
                    s = lax.dot_general(
                        k_ref[keys, window], q.astype(jnp.bfloat16), (((1,), (1,)), ((), ())),
                        preferred_element_type=jnp.float32,
                    )
                    s = s + bias_ref[0:width, :]
                    top = jnp.max(s, axis=0, keepdims=True)
                    p = jnp.exp2(s - top)
                    total = jnp.sum(p, axis=0, keepdims=True)
                    features = pl.ds(pl.multiple_of(h * SIZE, 16), SIZE)
                    c = jnp.dot(
                        vt_ref[features, keys], p.astype(jnp.bfloat16),
                        preferred_element_type=jnp.float32,
                    )
                    ctx_ref[features, :] = (c * (1.0 / total)).astype(jnp.bfloat16)
                    return inner

                lax.fori_loop(0, HEADS, one_head, 0, unroll=2)

        mixed = lax.dot_general(
            ctx_ref[...], wo_ref[...], (((0,), (0,)), ((), ())),
            preferred_element_type=jnp.float32,
        )
        hidden = x_ref[rows, :].astype(jnp.float32) + mixed
        at = lax.broadcasted_iota(jnp.int32, (QB, D), 0) + row0
        hidden = jnp.where((at >= lo) & (at < hi), hidden, 0.0)
        hid_ref[rows, :] = hidden.astype(jnp.bfloat16)
        return carry

    lax.fori_loop(0, blocks, attend, 0)

    hprev_ref[...] = hid_ref[0:LOCAL, :]
    hown_ref[...] = hid_ref[LOCAL:WIN, :]
    label = lax.broadcasted_iota(jnp.int32, (IMAGES, WIN), 0)
    at = lax.broadcasted_iota(jnp.int32, (IMAGES, WIN), 1)
    member = (label == image_ref[...]) & (at >= lo) & (at < hi)
    sums = jnp.dot(
        jnp.where(member, 1.0, 0.0).astype(jnp.bfloat16), hid_ref[0:WIN, :],
        preferred_element_type=jnp.float32,
    )
    pooled_ref[...] = (sums / lens_ref[...]).astype(jnp.bfloat16)


def attention(place, spans, image, lens, own, prev, gain, w_qkv, w_out, mine, other):
    hbm = pl.BlockSpec(memory_space=pltpu.HBM)
    vmem = pl.BlockSpec(memory_space=pltpu.VMEM)
    smem = pl.BlockSpec(memory_space=pltpu.SMEM)
    return pl.pallas_call(
        attention_kernel,
        out_shape=(
            jax.ShapeDtypeStruct((LOCAL, D), jnp.bfloat16),
            jax.ShapeDtypeStruct((LOCAL, D), jnp.bfloat16),
            jax.ShapeDtypeStruct((IMAGES, D), jnp.bfloat16),
        ),
        in_specs=[smem, smem, hbm, hbm, vmem, hbm, hbm, hbm, hbm, vmem, vmem, vmem],
        out_specs=(vmem, vmem, vmem),
        scratch_shapes=[
            pltpu.VMEM((PAD, D), jnp.bfloat16),
            pltpu.VMEM((D, 3 * D), jnp.bfloat16),
            pltpu.VMEM((D, D), jnp.bfloat16),
            pltpu.VMEM((PAD, D), jnp.bfloat16),
            pltpu.VMEM((PAD, D), jnp.bfloat16),
            pltpu.VMEM((D, PAD), jnp.bfloat16),
            pltpu.VMEM((D, QB), jnp.bfloat16),
            pltpu.VMEM((WIDTHS[-1], QB), jnp.float32),
            pltpu.VMEM((PAD, D), jnp.bfloat16),
            pltpu.SemaphoreType.DMA((2,)),
        ],
        compiler_params=pltpu.CompilerParams(vmem_limit_bytes=60 * 2**20),
        cost_estimate=pl.CostEstimate(
            flops=30_000_000_000, bytes_accessed=20_000_000, transcendentals=10_000_000
        ),
        name="attention",
    )(place, spans, own, prev, gain, w_qkv, w_out, mine, other, spans, image, lens)


def shards(tokens, lengths, ln_gain, w_qkv, w_out):
    x, co, z, yh, dp = (lax.axis_index(a) for a in ALL_AXES)
    shard = (x * 2 + co) * 8 + z * 2 + yh
    own = tokens[0]

    p0, p1 = first_pieces(w_qkv, w_out)
    r0 = moved(p0, Y_UP)
    r1 = moved(p1, Y_DOWN)
    a0 = jnp.stack([r0[0], r1[0]])
    b0 = jnp.stack([r0[1], r1[1]])
    sent, a0, b0 = lax.optimization_barrier((own, a0, b0))
    prev = lax.ppermute(sent, TOKEN_AXES, [(i, i + 1) for i in range(63)])
    a1, a2 = moved(a0, X_UP), moved(a0, X_DOWN)
    b1, b2 = moved(b0, Z_UP), moved(b0, Z_DOWN)
    a3, a4 = moved(a1[0], X_UP), moved(a2[1], X_DOWN)
    b3, b4 = moved(b1[0], Z_UP), moved(b2[1], Z_DOWN)
    mine = jnp.concatenate(
        [a0, b0, a1, a2, b1, b2, a3[None], a4[None], b3[None], b4[None]], axis=0
    )
    other = moved(mine, CORE)

    lens = lengths[0]
    ends = jnp.cumsum(lens)
    offsets = ends - lens
    first = (shard - 1) * LOCAL
    at = first + jnp.arange(PAD, dtype=jnp.int32)
    begun = offsets[:, None] <= at[None, :]
    image = jnp.sum(begun.astype(jnp.int32), axis=0) - 1
    start = jnp.max(jnp.where(begun, offsets[:, None], -WIN), axis=0) - first
    end = jnp.min(jnp.where(ends[:, None] > at[None, :], ends[:, None], 1 << 20), axis=0) - first
    spans = jnp.stack([start, end]).astype(jnp.int32)
    place = jnp.stack([x, z, co, dp]).astype(jnp.int32)

    hprev, hown, part = attention(
        place, spans, image[None, :WIN], lens.astype(jnp.float32)[:, None], own, prev,
        ln_gain[None], w_qkv, w_out, mine, other,
    )
    back = lax.ppermute(hprev, TOKEN_AXES, [(i + 1, i) for i in range(63)])

    swap = [(0, 1), (1, 0)]
    group = ("x", "z", "yh")
    part = part.reshape(2, IMAGES // 2, D)
    kept = lax.dynamic_index_in_dim(part, co, 0, keepdims=False)
    given = lax.dynamic_index_in_dim(part, 1 - co, 0, keepdims=False)
    kept = kept.astype(jnp.float32) + lax.ppermute(given, "co", swap).astype(jnp.float32)
    kept = kept.astype(jnp.bfloat16).reshape(32, 4, D)
    rows = lax.all_to_all(kept, group, 0, 0, tiled=True).astype(jnp.float32)
    rows = jnp.sum(rows, axis=0).astype(jnp.bfloat16)
    half = lax.all_to_all(jnp.broadcast_to(rows[None], (32, 4, D)), group, 0, 0, tiled=True)
    half = half.reshape(IMAGES // 2, D)
    rest = lax.ppermute(half, "co", swap)
    pooled = jnp.where(co == 0, jnp.stack([half, rest]), jnp.stack([rest, half]))
    pooled = pooled.reshape(1, IMAGES, D).astype(jnp.float32)

    limit = jnp.where(end[WIN - 1] == WIN, WIN, start[WIN - 1]) - LOCAL
    here = jnp.arange(LOCAL, dtype=jnp.int32)[:, None] < limit
    hidden = jnp.where(here, hown, back)[None]
    return hidden, pooled


def solution(mesh):
    fine = Mesh(mesh.devices.reshape(4, 2, 4, 2, 2), ALL_AXES)
    in_specs = (P("dp", TOKEN_AXES, None), P("dp", None), P(), P("dp", None), P("dp", None))
    out_specs = (P("dp", TOKEN_AXES, None), P("dp", None, None))
    return jax.shard_map(
        shards, mesh=fine, in_specs=in_specs, out_specs=out_specs, check_vma=False
    )
```

```python
import itertools

import jax
import jax.numpy as jnp
from jax import lax
from jax.experimental import pallas as pl
from jax.experimental.pallas import tpu as pltpu
from jax.sharding import Mesh
from jax.sharding import PartitionSpec as P


HEADS = 16
SIZE = 80
VROWS = 96
D = HEADS * SIZE
LOCAL = 512
WIN = 2 * LOCAL
PAD = WIN + 256
QB = 256
IMAGES = 256
WIDTHS = (256, 384, 512, 640, 768, 896, 1024)
HALF = D // 2
KR = 160
CG = 640
TOKEN_AXES = ("x", "co", "z", "yh")
ALL_AXES = TOKEN_AXES + ("dp",)
LOG2E = 1.4426950408889634


def permutation(move):
    def index(x, co, z, y):
        return ((x * 2 + co) * 8 + (z * 2 + y // 2)) * 2 + y % 2

    places = itertools.product(range(4), range(2), range(4), range(4))
    return [(index(*place), index(*move(*place))) for place in places]


Y_UP = permutation(lambda x, co, z, y: (x, co, z, (y + 1) % 4))
Y_DOWN = permutation(lambda x, co, z, y: (x, co, z, (y - 1) % 4))
X_UP = permutation(lambda x, co, z, y: ((x + 1) % 4, co, z, y))
X_DOWN = permutation(lambda x, co, z, y: ((x - 1) % 4, co, z, y))
Z_UP = permutation(lambda x, co, z, y: (x, co, (z + 1) % 4, y))
Z_DOWN = permutation(lambda x, co, z, y: (x, co, (z - 1) % 4, y))
CORE = permutation(lambda x, co, z, y: (x, 1 - co, z, y))


def moved(piece, pairs):
    return lax.ppermute(piece, ALL_AXES, pairs)


def first_pieces(w_qkv, w_out):
    x, co, z = (lax.axis_index(a) for a in ("x", "co", "z"))
    pieces = []
    for side in range(2):
        a = lax.dynamic_slice(w_qkv, (x * KR, (co * 2 + side) * CG), (KR, CG))
        b = lax.dynamic_slice(w_qkv, (z * KR, (4 + side) * CG), (KR, CG))
        c = lax.dynamic_slice(w_out, (z * KR, side * CG), (KR, CG))
        pieces.append(jnp.stack([a, jnp.where(co == 0, b, c)]))
    return pieces


def attention_kernel(
    place_ref, ends_ref, own_ref, prev_ref, gain_ref, wqkv_ref, wout_ref, mine_ref, other_ref,
    spans_ref, image_ref, lens_ref,
    hprev_ref, hown_ref, pooled_ref,
    x_ref, n_ref, w_ref, wo_ref, q_ref, k_ref, vt_ref, ctx_ref, bias_ref, hid_ref,
    s0_ref, s1_ref, p0_ref, p1_ref, top0_ref, top1_ref, sem,
):
    x, z, co, dp = (place_ref[i] for i in range(4))
    lo = ends_ref[0, LOCAL]
    hi = jnp.where(ends_ref[1, WIN - 1] == WIN, WIN, ends_ref[0, WIN - 1])
    base = (lo // 128) * 128
    blocks = (hi - base + QB - 1) // QB

    far = (1 - dp) * HALF
    order = (
        [(0, x, 0), (0, x, 1), (1, z, 0), (1, z, 1)]
        + [(0, (x + 3) % 4, 0), (0, (x + 3) % 4, 1), (0, (x + 1) % 4, 0), (0, (x + 1) % 4, 1)]
        + [(1, (z + 3) % 4, 0), (1, (z + 3) % 4, 1), (1, (z + 1) % 4, 0), (1, (z + 1) % 4, 1)]
        + [(0, (x + 2) % 4, 0), (0, (x + 2) % 4, 1), (1, (z + 2) % 4, 0), (1, (z + 2) % 4, 1)]
    )

    pltpu.make_async_copy(prev_ref, x_ref.at[pl.ds(0, LOCAL)], sem.at[0]).start()
    pltpu.make_async_copy(own_ref, x_ref.at[pl.ds(LOCAL, LOCAL)], sem.at[0]).start()

    def near(part, target, cols):
        return pltpu.make_async_copy(
            wout_ref if part == 3 else wqkv_ref.at[:, cols],
            target.at[pl.ds(pl.multiple_of(dp * HALF, 16), HALF), cols],
            sem.at[1 + part],
        )

    def distant(part, source, slot, row, side):
        target = wo_ref if part == 3 else w_ref
        rows = pl.ds(pl.multiple_of(far + row * KR, 16), KR)
        cols = pl.ds((0 if part == 3 else part * D) + side * CG, CG)
        return pltpu.make_async_copy(source.at[slot], target.at[rows, cols], sem.at[1 + part])

    columns = [pl.ds(0, D), pl.ds(D, D), pl.ds(2 * D, D), pl.ds(0, D)]
    targets = [w_ref, w_ref, w_ref, wo_ref]
    for part in range(4):
        near(part, targets[part], columns[part]).start()
        for source, core in ((mine_ref, co), (other_ref, 1 - co)):

            @pl.when(core == part % 2)
            def _(source=source, part=part):
                for slot, (kind, row, side) in enumerate(order):
                    if kind == part // 2:
                        distant(part, source, slot, row, side).start()

    def arrived(part):
        near(part, targets[part], columns[part]).wait()
        for slot in range(8):
            distant(part, mine_ref, slot, 0, 0).wait()

    x_ref[WIN:, :] = jnp.zeros((PAD - WIN, D), jnp.bfloat16)
    pltpu.make_async_copy(prev_ref, x_ref.at[pl.ds(0, LOCAL)], sem.at[0]).wait()
    pltpu.make_async_copy(own_ref, x_ref.at[pl.ds(LOCAL, LOCAL)], sem.at[0]).wait()

    def block_rows(j):
        row0 = pl.multiple_of(base + j * QB, 128)
        return row0, pl.ds(row0, QB)

    def normalize(j, carry):
        _, rows = block_rows(j)
        values = x_ref[rows, :].astype(jnp.float32)
        center = values - jnp.mean(values, axis=1, keepdims=True)
        spread = jnp.mean(center * center, axis=1, keepdims=True)
        normed = center * lax.rsqrt(spread + 1e-05) * gain_ref[...]
        n_ref[rows, :] = normed.astype(jnp.bfloat16)
        return carry

    lax.fori_loop(0, blocks, normalize, 0)
    k_ref[...] = jnp.zeros_like(k_ref)
    vt_ref[...] = jnp.zeros_like(vt_ref)
    hid_ref[...] = jnp.zeros_like(hid_ref)

    def project_q(j, carry):
        _, rows = block_rows(j)
        q = jnp.dot(n_ref[rows, :], w_ref[:, 0:D], preferred_element_type=jnp.float32)
        q_ref[rows, :] = (q * (LOG2E * SIZE**-0.5)).astype(jnp.bfloat16)
        return carry

    def project_k(j, carry):
        _, rows = block_rows(j)
        k = jnp.dot(n_ref[rows, :], w_ref[:, D : 2 * D], preferred_element_type=jnp.float32)
        k_ref[rows, :] = k.astype(jnp.bfloat16)
        return carry

    def project_v(j, carry):
        _, rows = block_rows(j)
        v = jnp.dot(n_ref[rows, :], w_ref[:, 2 * D :], preferred_element_type=jnp.float32)
        vt = v.T.astype(jnp.bfloat16)
        for h in range(HEADS):
            vt_ref[pl.ds(h * VROWS, SIZE), rows] = vt[h * SIZE : (h + 1) * SIZE]
            vt_ref[pl.ds(h * VROWS + SIZE, VROWS - SIZE), rows] = jnp.ones(
                (VROWS - SIZE, QB), jnp.bfloat16
            )
        return carry

    for part, project in enumerate((project_q, project_k, project_v)):
        arrived(part)
        lax.fori_loop(0, blocks, project, 0)
    arrived(3)

    def attend(j, carry):
        row0, rows = block_rows(j)
        least = ends_ref[0, jnp.maximum(row0, lo)]
        most = ends_ref[1, jnp.minimum(row0 + QB, hi) - 1]
        k0 = pl.multiple_of((least // 128) * 128, 128)
        need = most - k0
        start = spans_ref[0:1, rows]
        end = spans_ref[1:2, rows]
        for i, width in enumerate(WIDTHS):
            above = WIDTHS[i - 1] if i else 0

            @pl.when((need > above) & (need <= width))
            def _(width=width):
                keys = pl.ds(k0, width)
                at = lax.broadcasted_iota(jnp.int32, (width, QB), 0) + k0
                bias_ref[0:width, :] = jnp.where((at >= start) & (at < end), 0.0, -1e30)

                def scores(h, s_ref, top_ref):
                    w0 = pl.multiple_of(jnp.minimum((h * SIZE) // 128 * 128, D - 256), 128)
                    window = pl.ds(w0, 256)
                    lane = lax.broadcasted_iota(jnp.int32, (1, 256), 1) + (w0 - h * SIZE)
                    inside = jnp.where((lane >= 0) & (lane < SIZE), 1.0, 0.0)
                    q = q_ref[rows, window] * inside.astype(jnp.bfloat16)
                    s = lax.dot_general(
                        k_ref[keys, window], q, (((1,), (1,)), ((), ())),
                        preferred_element_type=jnp.float32,
                    )
                    s = s + bias_ref[0:width, :]
                    s_ref[0:width, :] = s
                    top_ref[...] = jnp.max(s, axis=0, keepdims=True)

                def weights(s_ref, top_ref, p_ref):
                    p_ref[0:width, :] = jnp.exp2(s_ref[0:width, :] - top_ref[...]).astype(
                        jnp.bfloat16
                    )

                def mix(h, p_ref):
                    features = pl.ds(pl.multiple_of(h * VROWS, 16), VROWS)
                    c = jnp.dot(
                        vt_ref[features, keys], p_ref[0:width, :],
                        preferred_element_type=jnp.float32,
                    )
                    ctx_ref[pl.ds(pl.multiple_of(h * SIZE, 16), SIZE), :] = (
                        c[0:SIZE] * (1.0 / c[SIZE : SIZE + 1])
                    ).astype(jnp.bfloat16)

                scores(0, s0_ref, top0_ref)

                def two_heads(i, inner):
                    h = i * 2
                    scores(h + 1, s1_ref, top1_ref)
                    weights(s0_ref, top0_ref, p0_ref)
                    mix(jnp.maximum(h - 1, 0), p1_ref)
                    scores(jnp.minimum(h + 2, HEADS - 1), s0_ref, top0_ref)
                    weights(s1_ref, top1_ref, p1_ref)
                    mix(h, p0_ref)
                    return inner

                lax.fori_loop(0, HEADS // 2, two_heads, 0)
                mix(HEADS - 1, p1_ref)

        mixed = lax.dot_general(
            ctx_ref[...], wo_ref[...], (((0,), (0,)), ((), ())),
            preferred_element_type=jnp.float32,
        )
        hidden = x_ref[rows, :].astype(jnp.float32) + mixed
        at = lax.broadcasted_iota(jnp.int32, (QB, D), 0) + row0
        hidden = jnp.where((at >= lo) & (at < hi), hidden, 0.0)
        hid_ref[rows, :] = hidden.astype(jnp.bfloat16)
        return carry

    lax.fori_loop(0, blocks, attend, 0)

    hprev_ref[...] = hid_ref[0:LOCAL, :]
    hown_ref[...] = hid_ref[LOCAL:WIN, :]
    label = lax.broadcasted_iota(jnp.int32, (IMAGES, WIN), 0)
    at = lax.broadcasted_iota(jnp.int32, (IMAGES, WIN), 1)
    member = (label == image_ref[...]) & (at >= lo) & (at < hi)
    sums = jnp.dot(
        jnp.where(member, 1.0, 0.0).astype(jnp.bfloat16), hid_ref[0:WIN, :],
        preferred_element_type=jnp.float32,
    )
    pooled_ref[...] = (sums / lens_ref[...]).astype(jnp.bfloat16)


def attention(place, spans, image, lens, own, prev, gain, w_qkv, w_out, mine, other):
    hbm = pl.BlockSpec(memory_space=pltpu.HBM)
    vmem = pl.BlockSpec(memory_space=pltpu.VMEM)
    smem = pl.BlockSpec(memory_space=pltpu.SMEM)
    return pl.pallas_call(
        attention_kernel,
        out_shape=(
            jax.ShapeDtypeStruct((LOCAL, D), jnp.bfloat16),
            jax.ShapeDtypeStruct((LOCAL, D), jnp.bfloat16),
            jax.ShapeDtypeStruct((IMAGES, D), jnp.bfloat16),
        ),
        in_specs=[smem, smem, hbm, hbm, vmem, hbm, hbm, hbm, hbm, vmem, vmem, vmem],
        out_specs=(vmem, vmem, vmem),
        scratch_shapes=[
            pltpu.VMEM((PAD, D), jnp.bfloat16),
            pltpu.VMEM((PAD, D), jnp.bfloat16),
            pltpu.VMEM((D, 3 * D), jnp.bfloat16),
            pltpu.VMEM((D, D), jnp.bfloat16),
            pltpu.VMEM((PAD, D), jnp.bfloat16),
            pltpu.VMEM((PAD, D), jnp.bfloat16),
            pltpu.VMEM((HEADS * VROWS, PAD), jnp.bfloat16),
            pltpu.VMEM((D, QB), jnp.bfloat16),
            pltpu.VMEM((WIDTHS[-1], QB), jnp.float32),
            pltpu.VMEM((PAD, D), jnp.bfloat16),
            pltpu.VMEM((WIDTHS[-1], QB), jnp.float32),
            pltpu.VMEM((WIDTHS[-1], QB), jnp.float32),
            pltpu.VMEM((WIDTHS[-1], QB), jnp.bfloat16),
            pltpu.VMEM((WIDTHS[-1], QB), jnp.bfloat16),
            pltpu.VMEM((1, QB), jnp.float32),
            pltpu.VMEM((1, QB), jnp.float32),
            pltpu.SemaphoreType.DMA((5,)),
        ],
        compiler_params=pltpu.CompilerParams(vmem_limit_bytes=60 * 2**20),
        cost_estimate=pl.CostEstimate(
            flops=30_000_000_000, bytes_accessed=20_000_000, transcendentals=10_000_000
        ),
        name="attention",
    )(place, spans, own, prev, gain, w_qkv, w_out, mine, other, spans, image, lens)


def layer(tokens, lengths, ln_gain, w_qkv, w_out):
    x, co, z, yh, dp = (lax.axis_index(a) for a in ALL_AXES)
    shard = (x * 2 + co) * 8 + z * 2 + yh
    own = tokens[0]

    p0, p1 = first_pieces(w_qkv, w_out)
    r0 = moved(p0, Y_UP)
    r1 = moved(p1, Y_DOWN)
    a0 = jnp.stack([r0[0], r1[0]])
    b0 = jnp.stack([r0[1], r1[1]])
    prev = lax.ppermute(own, TOKEN_AXES, [(i, i + 1) for i in range(63)])
    a1, a2 = moved(a0, X_UP), moved(a0, X_DOWN)
    b1, b2 = moved(b0, Z_UP), moved(b0, Z_DOWN)
    a3, a4 = moved(a1[0], X_UP), moved(a2[1], X_DOWN)
    b3, b4 = moved(b1[0], Z_UP), moved(b2[1], Z_DOWN)
    mine = jnp.concatenate(
        [a0, b0, a1, a2, b1, b2, a3[None], a4[None], b3[None], b4[None]], axis=0
    )
    other = moved(mine, CORE)

    lens = lengths[0]
    ends = jnp.cumsum(lens)
    offsets = ends - lens
    first = (shard - 1) * LOCAL
    at = first + jnp.arange(PAD, dtype=jnp.int32)
    begun = offsets[:, None] <= at[None, :]
    image = jnp.sum(begun.astype(jnp.int32), axis=0) - 1
    start = jnp.max(jnp.where(begun, offsets[:, None], -WIN), axis=0) - first
    end = jnp.min(jnp.where(ends[:, None] > at[None, :], ends[:, None], 1 << 20), axis=0) - first
    spans = jnp.stack([start, end]).astype(jnp.int32)
    place = jnp.stack([x, z, co, dp]).astype(jnp.int32)

    hprev, hown, part = attention(
        place, spans, image[None, :WIN], lens.astype(jnp.float32)[:, None], own, prev,
        ln_gain[None], w_qkv, w_out, mine, other,
    )
    back = lax.ppermute(hprev, TOKEN_AXES, [(i + 1, i) for i in range(63)])

    swap = [(0, 1), (1, 0)]
    group = ("x", "z", "yh")
    part = part.reshape(2, IMAGES // 2, D)
    kept = lax.dynamic_index_in_dim(part, co, 0, keepdims=False)
    given = lax.dynamic_index_in_dim(part, 1 - co, 0, keepdims=False)
    given = lax.ppermute(given, "co", swap)
    kept = kept.astype(jnp.float32) + given.astype(jnp.float32)
    kept = kept.astype(jnp.bfloat16).reshape(32, 4, D)
    rows = lax.all_to_all(kept, group, 0, 0, tiled=True).astype(jnp.float32)
    rows = jnp.sum(rows, axis=0).astype(jnp.bfloat16)
    half = lax.all_to_all(jnp.broadcast_to(rows[None], (32, 4, D)), group, 0, 0, tiled=True)
    half = half.reshape(IMAGES // 2, D)
    rest = lax.ppermute(half, "co", swap)
    pooled = jnp.where(co == 0, jnp.stack([half, rest]), jnp.stack([rest, half]))
    pooled = pooled.reshape(1, IMAGES, D).astype(jnp.float32)

    limit = jnp.where(end[WIN - 1] == WIN, WIN, start[WIN - 1]) - LOCAL
    here = jnp.arange(LOCAL, dtype=jnp.int32)[:, None] < limit
    hidden = jnp.where(here, hown, back)[None]
    return hidden, pooled


def solution(mesh):
    fine = Mesh(mesh.devices.reshape(4, 2, 4, 2, 2), ALL_AXES)
    in_specs = (P("dp", TOKEN_AXES, None), P("dp", None), P(), P("dp", None), P("dp", None))
    out_specs = (P("dp", TOKEN_AXES, None), P("dp", None, None))
    return jax.shard_map(layer, mesh=fine, in_specs=in_specs, out_specs=out_specs, check_vma=False)
```

```python
import itertools

import jax
import jax.numpy as jnp
from jax import lax
from jax.experimental import pallas as pl
from jax.experimental.pallas import tpu as pltpu
from jax.sharding import Mesh
from jax.sharding import PartitionSpec as P


HEADS = 16
SIZE = 80
VROWS = 96
D = HEADS * SIZE
LOCAL = 512
WIN = 2 * LOCAL
PAD = WIN + 256
QB = 256
IMAGES = 256
WIDTHS = (256, 384, 512, 640, 768, 896, 1024)
HALF = D // 2
KR = 160
TOKEN_AXES = ("x", "co", "z", "yh")
ALL_AXES = TOKEN_AXES + ("dp",)
LOG2E = 1.4426950408889634


def permutation(move):
    def index(x, co, z, y):
        return ((x * 2 + co) * 8 + (z * 2 + y // 2)) * 2 + y % 2

    places = itertools.product(range(4), range(2), range(4), range(4))
    return [(index(*place), index(*move(*place))) for place in places]


Y_UP = permutation(lambda x, co, z, y: (x, co, z, (y + 1) % 4))
Y_DOWN = permutation(lambda x, co, z, y: (x, co, z, (y - 1) % 4))
X_UP = permutation(lambda x, co, z, y: ((x + 1) % 4, co, z, y))
X_DOWN = permutation(lambda x, co, z, y: ((x - 1) % 4, co, z, y))
Z_UP = permutation(lambda x, co, z, y: (x, co, (z + 1) % 4, y))
Z_DOWN = permutation(lambda x, co, z, y: (x, co, (z - 1) % 4, y))
CORE = permutation(lambda x, co, z, y: (x, 1 - co, z, y))


def moved(piece, pairs):
    return lax.ppermute(piece, ALL_AXES, pairs)


def first_pieces(w_qkv, w_out):
    x, co = lax.axis_index("x"), lax.axis_index("co")
    pieces = []
    for side in range(2):
        part = co * 2 + side
        q = lax.dynamic_slice(w_qkv, (x * KR, jnp.minimum(part, 2) * D), (KR, D))
        o = lax.dynamic_slice(w_out, (x * KR, 0), (KR, D))
        pieces.append(q if side == 0 else jnp.where(co == 0, q, o))
    return pieces


def attention_kernel(
    place_ref, ends_ref, own_ref, prev_ref, gain_ref, wqkv_ref, wout_ref, *refs
):
    mine_refs, other_refs, refs = refs[:8], refs[8:16], refs[16:]
    (
        spans_ref, image_ref, lens_ref, hprev_ref, hown_ref, pooled_ref,
        x_ref, n_ref, w_ref, wo_ref, q_ref, k_ref, vt_ref, ctx_ref, bias_ref, hid_ref,
        s0_ref, s1_ref, p0_ref, p1_ref, top0_ref, top1_ref, sem,
    ) = refs
    x, co, dp = (place_ref[i] for i in range(3))
    lo = ends_ref[0, LOCAL]
    hi = jnp.where(ends_ref[1, WIN - 1] == WIN, WIN, ends_ref[0, WIN - 1])
    base = (lo // 128) * 128
    blocks = (hi - base + QB - 1) // QB

    far = (1 - dp) * HALF

    pltpu.make_async_copy(prev_ref, x_ref.at[pl.ds(0, LOCAL)], sem.at[0]).start()
    pltpu.make_async_copy(own_ref, x_ref.at[pl.ds(LOCAL, LOCAL)], sem.at[0]).start()

    def near(part, target, cols):
        return pltpu.make_async_copy(
            wout_ref if part == 3 else wqkv_ref.at[:, cols],
            target.at[pl.ds(pl.multiple_of(dp * HALF, 16), HALF), cols],
            sem.at[1 + part],
        )

    def distant(part, source, row):
        target = wo_ref if part == 3 else w_ref
        rows = pl.ds(pl.multiple_of(far + row * KR, 16), KR)
        return pltpu.make_async_copy(source, target.at[rows, columns[part]], sem.at[1 + part])

    columns = [pl.ds(0, D), pl.ds(D, D), pl.ds(2 * D, D), pl.ds(0, D)]
    targets = [w_ref, w_ref, w_ref, wo_ref]
    shift = (0, 3, 1, 2)
    for part in range(4):
        near(part, targets[part], columns[part]).start()
        for held, core in ((mine_refs, co), (other_refs, 1 - co)):

            @pl.when(core == part // 2)
            def _(held=held, part=part):
                for slot in range(4):
                    row = lax.rem(x + shift[slot], 4)
                    distant(part, held[slot * 2 + part % 2], row).start()

    def arrived(part):
        near(part, targets[part], columns[part]).wait()
        for _ in range(4):
            distant(part, mine_refs[0], 0).wait()

    x_ref[WIN:, :] = jnp.zeros((PAD - WIN, D), jnp.bfloat16)
    pltpu.make_async_copy(prev_ref, x_ref.at[pl.ds(0, LOCAL)], sem.at[0]).wait()
    pltpu.make_async_copy(own_ref, x_ref.at[pl.ds(LOCAL, LOCAL)], sem.at[0]).wait()

    def block_rows(j):
        row0 = pl.multiple_of(base + j * QB, 128)
        return row0, pl.ds(row0, QB)

    def normalize(j, carry):
        _, rows = block_rows(j)
        values = x_ref[rows, :].astype(jnp.float32)
        center = values - jnp.mean(values, axis=1, keepdims=True)
        spread = jnp.mean(center * center, axis=1, keepdims=True)
        normed = center * lax.rsqrt(spread + 1e-05) * gain_ref[...]
        n_ref[rows, :] = normed.astype(jnp.bfloat16)
        return carry

    lax.fori_loop(0, blocks, normalize, 0)
    k_ref[...] = jnp.zeros_like(k_ref)
    vt_ref[...] = jnp.zeros_like(vt_ref)
    hid_ref[...] = jnp.zeros_like(hid_ref)

    def project_q(j, carry):
        _, rows = block_rows(j)
        q = jnp.dot(n_ref[rows, :], w_ref[:, 0:D], preferred_element_type=jnp.float32)
        q_ref[rows, :] = (q * (LOG2E * SIZE**-0.5)).astype(jnp.bfloat16)
        return carry

    def project_k(j, carry):
        _, rows = block_rows(j)
        k = jnp.dot(n_ref[rows, :], w_ref[:, D : 2 * D], preferred_element_type=jnp.float32)
        k_ref[rows, :] = k.astype(jnp.bfloat16)
        return carry

    def project_v(j, carry):
        _, rows = block_rows(j)
        v = jnp.dot(n_ref[rows, :], w_ref[:, 2 * D :], preferred_element_type=jnp.float32)
        vt = v.T.astype(jnp.bfloat16)
        for h in range(HEADS):
            vt_ref[pl.ds(h * VROWS, SIZE), rows] = vt[h * SIZE : (h + 1) * SIZE]
            vt_ref[pl.ds(h * VROWS + SIZE, VROWS - SIZE), rows] = jnp.ones(
                (VROWS - SIZE, QB), jnp.bfloat16
            )
        return carry

    for part, project in enumerate((project_q, project_k, project_v)):
        arrived(part)
        lax.fori_loop(0, blocks, project, 0)
    arrived(3)

    def attend(j, carry):
        row0, rows = block_rows(j)
        least = ends_ref[0, jnp.maximum(row0, lo)]
        most = ends_ref[1, jnp.minimum(row0 + QB, hi) - 1]
        k0 = pl.multiple_of((least // 128) * 128, 128)
        need = most - k0
        start = spans_ref[0:1, rows]
        end = spans_ref[1:2, rows]
        for i, width in enumerate(WIDTHS):
            above = WIDTHS[i - 1] if i else 0

            @pl.when((need > above) & (need <= width))
            def _(width=width):
                keys = pl.ds(k0, width)
                at = lax.broadcasted_iota(jnp.int32, (width, QB), 0) + k0
                bias_ref[0:width, :] = jnp.where((at >= start) & (at < end), 0.0, -1e30)

                def scores(h, s_ref, top_ref):
                    w0 = pl.multiple_of(jnp.minimum((h * SIZE) // 128 * 128, D - 256), 128)
                    window = pl.ds(w0, 256)
                    lane = lax.broadcasted_iota(jnp.int32, (1, 256), 1) + (w0 - h * SIZE)
                    inside = jnp.where((lane >= 0) & (lane < SIZE), 1.0, 0.0)
                    q = q_ref[rows, window] * inside.astype(jnp.bfloat16)
                    s = lax.dot_general(
                        k_ref[keys, window], q, (((1,), (1,)), ((), ())),
                        preferred_element_type=jnp.float32,
                    )
                    s = s + bias_ref[0:width, :]
                    s_ref[0:width, :] = s
                    top_ref[...] = jnp.max(s, axis=0, keepdims=True)

                def weights(s_ref, top_ref, p_ref):
                    p_ref[0:width, :] = jnp.exp2(s_ref[0:width, :] - top_ref[...]).astype(
                        jnp.bfloat16
                    )

                def mix(h, p_ref):
                    features = pl.ds(pl.multiple_of(h * VROWS, 16), VROWS)
                    c = jnp.dot(
                        vt_ref[features, keys], p_ref[0:width, :],
                        preferred_element_type=jnp.float32,
                    )
                    ctx_ref[pl.ds(pl.multiple_of(h * SIZE, 16), SIZE), :] = (
                        c[0:SIZE] * (1.0 / c[SIZE : SIZE + 1])
                    ).astype(jnp.bfloat16)

                scores(0, s0_ref, top0_ref)

                def two_heads(i, inner):
                    h = i * 2
                    scores(h + 1, s1_ref, top1_ref)
                    weights(s0_ref, top0_ref, p0_ref)
                    mix(jnp.maximum(h - 1, 0), p1_ref)
                    scores(jnp.minimum(h + 2, HEADS - 1), s0_ref, top0_ref)
                    weights(s1_ref, top1_ref, p1_ref)
                    mix(h, p0_ref)
                    return inner

                lax.fori_loop(0, HEADS // 2, two_heads, 0)
                mix(HEADS - 1, p1_ref)

        mixed = lax.dot_general(
            ctx_ref[...], wo_ref[...], (((0,), (0,)), ((), ())),
            preferred_element_type=jnp.float32,
        )
        hidden = x_ref[rows, :].astype(jnp.float32) + mixed
        at = lax.broadcasted_iota(jnp.int32, (QB, D), 0) + row0
        hidden = jnp.where((at >= lo) & (at < hi), hidden, 0.0)
        hid_ref[rows, :] = hidden.astype(jnp.bfloat16)
        return carry

    lax.fori_loop(0, blocks, attend, 0)

    hprev_ref[...] = hid_ref[0:LOCAL, :]
    hown_ref[...] = hid_ref[LOCAL:WIN, :]
    label = lax.broadcasted_iota(jnp.int32, (IMAGES, WIN), 0)
    at = lax.broadcasted_iota(jnp.int32, (IMAGES, WIN), 1)
    member = (label == image_ref[...]) & (at >= lo) & (at < hi)
    sums = jnp.dot(
        jnp.where(member, 1.0, 0.0).astype(jnp.bfloat16), hid_ref[0:WIN, :],
        preferred_element_type=jnp.float32,
    )
    pooled_ref[...] = (sums / lens_ref[...]).astype(jnp.bfloat16)


def attention(place, spans, image, lens, own, prev, gain, w_qkv, w_out, mine, other):
    hbm = pl.BlockSpec(memory_space=pltpu.HBM)
    vmem = pl.BlockSpec(memory_space=pltpu.VMEM)
    smem = pl.BlockSpec(memory_space=pltpu.SMEM)
    return pl.pallas_call(
        attention_kernel,
        out_shape=(
            jax.ShapeDtypeStruct((LOCAL, D), jnp.bfloat16),
            jax.ShapeDtypeStruct((LOCAL, D), jnp.bfloat16),
            jax.ShapeDtypeStruct((IMAGES, D), jnp.bfloat16),
        ),
        in_specs=[smem, smem, hbm, hbm, vmem, hbm, hbm] + [hbm] * 16 + [vmem] * 3,
        out_specs=(vmem, vmem, vmem),
        scratch_shapes=[
            pltpu.VMEM((PAD, D), jnp.bfloat16),
            pltpu.VMEM((PAD, D), jnp.bfloat16),
            pltpu.VMEM((D, 3 * D), jnp.bfloat16),
            pltpu.VMEM((D, D), jnp.bfloat16),
            pltpu.VMEM((PAD, D), jnp.bfloat16),
            pltpu.VMEM((PAD, D), jnp.bfloat16),
            pltpu.VMEM((HEADS * VROWS, PAD), jnp.bfloat16),
            pltpu.VMEM((D, QB), jnp.bfloat16),
            pltpu.VMEM((WIDTHS[-1], QB), jnp.float32),
            pltpu.VMEM((PAD, D), jnp.bfloat16),
            pltpu.VMEM((WIDTHS[-1], QB), jnp.float32),
            pltpu.VMEM((WIDTHS[-1], QB), jnp.float32),
            pltpu.VMEM((WIDTHS[-1], QB), jnp.bfloat16),
            pltpu.VMEM((WIDTHS[-1], QB), jnp.bfloat16),
            pltpu.VMEM((1, QB), jnp.float32),
            pltpu.VMEM((1, QB), jnp.float32),
            pltpu.SemaphoreType.DMA((5,)),
        ],
        compiler_params=pltpu.CompilerParams(vmem_limit_bytes=60 * 2**20),
        cost_estimate=pl.CostEstimate(
            flops=30_000_000_000, bytes_accessed=20_000_000, transcendentals=10_000_000
        ),
        name="attention",
    )(place, spans, own, prev, gain, w_qkv, w_out, *mine, *other, spans, image, lens)


def layer(tokens, lengths, ln_gain, w_qkv, w_out):
    x, co, z, yh, dp = (lax.axis_index(a) for a in ALL_AXES)
    shard = (x * 2 + co) * 8 + z * 2 + yh
    own = tokens[0]

    p0, p1 = first_pieces(w_qkv, w_out)
    r0 = moved(p0, Y_UP)
    r1 = moved(p1, Y_DOWN)
    prev = lax.ppermute(own, TOKEN_AXES, [(i, i + 1) for i in range(63)])
    u0 = moved(r0, X_UP)
    d1 = moved(r1, X_DOWN)
    u1 = moved(r1, X_UP)
    d0 = moved(r0, X_DOWN)
    f0 = moved(u0, X_UP)
    f1 = moved(d1, X_DOWN)
    near = [moved(a, CORE) for a in (r0, r1)]
    ring = [moved(a, CORE) for a in (u0, u1, d0, d1)]
    last = [moved(a, CORE) for a in (f0, f1)]
    mine = [r0, r1, u0, u1, d0, d1, f0, f1]
    other = near + ring + last

    lens = lengths[0]
    ends = jnp.cumsum(lens)
    offsets = ends - lens
    first = (shard - 1) * LOCAL
    at = first + jnp.arange(PAD, dtype=jnp.int32)
    begun = offsets[:, None] <= at[None, :]
    image = jnp.sum(begun.astype(jnp.int32), axis=0) - 1
    start = jnp.max(jnp.where(begun, offsets[:, None], -WIN), axis=0) - first
    end = jnp.min(jnp.where(ends[:, None] > at[None, :], ends[:, None], 1 << 20), axis=0) - first
    spans = jnp.stack([start, end]).astype(jnp.int32)
    place = jnp.stack([x, co, dp]).astype(jnp.int32)

    hprev, hown, part = attention(
        place, spans, image[None, :WIN], lens.astype(jnp.float32)[:, None], own, prev,
        ln_gain[None], w_qkv, w_out, mine, other,
    )
    back = lax.ppermute(hprev, TOKEN_AXES, [(i + 1, i) for i in range(63)])

    swap = [(0, 1), (1, 0)]
    group = ("x", "z", "yh")
    part = part.reshape(2, IMAGES // 2, D)
    kept = lax.dynamic_index_in_dim(part, co, 0, keepdims=False)
    given = lax.dynamic_index_in_dim(part, 1 - co, 0, keepdims=False)
    given = lax.ppermute(given, "co", swap)
    kept = kept.astype(jnp.float32) + given.astype(jnp.float32)
    kept = kept.astype(jnp.bfloat16).reshape(32, 4, D)
    rows = lax.all_to_all(kept, group, 0, 0, tiled=True).astype(jnp.float32)
    rows = jnp.sum(rows, axis=0).astype(jnp.bfloat16)
    half = lax.all_to_all(jnp.broadcast_to(rows[None], (32, 4, D)), group, 0, 0, tiled=True)
    half = half.reshape(IMAGES // 2, D)
    rest = lax.ppermute(half, "co", swap)
    pooled = jnp.where(co == 0, jnp.stack([half, rest]), jnp.stack([rest, half]))
    pooled = pooled.reshape(1, IMAGES, D).astype(jnp.float32)

    limit = jnp.where(end[WIN - 1] == WIN, WIN, start[WIN - 1]) - LOCAL
    here = jnp.arange(LOCAL, dtype=jnp.int32)[:, None] < limit
    hidden = jnp.where(here, hown, back)[None]
    return hidden, pooled


def solution(mesh):
    fine = Mesh(mesh.devices.reshape(4, 2, 4, 2, 2), ALL_AXES)
    in_specs = (P("dp", TOKEN_AXES, None), P("dp", None), P(), P("dp", None), P("dp", None))
    out_specs = (P("dp", TOKEN_AXES, None), P("dp", None, None))
    return jax.shard_map(layer, mesh=fine, in_specs=in_specs, out_specs=out_specs, check_vma=False)
```

```python
import functools
import itertools

import jax
import jax.numpy as jnp
from jax import lax
from jax.experimental import pallas as pl
from jax.experimental.pallas import tpu as pltpu
from jax.sharding import Mesh
from jax.sharding import PartitionSpec as P


HEADS = 16
SIZE = 80
VROWS = 96
D = HEADS * SIZE
LOCAL = 512
WIN = 2 * LOCAL
QB = 256
IMAGES = 256
EDGE_WIDTHS = (256, 384, 512, 640)
OWN_WIDTHS = (256, 384, 512)
HALF = D // 2
KR = 160
TOKEN_AXES = ("x", "co", "z", "yh")
ALL_AXES = TOKEN_AXES + ("dp",)
LOG2E = 1.4426950408889634


def permutation(move):
    def index(x, co, z, y):
        return ((x * 2 + co) * 8 + (z * 2 + y // 2)) * 2 + y % 2

    places = itertools.product(range(4), range(2), range(4), range(4))
    return [(index(*place), index(*move(*place))) for place in places]


Y_UP = permutation(lambda x, co, z, y: (x, co, z, (y + 1) % 4))
Y_DOWN = permutation(lambda x, co, z, y: (x, co, z, (y - 1) % 4))
X_UP = permutation(lambda x, co, z, y: ((x + 1) % 4, co, z, y))
X_DOWN = permutation(lambda x, co, z, y: ((x - 1) % 4, co, z, y))
Z_UP = permutation(lambda x, co, z, y: (x, co, (z + 1) % 4, y))
Z_DOWN = permutation(lambda x, co, z, y: (x, co, (z - 1) % 4, y))
CORE = permutation(lambda x, co, z, y: (x, 1 - co, z, y))


WRAPS = [i for i in range(63) if i % 16 == 15]


def moved(piece, pairs):
    return lax.ppermute(piece, ALL_AXES, pairs)


def first_pieces(w_qkv, w_out):
    x, co = lax.axis_index("x"), lax.axis_index("co")
    pieces = []
    for side in range(2):
        part = co * 2 + side
        q = lax.dynamic_slice(w_qkv, (x * KR, jnp.minimum(part, 2) * D), (KR, D))
        o = lax.dynamic_slice(w_out, (x * KR, 0), (KR, D))
        pieces.append(q if side == 0 else jnp.where(co == 0, q, o))
    return pieces


def attention_kernel(edge, place_ref, ends_ref, *refs):
    widths = EDGE_WIDTHS if edge else OWN_WIDTHS
    window = WIN if edge else LOCAL
    if edge:
        prev_ref, late_ref, refs = refs[0], refs[1], refs[2:]
    own_ref, gain_ref, wqkv_ref, wout_ref, refs = *refs[:4], refs[4:]
    mine_refs, other_refs, spans_ref, refs = refs[:8], refs[8:16], refs[16], refs[17:]
    if edge:
        hprev_ref, hown_ref, sum_ref, refs = *refs[:3], refs[3:]
    else:
        image_ref, lens_ref, hedge_ref, sum_ref, hown_ref, pooled_ref, refs = *refs[:6], refs[6:]
    (
        x_ref, n_ref, w_ref, wo_ref, q_ref, k_ref, vt_ref, ctx_ref, bias_ref, hid_ref,
        s0_ref, s1_ref, p0_ref, p1_ref, top0_ref, top1_ref, sem,
    ) = refs
    x, co, dp, lo, hi, wrap = (place_ref[i] for i in range(6))
    base = (lo // 128) * 128
    blocks = (hi - base + QB - 1) // QB

    far = (1 - dp) * HALF

    inputs = [pltpu.make_async_copy(own_ref, x_ref.at[pl.ds(window - LOCAL, LOCAL)], sem.at[0])]
    inputs[0].start()
    if edge:
        inputs.append(pltpu.make_async_copy(prev_ref, x_ref.at[pl.ds(0, LOCAL)], sem.at[0]))

        @pl.when(wrap == 0)
        def _():
            inputs[1].start()

        @pl.when(wrap == 1)
        def _():
            pltpu.make_async_copy(late_ref, x_ref.at[pl.ds(0, LOCAL)], sem.at[0]).start()
    else:
        inputs.append(pltpu.make_async_copy(hedge_ref, hid_ref.at[pl.ds(0, LOCAL)], sem.at[5]))
        inputs[1].start()

    def near(part, target, cols):
        return pltpu.make_async_copy(
            wout_ref if part == 3 else wqkv_ref.at[:, cols],
            target.at[pl.ds(pl.multiple_of(dp * HALF, 16), HALF), cols],
            sem.at[1 + part],
        )

    def distant(part, source, row):
        target = wo_ref if part == 3 else w_ref
        rows = pl.ds(pl.multiple_of(far + row * KR, 16), KR)
        return pltpu.make_async_copy(source, target.at[rows, columns[part]], sem.at[1 + part])

    columns = [pl.ds(0, D), pl.ds(D, D), pl.ds(2 * D, D), pl.ds(0, D)]
    targets = [w_ref, w_ref, w_ref, wo_ref]
    shift = (0, 3, 1, 2)
    for part in range(4):
        near(part, targets[part], columns[part]).start()
        for held, core in ((mine_refs, co), (other_refs, 1 - co)):

            @pl.when(core == part // 2)
            def _(held=held, part=part):
                for slot in range(4):
                    row = lax.rem(x + shift[slot], 4)
                    distant(part, held[slot * 2 + part % 2], row).start()

    def arrived(part):
        near(part, targets[part], columns[part]).wait()
        for _ in range(4):
            distant(part, mine_refs[0], 0).wait()

    x_ref[window:, :] = jnp.zeros((x_ref.shape[0] - window, D), jnp.bfloat16)
    for copy in inputs:
        copy.wait()

    def block_rows(j):
        row0 = pl.multiple_of(base + j * QB, 128)
        return row0, pl.ds(row0, QB)

    def normalize(j, carry):
        _, rows = block_rows(j)
        values = x_ref[rows, :].astype(jnp.float32)
        center = values - jnp.mean(values, axis=1, keepdims=True)
        spread = jnp.mean(center * center, axis=1, keepdims=True)
        normed = center * lax.rsqrt(spread + 1e-05) * gain_ref[...]
        n_ref[rows, :] = normed.astype(jnp.bfloat16)
        return carry

    lax.fori_loop(0, blocks, normalize, 0)
    k_ref[...] = jnp.zeros_like(k_ref)
    vt_ref[...] = jnp.zeros_like(vt_ref)
    if edge:
        hid_ref[...] = jnp.zeros_like(hid_ref)

    def project_q(j, carry):
        _, rows = block_rows(j)
        q = jnp.dot(n_ref[rows, :], w_ref[:, 0:D], preferred_element_type=jnp.float32)
        q_ref[rows, :] = (q * (LOG2E * SIZE**-0.5)).astype(jnp.bfloat16)
        return carry

    def project_k(j, carry):
        _, rows = block_rows(j)
        k = jnp.dot(n_ref[rows, :], w_ref[:, D : 2 * D], preferred_element_type=jnp.float32)
        k_ref[rows, :] = k.astype(jnp.bfloat16)
        return carry

    def project_v(j, carry):
        _, rows = block_rows(j)
        v = jnp.dot(n_ref[rows, :], w_ref[:, 2 * D :], preferred_element_type=jnp.float32)
        vt = v.T.astype(jnp.bfloat16)
        for h in range(HEADS):
            vt_ref[pl.ds(h * VROWS, SIZE), rows] = vt[h * SIZE : (h + 1) * SIZE]
            vt_ref[pl.ds(h * VROWS + SIZE, VROWS - SIZE), rows] = jnp.ones(
                (VROWS - SIZE, QB), jnp.bfloat16
            )
        return carry

    for part, project in enumerate((project_q, project_k, project_v)):
        arrived(part)
        lax.fori_loop(0, blocks, project, 0)
    arrived(3)

    def attend(j, carry):
        row0, rows = block_rows(j)
        least = ends_ref[0, jnp.maximum(row0, lo)]
        most = ends_ref[1, jnp.minimum(row0 + QB, hi) - 1]
        k0 = pl.multiple_of((least // 128) * 128, 128)
        need = most - k0
        start = spans_ref[0:1, rows]
        end = spans_ref[1:2, rows]
        for i, width in enumerate(widths):
            above = widths[i - 1] if i else 0

            @pl.when((need > above) & (need <= width))
            def _(width=width):
                keys = pl.ds(k0, width)
                at = lax.broadcasted_iota(jnp.int32, (width, QB), 0) + k0
                bias_ref[0:width, :] = jnp.where((at >= start) & (at < end), 0.0, -1e30)

                def scores(h, s_ref, top_ref):
                    w0 = pl.multiple_of(jnp.minimum((h * SIZE) // 128 * 128, D - 256), 128)
                    lanes = pl.ds(w0, 256)
                    lane = lax.broadcasted_iota(jnp.int32, (1, 256), 1) + (w0 - h * SIZE)
                    inside = jnp.where((lane >= 0) & (lane < SIZE), 1.0, 0.0)
                    q = q_ref[rows, lanes] * inside.astype(jnp.bfloat16)
                    s = lax.dot_general(
                        k_ref[keys, lanes], q, (((1,), (1,)), ((), ())),
                        preferred_element_type=jnp.float32,
                    )
                    s = s + bias_ref[0:width, :]
                    s_ref[0:width, :] = s
                    top_ref[...] = jnp.max(s, axis=0, keepdims=True)

                def weights(s_ref, top_ref, p_ref):
                    p_ref[0:width, :] = jnp.exp2(s_ref[0:width, :] - top_ref[...]).astype(
                        jnp.bfloat16
                    )

                def mix(h, p_ref):
                    features = pl.ds(pl.multiple_of(h * VROWS, 16), VROWS)
                    c = jnp.dot(
                        vt_ref[features, keys], p_ref[0:width, :],
                        preferred_element_type=jnp.float32,
                    )
                    ctx_ref[pl.ds(pl.multiple_of(h * SIZE, 16), SIZE), :] = (
                        c[0:SIZE] * (1.0 / c[SIZE : SIZE + 1])
                    ).astype(jnp.bfloat16)

                scores(0, s0_ref, top0_ref)

                def two_heads(i, inner):
                    h = i * 2
                    scores(h + 1, s1_ref, top1_ref)
                    weights(s0_ref, top0_ref, p0_ref)
                    mix(jnp.maximum(h - 1, 0), p1_ref)
                    scores(jnp.minimum(h + 2, HEADS - 1), s0_ref, top0_ref)
                    weights(s1_ref, top1_ref, p1_ref)
                    mix(h, p0_ref)
                    return inner

                lax.fori_loop(0, HEADS // 2, two_heads, 0)
                mix(HEADS - 1, p1_ref)

        mixed = lax.dot_general(
            ctx_ref[...], wo_ref[...], (((0,), (0,)), ((), ())),
            preferred_element_type=jnp.float32,
        )
        hidden = x_ref[rows, :].astype(jnp.float32) + mixed
        at = lax.broadcasted_iota(jnp.int32, (QB, D), 0) + row0
        inside = (at >= lo) & (at < hi)
        hidden = hidden.astype(jnp.bfloat16)
        if edge:
            hid_ref[rows, :] = jnp.where(inside, hidden, jnp.zeros_like(hidden))
        else:
            hid_ref[rows, :] = jnp.where(inside, hidden, hid_ref[rows, :])
        return carry

    lax.fori_loop(0, blocks, attend, 0)

    if edge:
        hprev_ref[...] = hid_ref[0:LOCAL, :]
        hown_ref[...] = hid_ref[LOCAL:WIN, :]
        sum_ref[...] = jnp.dot(
            jnp.ones((8, WIN), jnp.bfloat16), hid_ref[0:WIN, :], preferred_element_type=jnp.float32
        )
        return
    hown_ref[...] = hid_ref[0:LOCAL, :]
    label = lax.broadcasted_iota(jnp.int32, (IMAGES, LOCAL), 0)
    at = lax.broadcasted_iota(jnp.int32, (IMAGES, LOCAL), 1)
    member = (label == image_ref[...]) & (at >= lo) & (at < hi)
    sums = jnp.dot(
        jnp.where(member, 1.0, 0.0).astype(jnp.bfloat16), hid_ref[0:LOCAL, :],
        preferred_element_type=jnp.float32,
    )
    label = lax.broadcasted_iota(jnp.int32, (IMAGES, D), 0)
    sums = sums + jnp.where(label == place_ref[6], sum_ref[0:1, :], 0.0)
    pooled_ref[...] = (sums / lens_ref[...]).astype(jnp.bfloat16)


def attention(edge, place, spans, inputs, gain, weights, extra):
    hbm = pl.BlockSpec(memory_space=pltpu.HBM)
    vmem = pl.BlockSpec(memory_space=pltpu.VMEM)
    smem = pl.BlockSpec(memory_space=pltpu.SMEM)
    rows = WIN + 256 if edge else LOCAL + 256
    width = (EDGE_WIDTHS if edge else OWN_WIDTHS)[-1]
    hidden = jax.ShapeDtypeStruct((LOCAL, D), jnp.bfloat16)
    if edge:
        outs = (hidden, hidden, jax.ShapeDtypeStruct((8, D), jnp.float32))
        tail = []
    else:
        outs = (hidden, jax.ShapeDtypeStruct((IMAGES, D), jnp.bfloat16))
        tail = [vmem, vmem, hbm, vmem]
    return pl.pallas_call(
        functools.partial(attention_kernel, edge),
        out_shape=outs,
        in_specs=[smem, smem] + [hbm] * len(inputs) + [vmem] + [hbm] * 18 + [vmem] + tail,
        out_specs=(vmem,) * len(outs),
        scratch_shapes=[
            pltpu.VMEM((rows, D), jnp.bfloat16),
            pltpu.VMEM((rows, D), jnp.bfloat16),
            pltpu.VMEM((D, 3 * D), jnp.bfloat16),
            pltpu.VMEM((D, D), jnp.bfloat16),
            pltpu.VMEM((rows, D), jnp.bfloat16),
            pltpu.VMEM((rows, D), jnp.bfloat16),
            pltpu.VMEM((HEADS * VROWS, rows), jnp.bfloat16),
            pltpu.VMEM((D, QB), jnp.bfloat16),
            pltpu.VMEM((width, QB), jnp.float32),
            pltpu.VMEM((rows, D), jnp.bfloat16),
            pltpu.VMEM((width, QB), jnp.float32),
            pltpu.VMEM((width, QB), jnp.float32),
            pltpu.VMEM((width, QB), jnp.bfloat16),
            pltpu.VMEM((width, QB), jnp.bfloat16),
            pltpu.VMEM((1, QB), jnp.float32),
            pltpu.VMEM((1, QB), jnp.float32),
            pltpu.SemaphoreType.DMA((6,)),
        ],
        compiler_params=pltpu.CompilerParams(vmem_limit_bytes=50 * 2**20),
        cost_estimate=pl.CostEstimate(
            flops=15_000_000_000, bytes_accessed=20_000_000, transcendentals=5_000_000
        ),
        name="edge_attention" if edge else "own_attention",
    )(place, spans, *inputs, gain, *weights, spans, *extra)


def layer(tokens, lengths, ln_gain, w_qkv, w_out):
    x, co, z, yh, dp = (lax.axis_index(a) for a in ALL_AXES)
    shard = (x * 2 + co) * 8 + z * 2 + yh
    own = tokens[0]

    p0, p1 = first_pieces(w_qkv, w_out)
    lent = lax.ppermute(own, TOKEN_AXES, [(i, i + 8) for i in WRAPS])
    r0 = moved(p0, Y_UP)
    r1 = moved(p1, Y_DOWN)
    prev = lax.ppermute(own, TOKEN_AXES, [(i, i + 1) for i in range(63) if i not in WRAPS])
    u0 = moved(r0, X_UP)
    d1 = moved(r1, X_DOWN)
    late = lax.ppermute(lent, TOKEN_AXES, [(i + 8, i + 1) for i in WRAPS])
    u1 = moved(r1, X_UP)
    d0 = moved(r0, X_DOWN)
    f0 = moved(u0, X_UP)
    f1 = moved(d1, X_DOWN)
    near = [moved(a, CORE) for a in (r0, r1)]
    ring = [moved(a, CORE) for a in (u0, u1, d0, d1)]
    last = [moved(a, CORE) for a in (f0, f1)]
    mine = [r0, r1, u0, u1, d0, d1, f0, f1]
    other = near + ring + last

    lens = lengths[0]
    ends = jnp.cumsum(lens)
    offsets = ends - lens
    first = (shard - 1) * LOCAL
    at = first + jnp.arange(WIN + 256, dtype=jnp.int32)
    begun = offsets[:, None] <= at[None, :]
    image = jnp.sum(begun.astype(jnp.int32), axis=0) - 1
    start = jnp.max(jnp.where(begun, offsets[:, None], -WIN), axis=0) - first
    end = jnp.min(jnp.where(ends[:, None] > at[None, :], ends[:, None], 1 << 20), axis=0) - first
    spans = jnp.stack([start, end]).astype(jnp.int32)
    low = start[LOCAL]
    cut = jnp.where(low < LOCAL, end[LOCAL], LOCAL)
    limit = jnp.where(end[WIN - 1] == WIN, WIN, start[WIN - 1])
    wrap = (co + z + yh == 0) & (x > 0)
    places = [
        jnp.stack([x, co, dp, lo, hi, wrap, image[LOCAL]]).astype(jnp.int32)
        for lo, hi in ((low, cut), (cut - LOCAL, limit - LOCAL))
    ]
    gain = ln_gain[None]
    weights = [w_qkv, w_out, *mine, *other]

    hprev, hedge, total = attention(True, places[0], spans, [prev, late, own], gain, weights, [])
    back = lax.ppermute(hprev, TOKEN_AXES, [(i + 1, i) for i in range(63)])
    hown, part = attention(
        False, places[1], spans[:, LOCAL:] - LOCAL, [own], gain, weights,
        [image[None, LOCAL:WIN], lens.astype(jnp.float32)[:, None], hedge, total],
    )

    swap = [(0, 1), (1, 0)]
    group = ("x", "z", "yh")
    part = part.reshape(2, IMAGES // 2, D)
    kept = lax.dynamic_index_in_dim(part, co, 0, keepdims=False)
    given = lax.dynamic_index_in_dim(part, 1 - co, 0, keepdims=False)
    given = lax.ppermute(given, "co", swap)
    kept = kept.astype(jnp.float32) + given.astype(jnp.float32)
    kept = kept.astype(jnp.bfloat16).reshape(32, 4, D)
    rows = lax.all_to_all(kept, group, 0, 0, tiled=True).astype(jnp.float32)
    rows = jnp.sum(rows, axis=0).astype(jnp.bfloat16)
    half = lax.all_to_all(jnp.broadcast_to(rows[None], (32, 4, D)), group, 0, 0, tiled=True)
    half = half.reshape(IMAGES // 2, D)
    rest = lax.ppermute(half, "co", swap)
    pooled = jnp.where(co == 0, jnp.stack([half, rest]), jnp.stack([rest, half]))
    pooled = pooled.reshape(1, IMAGES, D).astype(jnp.float32)

    here = jnp.arange(LOCAL, dtype=jnp.int32)[:, None] < limit - LOCAL
    hidden = jnp.where(here, hown, back)[None]
    return hidden, pooled


def solution(mesh):
    fine = Mesh(mesh.devices.reshape(4, 2, 4, 2, 2), ALL_AXES)
    in_specs = (P("dp", TOKEN_AXES, None), P("dp", None), P(), P("dp", None), P("dp", None))
    out_specs = (P("dp", TOKEN_AXES, None), P("dp", None, None))
    return jax.shard_map(layer, mesh=fine, in_specs=in_specs, out_specs=out_specs, check_vma=False)
```

```python
import functools
import itertools

import jax
import jax.numpy as jnp
from jax import lax
from jax.experimental import pallas as pl
from jax.experimental.pallas import tpu as pltpu
from jax.sharding import Mesh
from jax.sharding import PartitionSpec as P


HEADS = 16
SIZE = 80
VROWS = 96
D = HEADS * SIZE
LOCAL = 512
WIN = 2 * LOCAL
QB = 256
IMAGES = 256
WIDTHS = (256, 384, 512)
SHIFT = 16
HALF = D // 2
KR = 160
TOKEN_AXES = ("x", "co", "z", "yh")
ALL_AXES = TOKEN_AXES + ("dp",)
LOG2E = 1.4426950408889634


def permutation(move):
    def index(x, co, z, y):
        return ((x * 2 + co) * 8 + (z * 2 + y // 2)) * 2 + y % 2

    places = itertools.product(range(4), range(2), range(4), range(4))
    return [(index(*place), index(*move(*place))) for place in places]


Y_UP = permutation(lambda x, co, z, y: (x, co, z, (y + 1) % 4))
Y_DOWN = permutation(lambda x, co, z, y: (x, co, z, (y - 1) % 4))
X_UP = permutation(lambda x, co, z, y: ((x + 1) % 4, co, z, y))
X_DOWN = permutation(lambda x, co, z, y: ((x - 1) % 4, co, z, y))
Z_UP = permutation(lambda x, co, z, y: (x, co, (z + 1) % 4, y))
Z_DOWN = permutation(lambda x, co, z, y: (x, co, (z - 1) % 4, y))
CORE = permutation(lambda x, co, z, y: (x, 1 - co, z, y))


WRAPS = [i for i in range(63) if i % 16 == 15]


def moved(piece, pairs):
    return lax.ppermute(piece, ALL_AXES, pairs)


def first_pieces(w_qkv, w_out):
    x, co = lax.axis_index("x"), lax.axis_index("co")
    pieces = []
    for side in range(2):
        part = co * 2 + side
        q = lax.dynamic_slice(w_qkv, (x * KR, jnp.minimum(part, 2) * D), (KR, D))
        o = lax.dynamic_slice(w_out, (x * KR, 0), (KR, D))
        pieces.append(q if side == 0 else jnp.where(co == 0, q, o))
    return pieces


def attention_kernel(edge, place_ref, ends_ref, *refs):
    if edge:
        prev_ref, late_ref, refs = refs[0], refs[1], refs[2:]
    own_ref, gain_ref, wqkv_ref, wout_ref, refs = *refs[:4], refs[4:]
    mine_refs, other_refs, spans_ref, refs = refs[:8], refs[8:16], refs[16], refs[17:]
    if edge:
        hprev_ref, hown_ref, sum_ref, refs = *refs[:3], refs[3:]
    else:
        image_ref, lens_ref, hedge_ref, sum_ref, hown_ref, pooled_ref, refs = *refs[:6], refs[6:]
    if edge:
        wide_ref, refs = refs[0], refs[1:]
    (
        x_ref, n_ref, w_ref, wo_ref, q_ref, k_ref, vt_ref, ctx_ref, bias_ref, hid_ref,
        s0_ref, s1_ref, p0_ref, p1_ref, top0_ref, top1_ref, sem,
    ) = refs
    x, co, dp, lo, hi, wrap = (place_ref[i] for i in range(6))
    if edge:
        first = pl.multiple_of(lo // SHIFT * SHIFT, SHIFT)
        offset = lo - first
        base, lo, hi = 0, 0, hi - lo
    else:
        base = (lo // 128) * 128
    blocks = (hi - base + QB - 1) // QB

    far = (1 - dp) * HALF

    tokens_ref = wide_ref if edge else x_ref
    inputs = [
        pltpu.make_async_copy(
            own_ref, tokens_ref.at[pl.ds(LOCAL if edge else 0, LOCAL)], sem.at[0]
        )
    ]
    inputs[0].start()
    if edge:
        inputs.append(pltpu.make_async_copy(prev_ref, wide_ref.at[pl.ds(0, LOCAL)], sem.at[0]))

        @pl.when(wrap == 0)
        def _():
            inputs[1].start()

        @pl.when(wrap == 1)
        def _():
            pltpu.make_async_copy(late_ref, wide_ref.at[pl.ds(0, LOCAL)], sem.at[0]).start()
    else:
        inputs.append(pltpu.make_async_copy(hedge_ref, hid_ref.at[pl.ds(0, LOCAL)], sem.at[5]))
        inputs[1].start()

    def near(part, target, cols):
        return pltpu.make_async_copy(
            wout_ref if part == 3 else wqkv_ref.at[:, cols],
            target.at[pl.ds(pl.multiple_of(dp * HALF, 16), HALF), cols],
            sem.at[1 + part],
        )

    def distant(part, source, row):
        target = wo_ref if part == 3 else w_ref
        rows = pl.ds(pl.multiple_of(far + row * KR, 16), KR)
        return pltpu.make_async_copy(source, target.at[rows, columns[part]], sem.at[1 + part])

    columns = [pl.ds(0, D), pl.ds(D, D), pl.ds(2 * D, D), pl.ds(0, D)]
    targets = [w_ref, w_ref, w_ref, wo_ref]
    shift = (0, 3, 1, 2)
    for part in range(4):
        near(part, targets[part], columns[part]).start()
        for held, core in ((mine_refs, co), (other_refs, 1 - co)):

            @pl.when(core == part // 2)
            def _(held=held, part=part):
                for slot in range(4):
                    row = lax.rem(x + shift[slot], 4)
                    distant(part, held[slot * 2 + part % 2], row).start()

    def arrived(part):
        near(part, targets[part], columns[part]).wait()
        for _ in range(4):
            distant(part, mine_refs[0], 0).wait()

    if not edge:
        x_ref[LOCAL:, :] = jnp.zeros((x_ref.shape[0] - LOCAL, D), jnp.bfloat16)
    for copy in inputs:
        copy.wait()

    def mover(lag):
        out = lax.broadcasted_iota(jnp.int32, (QB, QB + SHIFT), 0)
        source = lax.broadcasted_iota(jnp.int32, (QB, QB + SHIFT), 1)
        return jnp.where(source == out + lag, 1.0, 0.0).astype(jnp.bfloat16)

    if edge:
        wide_ref[WIN:, :] = jnp.zeros((wide_ref.shape[0] - WIN, D), jnp.bfloat16)
        pick = mover(offset)

        def align(j, carry):
            rows = pl.ds(pl.multiple_of(first + j * QB, SHIFT), QB + SHIFT)
            taken = jnp.dot(pick, wide_ref[rows, :], preferred_element_type=jnp.float32)
            x_ref[pl.ds(pl.multiple_of(j * QB, QB), QB), :] = taken.astype(jnp.bfloat16)
            return carry

        lax.fori_loop(0, blocks, align, 0)

    def block_rows(j):
        row0 = pl.multiple_of(base + j * QB, 128)
        return row0, pl.ds(row0, QB)

    def normalize(j, carry):
        _, rows = block_rows(j)
        values = x_ref[rows, :].astype(jnp.float32)
        center = values - jnp.mean(values, axis=1, keepdims=True)
        spread = jnp.mean(center * center, axis=1, keepdims=True)
        normed = center * lax.rsqrt(spread + 1e-05) * gain_ref[...]
        n_ref[rows, :] = normed.astype(jnp.bfloat16)
        return carry

    lax.fori_loop(0, blocks, normalize, 0)
    k_ref[...] = jnp.zeros_like(k_ref)
    vt_ref[...] = jnp.zeros_like(vt_ref)
    if edge:
        hid_ref[...] = jnp.zeros_like(hid_ref)
        wide_ref[...] = jnp.zeros_like(wide_ref)

    def project_q(j, carry):
        _, rows = block_rows(j)
        q = jnp.dot(n_ref[rows, :], w_ref[:, 0:D], preferred_element_type=jnp.float32)
        q_ref[rows, :] = (q * (LOG2E * SIZE**-0.5)).astype(jnp.bfloat16)
        return carry

    def project_k(j, carry):
        _, rows = block_rows(j)
        k = jnp.dot(n_ref[rows, :], w_ref[:, D : 2 * D], preferred_element_type=jnp.float32)
        k_ref[rows, :] = k.astype(jnp.bfloat16)
        return carry

    def project_v(j, carry):
        _, rows = block_rows(j)
        v = jnp.dot(n_ref[rows, :], w_ref[:, 2 * D :], preferred_element_type=jnp.float32)
        vt = v.T.astype(jnp.bfloat16)
        for h in range(HEADS):
            vt_ref[pl.ds(h * VROWS, SIZE), rows] = vt[h * SIZE : (h + 1) * SIZE]
            vt_ref[pl.ds(h * VROWS + SIZE, VROWS - SIZE), rows] = jnp.ones(
                (VROWS - SIZE, QB), jnp.bfloat16
            )
        return carry

    for part, project in enumerate((project_q, project_k, project_v)):
        arrived(part)
        lax.fori_loop(0, blocks, project, 0)
    arrived(3)

    def attend(j, carry):
        row0, rows = block_rows(j)
        if edge:
            k0, need = 0, hi
            start, end = 0, hi
        else:
            least = ends_ref[0, jnp.maximum(row0, lo)]
            most = ends_ref[1, jnp.minimum(row0 + QB, hi) - 1]
            k0 = pl.multiple_of((least // 128) * 128, 128)
            need = most - k0
            start = spans_ref[0:1, rows]
            end = spans_ref[1:2, rows]
        for i, width in enumerate(WIDTHS):
            above = WIDTHS[i - 1] if i else 0

            @pl.when((need > above) & (need <= width))
            def _(width=width):
                keys = pl.ds(k0, width)
                at = lax.broadcasted_iota(jnp.int32, (width, QB), 0) + k0
                bias_ref[0:width, :] = jnp.where((at >= start) & (at < end), 0.0, -1e30)

                def scores(h, s_ref, top_ref):
                    w0 = pl.multiple_of(jnp.minimum((h * SIZE) // 128 * 128, D - 256), 128)
                    lanes = pl.ds(w0, 256)
                    lane = lax.broadcasted_iota(jnp.int32, (1, 256), 1) + (w0 - h * SIZE)
                    inside = jnp.where((lane >= 0) & (lane < SIZE), 1.0, 0.0)
                    q = q_ref[rows, lanes] * inside.astype(jnp.bfloat16)
                    s = lax.dot_general(
                        k_ref[keys, lanes], q, (((1,), (1,)), ((), ())),
                        preferred_element_type=jnp.float32,
                    )
                    s = s + bias_ref[0:width, :]
                    s_ref[0:width, :] = s
                    top_ref[...] = jnp.max(s, axis=0, keepdims=True)

                def weights(s_ref, top_ref, p_ref):
                    p_ref[0:width, :] = jnp.exp2(s_ref[0:width, :] - top_ref[...]).astype(
                        jnp.bfloat16
                    )

                def mix(h, p_ref):
                    features = pl.ds(pl.multiple_of(h * VROWS, 16), VROWS)
                    c = jnp.dot(
                        vt_ref[features, keys], p_ref[0:width, :],
                        preferred_element_type=jnp.float32,
                    )
                    ctx_ref[pl.ds(pl.multiple_of(h * SIZE, 16), SIZE), :] = (
                        c[0:SIZE] * (1.0 / c[SIZE : SIZE + 1])
                    ).astype(jnp.bfloat16)

                scores(0, s0_ref, top0_ref)

                def two_heads(i, inner):
                    h = i * 2
                    scores(h + 1, s1_ref, top1_ref)
                    weights(s0_ref, top0_ref, p0_ref)
                    mix(jnp.maximum(h - 1, 0), p1_ref)
                    scores(jnp.minimum(h + 2, HEADS - 1), s0_ref, top0_ref)
                    weights(s1_ref, top1_ref, p1_ref)
                    mix(h, p0_ref)
                    return inner

                lax.fori_loop(0, HEADS // 2, two_heads, 0)
                mix(HEADS - 1, p1_ref)

        mixed = lax.dot_general(
            ctx_ref[...], wo_ref[...], (((0,), (0,)), ((), ())),
            preferred_element_type=jnp.float32,
        )
        hidden = x_ref[rows, :].astype(jnp.float32) + mixed
        at = lax.broadcasted_iota(jnp.int32, (QB, D), 0) + row0
        inside = (at >= lo) & (at < hi)
        hidden = hidden.astype(jnp.bfloat16)
        if edge:
            hid_ref[pl.ds(pl.multiple_of(row0 + SHIFT, SHIFT), QB), :] = jnp.where(
                inside, hidden, jnp.zeros_like(hidden)
            )
        else:
            hid_ref[rows, :] = jnp.where(inside, hidden, hid_ref[rows, :])
        return carry

    lax.fori_loop(0, blocks, attend, 0)

    if edge:
        put = mover(SHIFT - offset)

        @pl.when(hi > 0)
        def _():
            for j in range(3):
                moved_rows = jnp.dot(
                    put, hid_ref[j * QB : (j + 1) * QB + SHIFT, :],
                    preferred_element_type=jnp.float32,
                )
                rows = pl.ds(pl.multiple_of(first + j * QB, SHIFT), QB)
                wide_ref[rows, :] = moved_rows.astype(jnp.bfloat16)

        hprev_ref[...] = wide_ref[0:LOCAL, :]
        hown_ref[...] = wide_ref[LOCAL:WIN, :]
        sum_ref[...] = jnp.dot(
            jnp.ones((8, LOCAL + SHIFT), jnp.bfloat16), hid_ref[0 : LOCAL + SHIFT, :],
            preferred_element_type=jnp.float32,
        )
        return
    hown_ref[...] = hid_ref[0:LOCAL, :]
    label = lax.broadcasted_iota(jnp.int32, (IMAGES, LOCAL), 0)
    at = lax.broadcasted_iota(jnp.int32, (IMAGES, LOCAL), 1)
    member = (label == image_ref[...]) & (at >= lo) & (at < hi)
    sums = jnp.dot(
        jnp.where(member, 1.0, 0.0).astype(jnp.bfloat16), hid_ref[0:LOCAL, :],
        preferred_element_type=jnp.float32,
    )
    label = lax.broadcasted_iota(jnp.int32, (IMAGES, D), 0)
    sums = sums + jnp.where(label == place_ref[6], sum_ref[0:1, :], 0.0)
    pooled_ref[...] = (sums / lens_ref[...]).astype(jnp.bfloat16)


def attention(edge, place, spans, inputs, gain, weights, extra):
    hbm = pl.BlockSpec(memory_space=pltpu.HBM)
    vmem = pl.BlockSpec(memory_space=pltpu.VMEM)
    smem = pl.BlockSpec(memory_space=pltpu.SMEM)
    rows = LOCAL + 256
    width = WIDTHS[-1]
    hidden = jax.ShapeDtypeStruct((LOCAL, D), jnp.bfloat16)
    if edge:
        outs = (hidden, hidden, jax.ShapeDtypeStruct((8, D), jnp.float32))
        tail = []
    else:
        outs = (hidden, jax.ShapeDtypeStruct((IMAGES, D), jnp.bfloat16))
        tail = [vmem, vmem, hbm, vmem]
    return pl.pallas_call(
        functools.partial(attention_kernel, edge),
        out_shape=outs,
        in_specs=[smem, smem] + [hbm] * len(inputs) + [vmem] + [hbm] * 18 + [vmem] + tail,
        out_specs=(vmem,) * len(outs),
        scratch_shapes=([pltpu.VMEM((WIN + 3 * QB, D), jnp.bfloat16)] if edge else [])
        + [
            pltpu.VMEM((rows, D), jnp.bfloat16),
            pltpu.VMEM((rows, D), jnp.bfloat16),
            pltpu.VMEM((D, 3 * D), jnp.bfloat16),
            pltpu.VMEM((D, D), jnp.bfloat16),
            pltpu.VMEM((rows, D), jnp.bfloat16),
            pltpu.VMEM((rows, D), jnp.bfloat16),
            pltpu.VMEM((HEADS * VROWS, rows), jnp.bfloat16),
            pltpu.VMEM((D, QB), jnp.bfloat16),
            pltpu.VMEM((width, QB), jnp.float32),
            pltpu.VMEM((rows + 2 * SHIFT, D), jnp.bfloat16),
            pltpu.VMEM((width, QB), jnp.float32),
            pltpu.VMEM((width, QB), jnp.float32),
            pltpu.VMEM((width, QB), jnp.bfloat16),
            pltpu.VMEM((width, QB), jnp.bfloat16),
            pltpu.VMEM((1, QB), jnp.float32),
            pltpu.VMEM((1, QB), jnp.float32),
            pltpu.SemaphoreType.DMA((6,)),
        ],
        compiler_params=pltpu.CompilerParams(vmem_limit_bytes=50 * 2**20),
        cost_estimate=pl.CostEstimate(
            flops=15_000_000_000, bytes_accessed=20_000_000, transcendentals=5_000_000
        ),
        name="edge_attention" if edge else "own_attention",
    )(place, spans, *inputs, gain, *weights, spans, *extra)


def layer(tokens, lengths, ln_gain, w_qkv, w_out):
    x, co, z, yh, dp = (lax.axis_index(a) for a in ALL_AXES)
    shard = (x * 2 + co) * 8 + z * 2 + yh
    own = tokens[0]

    p0, p1 = first_pieces(w_qkv, w_out)
    lent = lax.ppermute(own, TOKEN_AXES, [(i, i + 8) for i in WRAPS])
    r0 = moved(p0, Y_UP)
    r1 = moved(p1, Y_DOWN)
    prev = lax.ppermute(own, TOKEN_AXES, [(i, i + 1) for i in range(63) if i not in WRAPS])
    u0 = moved(r0, X_UP)
    d1 = moved(r1, X_DOWN)
    late = lax.ppermute(lent, TOKEN_AXES, [(i + 8, i + 1) for i in WRAPS])
    u1 = moved(r1, X_UP)
    d0 = moved(r0, X_DOWN)
    f0 = moved(u0, X_UP)
    f1 = moved(d1, X_DOWN)
    near = [moved(a, CORE) for a in (r0, r1)]
    ring = [moved(a, CORE) for a in (u0, u1, d0, d1)]
    last = [moved(a, CORE) for a in (f0, f1)]
    mine = [r0, r1, u0, u1, d0, d1, f0, f1]
    other = near + ring + last

    lens = lengths[0]
    ends = jnp.cumsum(lens)
    offsets = ends - lens
    first = (shard - 1) * LOCAL
    at = first + jnp.arange(WIN + 256, dtype=jnp.int32)
    begun = offsets[:, None] <= at[None, :]
    image = jnp.sum(begun.astype(jnp.int32), axis=0) - 1
    start = jnp.max(jnp.where(begun, offsets[:, None], -WIN), axis=0) - first
    end = jnp.min(jnp.where(ends[:, None] > at[None, :], ends[:, None], 1 << 20), axis=0) - first
    spans = jnp.stack([start, end]).astype(jnp.int32)
    low = start[LOCAL]
    cut = jnp.where(low < LOCAL, end[LOCAL], LOCAL)
    limit = jnp.where(end[WIN - 1] == WIN, WIN, start[WIN - 1])
    wrap = (co + z + yh == 0) & (x > 0)
    places = [
        jnp.stack([x, co, dp, lo, hi, wrap, image[LOCAL]]).astype(jnp.int32)
        for lo, hi in ((low, cut), (cut - LOCAL, limit - LOCAL))
    ]
    gain = ln_gain[None]
    weights = [w_qkv, w_out, *mine, *other]

    hprev, hedge, total = attention(True, places[0], spans, [prev, late, own], gain, weights, [])
    back = lax.ppermute(hprev, TOKEN_AXES, [(i + 1, i) for i in range(63)])
    hown, part = attention(
        False, places[1], spans[:, LOCAL:] - LOCAL, [own], gain, weights,
        [image[None, LOCAL:WIN], lens.astype(jnp.float32)[:, None], hedge, total],
    )

    swap = [(0, 1), (1, 0)]
    group = ("x", "z", "yh")
    part = part.reshape(2, IMAGES // 2, D)
    kept = lax.dynamic_index_in_dim(part, co, 0, keepdims=False)
    given = lax.dynamic_index_in_dim(part, 1 - co, 0, keepdims=False)
    given = lax.ppermute(given, "co", swap)
    kept = kept.astype(jnp.float32) + given.astype(jnp.float32)
    kept = kept.astype(jnp.bfloat16).reshape(32, 4, D)
    rows = lax.all_to_all(kept, group, 0, 0, tiled=True).astype(jnp.float32)
    rows = jnp.sum(rows, axis=0).astype(jnp.bfloat16)
    half = lax.all_to_all(jnp.broadcast_to(rows[None], (32, 4, D)), group, 0, 0, tiled=True)
    half = half.reshape(IMAGES // 2, D)
    rest = lax.ppermute(half, "co", swap)
    pooled = jnp.where(co == 0, jnp.stack([half, rest]), jnp.stack([rest, half]))
    pooled = pooled.reshape(1, IMAGES, D).astype(jnp.float32)

    here = jnp.arange(LOCAL, dtype=jnp.int32)[:, None] < limit - LOCAL
    hidden = jnp.where(here, hown, back)[None]
    return hidden, pooled


def solution(mesh):
    fine = Mesh(mesh.devices.reshape(4, 2, 4, 2, 2), ALL_AXES)
    in_specs = (P("dp", TOKEN_AXES, None), P("dp", None), P(), P("dp", None), P("dp", None))
    out_specs = (P("dp", TOKEN_AXES, None), P("dp", None, None))
    return jax.shard_map(layer, mesh=fine, in_specs=in_specs, out_specs=out_specs, check_vma=False)
```

```python
import functools
import itertools

import jax
import jax.numpy as jnp
from jax import lax
from jax.experimental import pallas as pl
from jax.experimental.pallas import tpu as pltpu
from jax.sharding import Mesh
from jax.sharding import PartitionSpec as P


HEADS = 16
SIZE = 80
VROWS = 96
D = HEADS * SIZE
LOCAL = 512
WIN = 2 * LOCAL
QB = 256
IMAGES = 256
WIDTHS = (256, 384, 512)
SHIFT = 16
SLOTS = 16
HALF = D // 2
KR = 160
TOKEN_AXES = ("x", "co", "z", "yh")
ALL_AXES = TOKEN_AXES + ("dp",)
GROUP = ("x", "z", "yh")
SWAP = [(0, 1), (1, 0)]
LOG2E = 1.4426950408889634


def permutation(move):
    def index(x, co, z, y):
        return ((x * 2 + co) * 8 + (z * 2 + y // 2)) * 2 + y % 2

    places = itertools.product(range(4), range(2), range(4), range(4))
    return [(index(*place), index(*move(*place))) for place in places]


Y_UP = permutation(lambda x, co, z, y: (x, co, z, (y + 1) % 4))
Y_DOWN = permutation(lambda x, co, z, y: (x, co, z, (y - 1) % 4))
X_UP = permutation(lambda x, co, z, y: ((x + 1) % 4, co, z, y))
X_DOWN = permutation(lambda x, co, z, y: ((x - 1) % 4, co, z, y))
Z_UP = permutation(lambda x, co, z, y: (x, co, (z + 1) % 4, y))
Z_DOWN = permutation(lambda x, co, z, y: (x, co, (z - 1) % 4, y))
CORE = permutation(lambda x, co, z, y: (x, 1 - co, z, y))


WRAPS = [i for i in range(63) if i % 16 == 15]


def moved(piece, pairs):
    return lax.ppermute(piece, ALL_AXES, pairs)


def first_pieces(w_qkv, w_out):
    x, co = lax.axis_index("x"), lax.axis_index("co")
    pieces = []
    for side in range(2):
        part = co * 2 + side
        q = lax.dynamic_slice(w_qkv, (x * KR, jnp.minimum(part, 2) * D), (KR, D))
        o = lax.dynamic_slice(w_out, (x * KR, 0), (KR, D))
        pieces.append(q if side == 0 else jnp.where(co == 0, q, o))
    return pieces


def attention_kernel(edge, place_ref, ends_ref, *refs):
    if edge:
        prev_ref, late_ref, refs = refs[0], refs[1], refs[2:]
    own_ref, gain_ref, wqkv_ref, wout_ref, refs = *refs[:4], refs[4:]
    mine_refs, other_refs, spans_ref, refs = refs[:8], refs[8:16], refs[16], refs[17:]
    if edge:
        hprev_ref, hown_ref, sum_ref, refs = *refs[:3], refs[3:]
    else:
        image_ref, lens_ref, hedge_ref, sum_ref, hown_ref, pooled_ref, few_ref, refs = *refs[:7], refs[7:]
    if edge:
        wide_ref, refs = refs[0], refs[1:]
    (
        x_ref, n_ref, w_ref, wo_ref, q_ref, k_ref, vt_ref, ctx_ref, bias_ref, hid_ref,
        s0_ref, s1_ref, p0_ref, p1_ref, top0_ref, top1_ref, sem,
    ) = refs
    x, co, dp, lo, hi, wrap = (place_ref[i] for i in range(6))
    if edge:
        first = pl.multiple_of(lo // SHIFT * SHIFT, SHIFT)
        offset = lo - first
        base, lo, hi = 0, 0, hi - lo
    else:
        base = (lo // 128) * 128
    blocks = (hi - base + QB - 1) // QB

    far = (1 - dp) * HALF

    tokens_ref = wide_ref if edge else x_ref
    inputs = [
        pltpu.make_async_copy(
            own_ref, tokens_ref.at[pl.ds(LOCAL if edge else 0, LOCAL)], sem.at[0]
        )
    ]
    inputs[0].start()
    if edge:
        inputs.append(pltpu.make_async_copy(prev_ref, wide_ref.at[pl.ds(0, LOCAL)], sem.at[0]))

        @pl.when(wrap == 0)
        def _():
            inputs[1].start()

        @pl.when(wrap == 1)
        def _():
            pltpu.make_async_copy(late_ref, wide_ref.at[pl.ds(0, LOCAL)], sem.at[0]).start()
    else:
        inputs.append(pltpu.make_async_copy(hedge_ref, hid_ref.at[pl.ds(0, LOCAL)], sem.at[5]))
        inputs[1].start()

    def near(part, target, cols):
        return pltpu.make_async_copy(
            wout_ref if part == 3 else wqkv_ref.at[:, cols],
            target.at[pl.ds(pl.multiple_of(dp * HALF, 16), HALF), cols],
            sem.at[1 + part],
        )

    def distant(part, source, row):
        target = wo_ref if part == 3 else w_ref
        rows = pl.ds(pl.multiple_of(far + row * KR, 16), KR)
        return pltpu.make_async_copy(source, target.at[rows, columns[part]], sem.at[1 + part])

    columns = [pl.ds(0, D), pl.ds(D, D), pl.ds(2 * D, D), pl.ds(0, D)]
    targets = [w_ref, w_ref, w_ref, wo_ref]
    shift = (0, 3, 1, 2)
    for part in range(4):
        near(part, targets[part], columns[part]).start()
        for held, core in ((mine_refs, co), (other_refs, 1 - co)):

            @pl.when(core == part // 2)
            def _(held=held, part=part):
                for slot in range(4):
                    row = lax.rem(x + shift[slot], 4)
                    distant(part, held[slot * 2 + part % 2], row).start()

    def arrived(part):
        near(part, targets[part], columns[part]).wait()
        for _ in range(4):
            distant(part, mine_refs[0], 0).wait()

    if not edge:
        x_ref[LOCAL:, :] = jnp.zeros((x_ref.shape[0] - LOCAL, D), jnp.bfloat16)
    for copy in inputs:
        copy.wait()

    def mover(lag):
        out = lax.broadcasted_iota(jnp.int32, (QB, QB + SHIFT), 0)
        source = lax.broadcasted_iota(jnp.int32, (QB, QB + SHIFT), 1)
        return jnp.where(source == out + lag, 1.0, 0.0).astype(jnp.bfloat16)

    if edge:
        wide_ref[WIN:, :] = jnp.zeros((wide_ref.shape[0] - WIN, D), jnp.bfloat16)
        pick = mover(offset)

        def align(j, carry):
            rows = pl.ds(pl.multiple_of(first + j * QB, SHIFT), QB + SHIFT)
            taken = jnp.dot(pick, wide_ref[rows, :], preferred_element_type=jnp.float32)
            x_ref[pl.ds(pl.multiple_of(j * QB, QB), QB), :] = taken.astype(jnp.bfloat16)
            return carry

        lax.fori_loop(0, blocks, align, 0)

    def block_rows(j):
        row0 = pl.multiple_of(base + j * QB, 128)
        return row0, pl.ds(row0, QB)

    def normalize(j, carry):
        _, rows = block_rows(j)
        values = x_ref[rows, :].astype(jnp.float32)
        center = values - jnp.mean(values, axis=1, keepdims=True)
        spread = jnp.mean(center * center, axis=1, keepdims=True)
        normed = center * lax.rsqrt(spread + 1e-05) * gain_ref[...]
        n_ref[rows, :] = normed.astype(jnp.bfloat16)
        return carry

    lax.fori_loop(0, blocks, normalize, 0)
    k_ref[...] = jnp.zeros_like(k_ref)
    vt_ref[...] = jnp.zeros_like(vt_ref)
    if edge:
        hid_ref[...] = jnp.zeros_like(hid_ref)
        wide_ref[...] = jnp.zeros_like(wide_ref)

    def project_q(j, carry):
        _, rows = block_rows(j)
        q = jnp.dot(n_ref[rows, :], w_ref[:, 0:D], preferred_element_type=jnp.float32)
        q_ref[rows, :] = (q * (LOG2E * SIZE**-0.5)).astype(jnp.bfloat16)
        return carry

    def project_k(j, carry):
        _, rows = block_rows(j)
        k = jnp.dot(n_ref[rows, :], w_ref[:, D : 2 * D], preferred_element_type=jnp.float32)
        k_ref[rows, :] = k.astype(jnp.bfloat16)
        return carry

    def project_v(j, carry):
        _, rows = block_rows(j)
        v = jnp.dot(n_ref[rows, :], w_ref[:, 2 * D :], preferred_element_type=jnp.float32)
        vt = v.T.astype(jnp.bfloat16)
        for h in range(HEADS):
            vt_ref[pl.ds(h * VROWS, SIZE), rows] = vt[h * SIZE : (h + 1) * SIZE]
            vt_ref[pl.ds(h * VROWS + SIZE, VROWS - SIZE), rows] = jnp.ones(
                (VROWS - SIZE, QB), jnp.bfloat16
            )
        return carry

    for part, project in enumerate((project_q, project_k, project_v)):
        arrived(part)
        lax.fori_loop(0, blocks, project, 0)
    arrived(3)

    def attend(j, carry):
        row0, rows = block_rows(j)
        if edge:
            k0, need = 0, hi
            start, end = 0, hi
        else:
            least = ends_ref[0, jnp.maximum(row0, lo)]
            most = ends_ref[1, jnp.minimum(row0 + QB, hi) - 1]
            k0 = pl.multiple_of((least // 128) * 128, 128)
            need = most - k0
            start = spans_ref[0:1, rows]
            end = spans_ref[1:2, rows]
        for i, width in enumerate(WIDTHS):
            above = WIDTHS[i - 1] if i else 0

            @pl.when((need > above) & (need <= width))
            def _(width=width):
                keys = pl.ds(k0, width)
                at = lax.broadcasted_iota(jnp.int32, (width, QB), 0) + k0
                bias_ref[0:width, :] = jnp.where((at >= start) & (at < end), 0.0, -1e30)

                def scores(h, s_ref, top_ref):
                    w0 = pl.multiple_of(jnp.minimum((h * SIZE) // 128 * 128, D - 256), 128)
                    lanes = pl.ds(w0, 256)
                    lane = lax.broadcasted_iota(jnp.int32, (1, 256), 1) + (w0 - h * SIZE)
                    inside = jnp.where((lane >= 0) & (lane < SIZE), 1.0, 0.0)
                    q = q_ref[rows, lanes] * inside.astype(jnp.bfloat16)
                    s = lax.dot_general(
                        k_ref[keys, lanes], q, (((1,), (1,)), ((), ())),
                        preferred_element_type=jnp.float32,
                    )
                    s = s + bias_ref[0:width, :]
                    s_ref[0:width, :] = s
                    top_ref[...] = jnp.max(s, axis=0, keepdims=True)

                def weights(s_ref, top_ref, p_ref):
                    p_ref[0:width, :] = jnp.exp2(s_ref[0:width, :] - top_ref[...]).astype(
                        jnp.bfloat16
                    )

                def mix(h, p_ref):
                    features = pl.ds(pl.multiple_of(h * VROWS, 16), VROWS)
                    c = jnp.dot(
                        vt_ref[features, keys], p_ref[0:width, :],
                        preferred_element_type=jnp.float32,
                    )
                    ctx_ref[pl.ds(pl.multiple_of(h * SIZE, 16), SIZE), :] = (
                        c[0:SIZE] * (1.0 / c[SIZE : SIZE + 1])
                    ).astype(jnp.bfloat16)

                scores(0, s0_ref, top0_ref)

                def two_heads(i, inner):
                    h = i * 2
                    scores(h + 1, s1_ref, top1_ref)
                    weights(s0_ref, top0_ref, p0_ref)
                    mix(jnp.maximum(h - 1, 0), p1_ref)
                    scores(jnp.minimum(h + 2, HEADS - 1), s0_ref, top0_ref)
                    weights(s1_ref, top1_ref, p1_ref)
                    mix(h, p0_ref)
                    return inner

                lax.fori_loop(0, HEADS // 2, two_heads, 0)
                mix(HEADS - 1, p1_ref)

        mixed = lax.dot_general(
            ctx_ref[...], wo_ref[...], (((0,), (0,)), ((), ())),
            preferred_element_type=jnp.float32,
        )
        hidden = x_ref[rows, :].astype(jnp.float32) + mixed
        at = lax.broadcasted_iota(jnp.int32, (QB, D), 0) + row0
        inside = (at >= lo) & (at < hi)
        hidden = hidden.astype(jnp.bfloat16)
        if edge:
            hid_ref[pl.ds(pl.multiple_of(row0 + SHIFT, SHIFT), QB), :] = jnp.where(
                inside, hidden, jnp.zeros_like(hidden)
            )
        else:
            hid_ref[rows, :] = jnp.where(inside, hidden, hid_ref[rows, :])
        return carry

    lax.fori_loop(0, blocks, attend, 0)

    if edge:
        put = mover(SHIFT - offset)

        @pl.when(hi > 0)
        def _():
            for j in range(3):
                moved_rows = jnp.dot(
                    put, hid_ref[j * QB : (j + 1) * QB + SHIFT, :],
                    preferred_element_type=jnp.float32,
                )
                rows = pl.ds(pl.multiple_of(first + j * QB, SHIFT), QB)
                wide_ref[rows, :] = moved_rows.astype(jnp.bfloat16)

        hprev_ref[...] = wide_ref[0:LOCAL, :]
        hown_ref[...] = wide_ref[LOCAL:WIN, :]
        sum_ref[...] = jnp.dot(
            jnp.ones((8, LOCAL + SHIFT), jnp.bfloat16), hid_ref[0 : LOCAL + SHIFT, :],
            preferred_element_type=jnp.float32,
        )
        return
    hown_ref[...] = hid_ref[0:LOCAL, :]
    label = lax.broadcasted_iota(jnp.int32, (IMAGES, LOCAL), 0)
    at = lax.broadcasted_iota(jnp.int32, (IMAGES, LOCAL), 1)
    member = (label == image_ref[...]) & (at >= lo) & (at < hi)
    sums = jnp.dot(
        jnp.where(member, 1.0, 0.0).astype(jnp.bfloat16), hid_ref[0:LOCAL, :],
        preferred_element_type=jnp.float32,
    )
    label = lax.broadcasted_iota(jnp.int32, (IMAGES, D), 0)
    sums = sums + jnp.where(label == place_ref[6], sum_ref[0:1, :], 0.0)
    pooled_ref[...] = (sums / lens_ref[...]).astype(jnp.bfloat16)
    label = lax.broadcasted_iota(jnp.int32, (SLOTS, LOCAL), 0) + place_ref[6]
    at = lax.broadcasted_iota(jnp.int32, (SLOTS, LOCAL), 1)
    member = (label == image_ref[...]) & (at >= lo) & (at < hi)
    sums = jnp.dot(
        jnp.where(member, 1.0, 0.0).astype(jnp.bfloat16), hid_ref[0:LOCAL, :],
        preferred_element_type=jnp.float32,
    )
    label = lax.broadcasted_iota(jnp.int32, (SLOTS, D), 0)
    sums = sums + jnp.where(label == 0, sum_ref[0:1, :], 0.0)
    few_ref[...] = sums.astype(jnp.bfloat16)


def unpack_kernel(near_ref, far_ref, slot_ref, lens_ref, out_ref):
    at = lax.broadcasted_iota(jnp.int32, (IMAGES, 32 * SLOTS), 1)
    sums = jnp.zeros((IMAGES, D), jnp.float32)
    for i, ref in enumerate((near_ref, far_ref)):
        pick = jnp.where(slot_ref[...] == at + i * 32 * SLOTS, 1.0, 0.0).astype(jnp.bfloat16)
        sums = sums + jnp.dot(pick, ref[...], preferred_element_type=jnp.float32)
    out_ref[...] = sums / lens_ref[...]


def unpack(near, far, slot, lens):
    vmem = pl.BlockSpec(memory_space=pltpu.VMEM)
    return pl.pallas_call(
        unpack_kernel,
        out_shape=jax.ShapeDtypeStruct((IMAGES, D), jnp.float32),
        in_specs=[vmem] * 4,
        out_specs=vmem,
        name="unpack",
    )(near, far, slot, lens)


def attention(edge, place, spans, inputs, gain, weights, extra):
    hbm = pl.BlockSpec(memory_space=pltpu.HBM)
    vmem = pl.BlockSpec(memory_space=pltpu.VMEM)
    smem = pl.BlockSpec(memory_space=pltpu.SMEM)
    rows = LOCAL + 256
    width = WIDTHS[-1]
    hidden = jax.ShapeDtypeStruct((LOCAL, D), jnp.bfloat16)
    if edge:
        outs = (hidden, hidden, jax.ShapeDtypeStruct((8, D), jnp.float32))
        tail = []
    else:
        outs = (
            hidden,
            jax.ShapeDtypeStruct((IMAGES, D), jnp.bfloat16),
            jax.ShapeDtypeStruct((SLOTS, D), jnp.bfloat16),
        )
        tail = [vmem, vmem, hbm, vmem]
    return pl.pallas_call(
        functools.partial(attention_kernel, edge),
        out_shape=outs,
        in_specs=[smem, smem] + [hbm] * len(inputs) + [vmem] + [hbm] * 18 + [vmem] + tail,
        out_specs=(vmem,) * len(outs),
        scratch_shapes=([pltpu.VMEM((WIN + 3 * QB, D), jnp.bfloat16)] if edge else [])
        + [
            pltpu.VMEM((rows, D), jnp.bfloat16),
            pltpu.VMEM((rows, D), jnp.bfloat16),
            pltpu.VMEM((D, 3 * D), jnp.bfloat16),
            pltpu.VMEM((D, D), jnp.bfloat16),
            pltpu.VMEM((rows, D), jnp.bfloat16),
            pltpu.VMEM((rows, D), jnp.bfloat16),
            pltpu.VMEM((HEADS * VROWS, rows), jnp.bfloat16),
            pltpu.VMEM((D, QB), jnp.bfloat16),
            pltpu.VMEM((width, QB), jnp.float32),
            pltpu.VMEM((rows + 2 * SHIFT, D), jnp.bfloat16),
            pltpu.VMEM((width, QB), jnp.float32),
            pltpu.VMEM((width, QB), jnp.float32),
            pltpu.VMEM((width, QB), jnp.bfloat16),
            pltpu.VMEM((width, QB), jnp.bfloat16),
            pltpu.VMEM((1, QB), jnp.float32),
            pltpu.VMEM((1, QB), jnp.float32),
            pltpu.SemaphoreType.DMA((6,)),
        ],
        compiler_params=pltpu.CompilerParams(vmem_limit_bytes=50 * 2**20),
        cost_estimate=pl.CostEstimate(
            flops=15_000_000_000, bytes_accessed=20_000_000, transcendentals=5_000_000
        ),
        name="edge_attention" if edge else "own_attention",
    )(place, spans, *inputs, gain, *weights, spans, *extra)


def layer(tokens, lengths, ln_gain, w_qkv, w_out):
    x, co, z, yh, dp = (lax.axis_index(a) for a in ALL_AXES)
    shard = (x * 2 + co) * 8 + z * 2 + yh
    own = tokens[0]

    p0, p1 = first_pieces(w_qkv, w_out)
    lent = lax.ppermute(own, TOKEN_AXES, [(i, i + 8) for i in WRAPS])
    r0 = moved(p0, Y_UP)
    r1 = moved(p1, Y_DOWN)
    prev = lax.ppermute(own, TOKEN_AXES, [(i, i + 1) for i in range(63) if i not in WRAPS])
    u0 = moved(r0, X_UP)
    d1 = moved(r1, X_DOWN)
    late = lax.ppermute(lent, TOKEN_AXES, [(i + 8, i + 1) for i in WRAPS])
    u1 = moved(r1, X_UP)
    d0 = moved(r0, X_DOWN)
    f0 = moved(u0, X_UP)
    f1 = moved(d1, X_DOWN)
    near = [moved(a, CORE) for a in (r0, r1)]
    ring = [moved(a, CORE) for a in (u0, u1, d0, d1)]
    last = [moved(a, CORE) for a in (f0, f1)]
    mine = [r0, r1, u0, u1, d0, d1, f0, f1]
    other = near + ring + last

    lens = lengths[0]
    ends = jnp.cumsum(lens)
    offsets = ends - lens
    first = (shard - 1) * LOCAL
    at = first + jnp.arange(WIN + 256, dtype=jnp.int32)
    begun = offsets[:, None] <= at[None, :]
    image = jnp.sum(begun.astype(jnp.int32), axis=0) - 1
    start = jnp.max(jnp.where(begun, offsets[:, None], -WIN), axis=0) - first
    end = jnp.min(jnp.where(ends[:, None] > at[None, :], ends[:, None], 1 << 20), axis=0) - first
    spans = jnp.stack([start, end]).astype(jnp.int32)
    low = start[LOCAL]
    cut = jnp.where(low < LOCAL, end[LOCAL], LOCAL)
    limit = jnp.where(end[WIN - 1] == WIN, WIN, start[WIN - 1])
    wrap = (co + z + yh == 0) & (x > 0)
    places = [
        jnp.stack([x, co, dp, lo, hi, wrap, image[LOCAL]]).astype(jnp.int32)
        for lo, hi in ((low, cut), (cut - LOCAL, limit - LOCAL))
    ]
    owner = (ends - 1) // LOCAL
    leader = jnp.sum((offsets[None, :] <= owner[:, None] * LOCAL).astype(jnp.int32), axis=1) - 1
    rank = jnp.arange(IMAGES, dtype=jnp.int32) - leader
    group = owner // 16 * 8 + owner % 8
    slot = jnp.where(owner // 8 % 2 == co, 0, 32 * SLOTS) + group * SLOTS + rank
    slot = slot[:, None]
    crowded = jnp.full((8, 128), jnp.max(rank) >= SLOTS).astype(jnp.float32)
    elsewhere = lax.ppermute(crowded, "dp", SWAP)
    fits = crowded[0, 0] + elsewhere[0, 0] == 0.0

    gain = ln_gain[None]
    weights = [w_qkv, w_out, *mine, *other]

    hprev, hedge, total = attention(True, places[0], spans, [prev, late, own], gain, weights, [])
    back = lax.ppermute(hprev, TOKEN_AXES, [(i + 1, i) for i in range(63)])
    hown, part, few = attention(
        False, places[1], spans[:, LOCAL:] - LOCAL, [own], gain, weights,
        [image[None, LOCAL:WIN], lens.astype(jnp.float32)[:, None], hedge, total],
    )

    lens_column = lens.astype(jnp.float32)[:, None]

    def pooled_directly(few, part):
        near = lax.all_to_all(
            jnp.broadcast_to(few[None], (32, SLOTS, D)), GROUP, 0, 0, tiled=True
        ).reshape(32 * SLOTS, D)
        far = lax.ppermute(near, "co", SWAP)
        return unpack(near, far, slot, lens_column)

    def pooled_by_sums(few, part):
        part = part.reshape(2, IMAGES // 2, D)
        kept = lax.dynamic_index_in_dim(part, co, 0, keepdims=False)
        given = lax.dynamic_index_in_dim(part, 1 - co, 0, keepdims=False)
        given = lax.ppermute(given, "co", SWAP)
        kept = kept.astype(jnp.float32) + given.astype(jnp.float32)
        kept = kept.astype(jnp.bfloat16).reshape(32, 4, D)
        rows = lax.all_to_all(kept, GROUP, 0, 0, tiled=True).astype(jnp.float32)
        rows = jnp.sum(rows, axis=0).astype(jnp.bfloat16)
        half = lax.all_to_all(jnp.broadcast_to(rows[None], (32, 4, D)), GROUP, 0, 0, tiled=True)
        half = half.reshape(IMAGES // 2, D)
        rest = lax.ppermute(half, "co", SWAP)
        pooled = jnp.where(co == 0, jnp.stack([half, rest]), jnp.stack([rest, half]))
        return pooled.reshape(IMAGES, D).astype(jnp.float32)

    pooled = lax.cond(fits, pooled_directly, pooled_by_sums, few, part)[None]

    here = jnp.arange(LOCAL, dtype=jnp.int32)[:, None] < limit - LOCAL
    hidden = jnp.where(here, hown, back)[None]
    return hidden, pooled


def solution(mesh):
    fine = Mesh(mesh.devices.reshape(4, 2, 4, 2, 2), ALL_AXES)
    in_specs = (P("dp", TOKEN_AXES, None), P("dp", None), P(), P("dp", None), P("dp", None))
    out_specs = (P("dp", TOKEN_AXES, None), P("dp", None, None))
    return jax.shard_map(layer, mesh=fine, in_specs=in_specs, out_specs=out_specs, check_vma=False)
```

```python
import functools
import itertools

import jax
import jax.numpy as jnp
from jax import lax
from jax.experimental import pallas as pl
from jax.experimental.pallas import tpu as pltpu
from jax.sharding import Mesh
from jax.sharding import PartitionSpec as P


HEADS = 16
SIZE = 80
VROWS = 96
D = HEADS * SIZE
LOCAL = 512
WIN = 2 * LOCAL
QB = 256
IMAGES = 256
WIDTHS = (256, 384, 512)
SHIFT = 16
SLOTS = 16
HALF = D // 2
KR = 160
TOKEN_AXES = ("x", "co", "z", "yh")
ALL_AXES = TOKEN_AXES + ("dp",)
GROUP = ("x", "z", "yh")
SWAP = [(0, 1), (1, 0)]
LOG2E = 1.4426950408889634


def permutation(move):
    def index(x, co, z, y):
        return ((x * 2 + co) * 8 + (z * 2 + y // 2)) * 2 + y % 2

    places = itertools.product(range(4), range(2), range(4), range(4))
    return [(index(*place), index(*move(*place))) for place in places]


Y_UP = permutation(lambda x, co, z, y: (x, co, z, (y + 1) % 4))
Y_DOWN = permutation(lambda x, co, z, y: (x, co, z, (y - 1) % 4))
X_UP = permutation(lambda x, co, z, y: ((x + 1) % 4, co, z, y))
X_DOWN = permutation(lambda x, co, z, y: ((x - 1) % 4, co, z, y))
Z_UP = permutation(lambda x, co, z, y: (x, co, (z + 1) % 4, y))
Z_DOWN = permutation(lambda x, co, z, y: (x, co, (z - 1) % 4, y))
CORE = permutation(lambda x, co, z, y: (x, 1 - co, z, y))


def moved(piece, pairs):
    return lax.ppermute(piece, ALL_AXES, pairs)


def first_pieces(w_qkv, w_out):
    x, co, z = (lax.axis_index(a) for a in ("x", "co", "z"))
    near = lax.dynamic_slice(w_qkv, (x * KR, co * 2 * D), (KR, D))
    q = lax.dynamic_slice(w_qkv, (z * KR, D), (KR, D))
    o = lax.dynamic_slice(w_out, (z * KR, 0), (KR, D))
    return near, jnp.where(co == 0, q, o)


def attention_kernel(edge, place_ref, ends_ref, *refs):
    if edge:
        prev_ref, refs = refs[0], refs[1:]
    own_ref, gain_ref, wqkv_ref, wout_ref, refs = *refs[:4], refs[4:]
    mine_refs, other_refs, spans_ref, refs = refs[:10], refs[10:20], refs[20], refs[21:]
    if edge:
        lens_ref, hin_ref, sum_ref, refs = *refs[:3], refs[3:]
        hprev_ref, hown_ref, pooled_ref, few_ref, refs = *refs[:4], refs[4:]
    else:
        image_ref, hown_ref, sum_ref, refs = *refs[:3], refs[3:]
    if edge:
        wide_ref, refs = refs[0], refs[1:]
    (
        x_ref, n_ref, w_ref, wo_ref, q_ref, k_ref, vt_ref, ctx_ref, bias_ref, hid_ref,
        s0_ref, s1_ref, p0_ref, p1_ref, top0_ref, top1_ref, sem,
    ) = refs
    x, co, dp, lo, hi, z = (place_ref[i] for i in range(6))
    if edge:
        first = pl.multiple_of(lo // SHIFT * SHIFT, SHIFT)
        offset = lo - first
        base, lo, hi = 0, 0, hi - lo
    else:
        base = (lo // 128) * 128
    blocks = (hi - base + QB - 1) // QB

    far = (1 - dp) * HALF

    tokens_ref = wide_ref if edge else x_ref
    inputs = [
        pltpu.make_async_copy(
            own_ref, tokens_ref.at[pl.ds(LOCAL if edge else 0, LOCAL)], sem.at[0]
        )
    ]
    inputs[0].start()
    if edge:
        inputs.append(pltpu.make_async_copy(prev_ref, wide_ref.at[pl.ds(0, LOCAL)], sem.at[0]))
        inputs[1].start()

    def near(part, target, cols):
        return pltpu.make_async_copy(
            wout_ref if part == 3 else wqkv_ref.at[:, cols],
            target.at[pl.ds(pl.multiple_of(dp * HALF, 16), HALF), cols],
            sem.at[1 + part],
        )

    def distant(part, source, row, count):
        target = wo_ref if part == 3 else w_ref
        rows = pl.ds(pl.multiple_of(far + row, 16), count)
        return pltpu.make_async_copy(source, target.at[rows, columns[part]], sem.at[1 + part])

    columns = [pl.ds(0, D), pl.ds(D, D), pl.ds(2 * D, D), pl.ds(0, D)]
    targets = [w_ref, w_ref, w_ref, wo_ref]
    for part in range(4):
        near(part, targets[part], columns[part]).start()
        side = part % 2
        turn = z if side else x
        for held, core in ((mine_refs, co), (other_refs, 1 - co)):

            @pl.when(core == part // 2)
            def _(held=held, part=part, side=side, turn=turn):
                for slot, shift in enumerate((0, 3, 1)):
                    row = lax.rem(turn + shift, 4) * KR
                    distant(part, held[slot * 2 + side], row, KR).start()
                row = lax.rem(turn + 2, 4) * KR
                distant(part, held[6 + side], row, KR // 2).start()
                distant(part, held[8 + side], row + KR // 2, KR // 2).start()

    def arrived(part):
        near(part, targets[part], columns[part]).wait()
        for _ in range(4):
            distant(part, mine_refs[0], 0, KR).wait()

    if not edge:
        x_ref[LOCAL:, :] = jnp.zeros((x_ref.shape[0] - LOCAL, D), jnp.bfloat16)
    for copy in inputs:
        copy.wait()

    def mover(lag):
        out = lax.broadcasted_iota(jnp.int32, (QB, QB + SHIFT), 0)
        source = lax.broadcasted_iota(jnp.int32, (QB, QB + SHIFT), 1)
        return jnp.where(source == out + lag, 1.0, 0.0).astype(jnp.bfloat16)

    if edge:
        wide_ref[WIN:, :] = jnp.zeros((wide_ref.shape[0] - WIN, D), jnp.bfloat16)
        pick = mover(offset)

        def align(j, carry):
            rows = pl.ds(pl.multiple_of(first + j * QB, SHIFT), QB + SHIFT)
            taken = jnp.dot(pick, wide_ref[rows, :], preferred_element_type=jnp.float32)
            x_ref[pl.ds(pl.multiple_of(j * QB, QB), QB), :] = taken.astype(jnp.bfloat16)
            return carry

        lax.fori_loop(0, blocks, align, 0)

    def block_rows(j):
        row0 = pl.multiple_of(base + j * QB, 128)
        return row0, pl.ds(row0, QB)

    def normalize(j, carry):
        _, rows = block_rows(j)
        values = x_ref[rows, :].astype(jnp.float32)
        center = values - jnp.mean(values, axis=1, keepdims=True)
        spread = jnp.mean(center * center, axis=1, keepdims=True)
        normed = center * lax.rsqrt(spread + 1e-05) * gain_ref[...]
        n_ref[rows, :] = normed.astype(jnp.bfloat16)
        return carry

    lax.fori_loop(0, blocks, normalize, 0)
    k_ref[...] = jnp.zeros_like(k_ref)
    vt_ref[...] = jnp.zeros_like(vt_ref)
    hid_ref[...] = jnp.zeros_like(hid_ref)
    if edge:
        wide_ref[...] = jnp.zeros_like(wide_ref)

    def project_q(j, carry):
        _, rows = block_rows(j)
        q = jnp.dot(n_ref[rows, :], w_ref[:, 0:D], preferred_element_type=jnp.float32)
        q_ref[rows, :] = (q * (LOG2E * SIZE**-0.5)).astype(jnp.bfloat16)
        return carry

    def project_k(j, carry):
        _, rows = block_rows(j)
        k = jnp.dot(n_ref[rows, :], w_ref[:, D : 2 * D], preferred_element_type=jnp.float32)
        k_ref[rows, :] = k.astype(jnp.bfloat16)
        return carry

    def project_v(j, carry):
        _, rows = block_rows(j)
        v = jnp.dot(n_ref[rows, :], w_ref[:, 2 * D :], preferred_element_type=jnp.float32)
        vt = v.T.astype(jnp.bfloat16)
        for h in range(HEADS):
            vt_ref[pl.ds(h * VROWS, SIZE), rows] = vt[h * SIZE : (h + 1) * SIZE]
            vt_ref[pl.ds(h * VROWS + SIZE, VROWS - SIZE), rows] = jnp.ones(
                (VROWS - SIZE, QB), jnp.bfloat16
            )
        return carry

    for part, project in enumerate((project_q, project_k, project_v)):
        arrived(part)
        lax.fori_loop(0, blocks, project, 0)
    arrived(3)

    def attend(j, carry):
        row0, rows = block_rows(j)
        if edge:
            k0, need = 0, hi
            start, end = 0, hi
        else:
            least = ends_ref[0, jnp.maximum(row0, lo)]
            most = ends_ref[1, jnp.minimum(row0 + QB, hi) - 1]
            k0 = pl.multiple_of((least // 128) * 128, 128)
            need = most - k0
            start = spans_ref[0:1, rows]
            end = spans_ref[1:2, rows]
        for i, width in enumerate(WIDTHS):
            above = WIDTHS[i - 1] if i else 0

            @pl.when((need > above) & (need <= width))
            def _(width=width):
                keys = pl.ds(k0, width)
                at = lax.broadcasted_iota(jnp.int32, (width, QB), 0) + k0
                bias_ref[0:width, :] = jnp.where((at >= start) & (at < end), 0.0, -1e30)

                def scores(h, s_ref, top_ref):
                    w0 = pl.multiple_of(jnp.minimum((h * SIZE) // 128 * 128, D - 256), 128)
                    lanes = pl.ds(w0, 256)
                    lane = lax.broadcasted_iota(jnp.int32, (1, 256), 1) + (w0 - h * SIZE)
                    inside = jnp.where((lane >= 0) & (lane < SIZE), 1.0, 0.0)
                    q = q_ref[rows, lanes] * inside.astype(jnp.bfloat16)
                    s = lax.dot_general(
                        k_ref[keys, lanes], q, (((1,), (1,)), ((), ())),
                        preferred_element_type=jnp.float32,
                    )
                    s = s + bias_ref[0:width, :]
                    s_ref[0:width, :] = s
                    top_ref[...] = jnp.max(s, axis=0, keepdims=True)

                def weights(s_ref, top_ref, p_ref):
                    p_ref[0:width, :] = jnp.exp2(s_ref[0:width, :] - top_ref[...]).astype(
                        jnp.bfloat16
                    )

                def mix(h, p_ref):
                    features = pl.ds(pl.multiple_of(h * VROWS, 16), VROWS)
                    c = jnp.dot(
                        vt_ref[features, keys], p_ref[0:width, :],
                        preferred_element_type=jnp.float32,
                    )
                    ctx_ref[pl.ds(pl.multiple_of(h * SIZE, 16), SIZE), :] = (
                        c[0:SIZE] * (1.0 / c[SIZE : SIZE + 1])
                    ).astype(jnp.bfloat16)

                scores(0, s0_ref, top0_ref)

                def two_heads(i, inner):
                    h = i * 2
                    scores(h + 1, s1_ref, top1_ref)
                    weights(s0_ref, top0_ref, p0_ref)
                    mix(jnp.maximum(h - 1, 0), p1_ref)
                    scores(jnp.minimum(h + 2, HEADS - 1), s0_ref, top0_ref)
                    weights(s1_ref, top1_ref, p1_ref)
                    mix(h, p0_ref)
                    return inner

                lax.fori_loop(0, HEADS // 2, two_heads, 0)
                mix(HEADS - 1, p1_ref)

        mixed = lax.dot_general(
            ctx_ref[...], wo_ref[...], (((0,), (0,)), ((), ())),
            preferred_element_type=jnp.float32,
        )
        hidden = x_ref[rows, :].astype(jnp.float32) + mixed
        at = lax.broadcasted_iota(jnp.int32, (QB, D), 0) + row0
        inside = (at >= lo) & (at < hi)
        hidden = hidden.astype(jnp.bfloat16)
        if edge:
            hid_ref[pl.ds(pl.multiple_of(row0 + SHIFT, SHIFT), QB), :] = jnp.where(
                inside, hidden, jnp.zeros_like(hidden)
            )
        else:
            hid_ref[rows, :] = jnp.where(inside, hidden, hid_ref[rows, :])
        return carry

    lax.fori_loop(0, blocks, attend, 0)

    if edge:
        put = mover(SHIFT - offset)

        @pl.when(hi > 0)
        def _():
            for j in range(3):
                moved_rows = jnp.dot(
                    put, hid_ref[j * QB : (j + 1) * QB + SHIFT, :],
                    preferred_element_type=jnp.float32,
                )
                rows = pl.ds(pl.multiple_of(first + j * QB, SHIFT), QB)
                wide_ref[rows, :] = moved_rows.astype(jnp.bfloat16)

        hprev_ref[...] = wide_ref[0:LOCAL, :]
        hown_ref[...] = hin_ref[...] + wide_ref[LOCAL:WIN, :]
        extra = jnp.dot(
            jnp.ones((8, LOCAL + SHIFT), jnp.bfloat16), hid_ref[0 : LOCAL + SHIFT, :],
            preferred_element_type=jnp.float32,
        )
        label = lax.broadcasted_iota(jnp.int32, (IMAGES, D), 0)
        sums = sum_ref[...] + jnp.where(label == place_ref[6], extra[0:1, :], 0.0)
        pooled = (sums / lens_ref[...]).astype(jnp.bfloat16)
        pooled_ref[...] = pooled
        label = lax.broadcasted_iota(jnp.int32, (SLOTS, IMAGES), 0) + place_ref[6]
        pick = lax.broadcasted_iota(jnp.int32, (SLOTS, IMAGES), 1) == label
        few_ref[...] = jnp.dot(
            jnp.where(pick, 1.0, 0.0).astype(jnp.bfloat16), pooled,
            preferred_element_type=jnp.float32,
        ).astype(jnp.bfloat16)
        return
    hown_ref[...] = hid_ref[0:LOCAL, :]
    label = lax.broadcasted_iota(jnp.int32, (IMAGES, LOCAL), 0)
    at = lax.broadcasted_iota(jnp.int32, (IMAGES, LOCAL), 1)
    member = (label == image_ref[...]) & (at >= lo) & (at < hi)
    sums = jnp.dot(
        jnp.where(member, 1.0, 0.0).astype(jnp.bfloat16), hid_ref[0:LOCAL, :],
        preferred_element_type=jnp.float32,
    )
    sum_ref[...] = sums


def unpack_kernel(near_ref, far_ref, slot_ref, out_ref):
    at = lax.broadcasted_iota(jnp.int32, (32 * SLOTS, IMAGES), 0)
    means = jnp.zeros((IMAGES, D), jnp.float32)
    for i, ref in enumerate((near_ref, far_ref)):
        pick = jnp.where(slot_ref[...] == at + i * 32 * SLOTS, 1.0, 0.0).astype(jnp.bfloat16)
        means = means + lax.dot_general(
            pick, ref[...], (((0,), (0,)), ((), ())), preferred_element_type=jnp.float32
        )
    out_ref[...] = means


def unpack(near, far, slot):
    vmem = pl.BlockSpec(memory_space=pltpu.VMEM)
    return pl.pallas_call(
        unpack_kernel,
        out_shape=jax.ShapeDtypeStruct((IMAGES, D), jnp.float32),
        in_specs=[vmem] * 3,
        out_specs=vmem,
        compiler_params=pltpu.CompilerParams(vmem_limit_bytes=16 * 2**20),
        name="unpack",
    )(near, far, slot)


def attention(edge, place, spans, inputs, gain, weights, extra):
    hbm = pl.BlockSpec(memory_space=pltpu.HBM)
    vmem = pl.BlockSpec(memory_space=pltpu.VMEM)
    smem = pl.BlockSpec(memory_space=pltpu.SMEM)
    rows = LOCAL + 256
    width = WIDTHS[-1]
    hidden = jax.ShapeDtypeStruct((LOCAL, D), jnp.bfloat16)
    sums = jax.ShapeDtypeStruct((IMAGES, D), jnp.float32)
    if edge:
        pooled = jax.ShapeDtypeStruct((IMAGES, D), jnp.bfloat16)
        outs = (hidden, hidden, pooled, jax.ShapeDtypeStruct((SLOTS, D), jnp.bfloat16))
        tail = [vmem, vmem, vmem]
    else:
        outs = (hidden, sums)
        tail = [vmem]
    return pl.pallas_call(
        functools.partial(attention_kernel, edge),
        out_shape=outs,
        in_specs=[smem, smem] + [hbm] * len(inputs) + [vmem] + [hbm] * 22 + [vmem] + tail,
        out_specs=(vmem,) * len(outs),
        scratch_shapes=([pltpu.VMEM((WIN + 3 * QB, D), jnp.bfloat16)] if edge else [])
        + [
            pltpu.VMEM((rows, D), jnp.bfloat16),
            pltpu.VMEM((rows, D), jnp.bfloat16),
            pltpu.VMEM((D, 3 * D), jnp.bfloat16),
            pltpu.VMEM((D, D), jnp.bfloat16),
            pltpu.VMEM((rows, D), jnp.bfloat16),
            pltpu.VMEM((rows, D), jnp.bfloat16),
            pltpu.VMEM((HEADS * VROWS, rows), jnp.bfloat16),
            pltpu.VMEM((D, QB), jnp.bfloat16),
            pltpu.VMEM((width, QB), jnp.float32),
            pltpu.VMEM((rows + 2 * SHIFT, D), jnp.bfloat16),
            pltpu.VMEM((width, QB), jnp.float32),
            pltpu.VMEM((width, QB), jnp.float32),
            pltpu.VMEM((width, QB), jnp.bfloat16),
            pltpu.VMEM((width, QB), jnp.bfloat16),
            pltpu.VMEM((1, QB), jnp.float32),
            pltpu.VMEM((1, QB), jnp.float32),
            pltpu.SemaphoreType.DMA((6,)),
        ],
        compiler_params=pltpu.CompilerParams(vmem_limit_bytes=50 * 2**20),
        cost_estimate=pl.CostEstimate(
            flops=15_000_000_000, bytes_accessed=20_000_000, transcendentals=5_000_000
        ),
        name="edge_attention" if edge else "own_attention",
    )(place, spans, *inputs, gain, *weights, spans, *extra)


def layer(tokens, lengths, ln_gain, w_qkv, w_out):
    x, co, z, yh, dp = (lax.axis_index(a) for a in ALL_AXES)
    shard = (x * 2 + co) * 8 + z * 2 + yh
    own = tokens[0]

    p0, p1 = first_pieces(w_qkv, w_out)
    r0 = moved(p0, Y_UP)
    r1 = moved(p1, Y_DOWN)
    ux, dx = moved(r0, X_UP), moved(r0, X_DOWN)
    uz, dz = moved(r1, Z_UP), moved(r1, Z_DOWN)
    half = KR // 2
    fx, fz = moved(ux[:half], X_UP), moved(uz[:half], Z_UP)
    gx, gz = moved(dx[half:], X_DOWN), moved(dz[half:], Z_DOWN)
    prev = lax.ppermute(own, TOKEN_AXES, [(i, i + 1) for i in range(63)])
    near = [moved(a, CORE) for a in (r0, r1, ux, uz, dx, dz)]
    last = [moved(a, CORE) for a in (fx, fz, gx, gz)]
    mine = [r0, r1, ux, uz, dx, dz, fx, fz, gx, gz]
    other = near + last

    lens = lengths[0]
    ends = jnp.cumsum(lens)
    offsets = ends - lens
    first = (shard - 1) * LOCAL
    at = first + jnp.arange(WIN + 256, dtype=jnp.int32)
    begun = offsets[:, None] <= at[None, :]
    image = jnp.sum(begun.astype(jnp.int32), axis=0) - 1
    start = jnp.max(jnp.where(begun, offsets[:, None], -WIN), axis=0) - first
    end = jnp.min(jnp.where(ends[:, None] > at[None, :], ends[:, None], 1 << 20), axis=0) - first
    spans = jnp.stack([start, end]).astype(jnp.int32)
    low = start[LOCAL]
    cut = jnp.where(low < LOCAL, end[LOCAL], LOCAL)
    limit = jnp.where(end[WIN - 1] == WIN, WIN, start[WIN - 1])
    places = [
        jnp.stack([x, co, dp, lo, hi, z, image[LOCAL]]).astype(jnp.int32)
        for lo, hi in ((low, cut), (cut - LOCAL, limit - LOCAL))
    ]
    owner = (ends - 1) // LOCAL
    leader = jnp.sum((offsets[None, :] <= owner[:, None] * LOCAL).astype(jnp.int32), axis=1) - 1
    rank = jnp.arange(IMAGES, dtype=jnp.int32) - leader
    group = owner // 16 * 8 + owner % 8
    slot = jnp.where(owner // 8 % 2 == co, 0, 32 * SLOTS) + group * SLOTS + rank
    slot = slot[None]
    crowded = jnp.full((8, 128), jnp.max(rank) >= SLOTS).astype(jnp.float32)
    elsewhere = lax.ppermute(crowded, "dp", SWAP)
    fits = crowded[0, 0] + elsewhere[0, 0] == 0.0

    gain = ln_gain[None]
    weights = [w_qkv, w_out, *mine, *other]

    hown, sums = attention(
        False, places[1], spans[:, LOCAL:] - LOCAL, [own], gain, weights, [image[None, LOCAL:WIN]]
    )
    hprev, hown, part, few = attention(
        True, places[0], spans, [prev, own], gain, weights,
        [lens.astype(jnp.float32)[:, None], hown, sums],
    )
    back = lax.ppermute(hprev, TOKEN_AXES, [(i + 1, i) for i in range(63)])

    def pooled_directly(few, part):
        near = lax.all_to_all(
            jnp.broadcast_to(few[None], (32, SLOTS, D)), GROUP, 0, 0, tiled=True
        ).reshape(32 * SLOTS, D)
        far = lax.ppermute(near, "co", SWAP)
        return unpack(near, far, slot)

    def pooled_by_sums(few, part):
        part = part.reshape(2, IMAGES // 2, D)
        kept = lax.dynamic_index_in_dim(part, co, 0, keepdims=False)
        given = lax.dynamic_index_in_dim(part, 1 - co, 0, keepdims=False)
        given = lax.ppermute(given, "co", SWAP)
        kept = kept.astype(jnp.float32) + given.astype(jnp.float32)
        kept = kept.astype(jnp.bfloat16).reshape(32, 4, D)
        rows = lax.all_to_all(kept, GROUP, 0, 0, tiled=True).astype(jnp.float32)
        rows = jnp.sum(rows, axis=0).astype(jnp.bfloat16)
        half = lax.all_to_all(jnp.broadcast_to(rows[None], (32, 4, D)), GROUP, 0, 0, tiled=True)
        half = half.reshape(IMAGES // 2, D)
        rest = lax.ppermute(half, "co", SWAP)
        pooled = jnp.where(co == 0, jnp.stack([half, rest]), jnp.stack([rest, half]))
        return pooled.reshape(IMAGES, D).astype(jnp.float32)

    pooled = lax.cond(fits, pooled_directly, pooled_by_sums, few, part)[None]

    here = jnp.arange(LOCAL, dtype=jnp.int32)[:, None] < limit - LOCAL
    hidden = jnp.where(here, hown, back)[None]
    return hidden, pooled


def solution(mesh):
    fine = Mesh(mesh.devices.reshape(4, 2, 4, 2, 2), ALL_AXES)
    in_specs = (P("dp", TOKEN_AXES, None), P("dp", None), P(), P("dp", None), P("dp", None))
    out_specs = (P("dp", TOKEN_AXES, None), P("dp", None, None))
    return jax.shard_map(layer, mesh=fine, in_specs=in_specs, out_specs=out_specs, check_vma=False)
```

```python
import functools
import itertools

import jax
import jax.numpy as jnp
from jax import lax
from jax.experimental import pallas as pl
from jax.experimental.pallas import tpu as pltpu
from jax.sharding import Mesh
from jax.sharding import PartitionSpec as P


HEADS = 16
SIZE = 80
VROWS = 96
D = HEADS * SIZE
LOCAL = 512
WIN = 2 * LOCAL
QB = 256
IMAGES = 256
WIDTHS = (256, 384, 512)
SHIFT = 16
SLOTS = 16
HALF = D // 2
KR = 160
TOKEN_AXES = ("x", "co", "z", "yh")
ALL_AXES = TOKEN_AXES + ("dp",)
GROUP = ("x", "z", "yh")
SWAP = [(0, 1), (1, 0)]
LOG2E = 1.4426950408889634


def permutation(move):
    def index(x, co, z, y):
        return ((x * 2 + co) * 8 + (z * 2 + y // 2)) * 2 + y % 2

    places = itertools.product(range(4), range(2), range(4), range(4))
    return [(index(*place), index(*move(*place))) for place in places]


Y_UP = permutation(lambda x, co, z, y: (x, co, z, (y + 1) % 4))
Y_DOWN = permutation(lambda x, co, z, y: (x, co, z, (y - 1) % 4))
X_UP = permutation(lambda x, co, z, y: ((x + 1) % 4, co, z, y))
X_DOWN = permutation(lambda x, co, z, y: ((x - 1) % 4, co, z, y))
Z_UP = permutation(lambda x, co, z, y: (x, co, (z + 1) % 4, y))
Z_DOWN = permutation(lambda x, co, z, y: (x, co, (z - 1) % 4, y))
CORE = permutation(lambda x, co, z, y: (x, 1 - co, z, y))


def moved(piece, pairs):
    return lax.ppermute(piece, ALL_AXES, pairs)


def first_pieces(w_qkv, w_out):
    x, co, z = (lax.axis_index(a) for a in ("x", "co", "z"))
    near = lax.dynamic_slice(w_qkv, (x * KR, co * 2 * D), (KR, D))
    q = lax.dynamic_slice(w_qkv, (z * KR, D), (KR, D))
    o = lax.dynamic_slice(w_out, (z * KR, 0), (KR, D))
    return near, jnp.where(co == 0, q, o)


def attention_kernel(edge, place_ref, ends_ref, *refs):
    if edge:
        prev_ref, refs = refs[0], refs[1:]
    own_ref, gain_ref, wqkv_ref, wout_ref, refs = *refs[:4], refs[4:]
    mine_refs, other_refs, spans_ref, refs = refs[:10], refs[10:20], refs[20], refs[21:]
    if edge:
        lens_ref, hin_ref, sum_ref, refs = *refs[:3], refs[3:]
        hprev_ref, hown_ref, pooled_ref, few_ref, refs = *refs[:4], refs[4:]
    else:
        image_ref, lens_ref, hown_ref, sum_ref, few_ref, refs = *refs[:5], refs[5:]
    if edge:
        wide_ref, refs = refs[0], refs[1:]
    (
        x_ref, n_ref, w_ref, wo_ref, q_ref, k_ref, vt_ref, ctx_ref, bias_ref, hid_ref,
        s0_ref, s1_ref, p0_ref, p1_ref, top0_ref, top1_ref, sem,
    ) = refs
    x, co, dp, lo, hi, z = (place_ref[i] for i in range(6))
    if edge:
        first = pl.multiple_of(lo // SHIFT * SHIFT, SHIFT)
        offset = lo - first
        base, lo, hi = 0, 0, hi - lo
    else:
        base = (lo // 128) * 128
    blocks = (hi - base + QB - 1) // QB

    far = (1 - dp) * HALF

    tokens_ref = wide_ref if edge else x_ref
    inputs = [
        pltpu.make_async_copy(
            own_ref, tokens_ref.at[pl.ds(LOCAL if edge else 0, LOCAL)], sem.at[0]
        )
    ]
    inputs[0].start()
    if edge:
        inputs.append(pltpu.make_async_copy(prev_ref, wide_ref.at[pl.ds(0, LOCAL)], sem.at[0]))
        inputs[1].start()

    def near(part, target, cols):
        return pltpu.make_async_copy(
            wout_ref if part == 3 else wqkv_ref.at[:, cols],
            target.at[pl.ds(pl.multiple_of(dp * HALF, 16), HALF), cols],
            sem.at[1 + part],
        )

    def distant(part, source, row, count):
        target = wo_ref if part == 3 else w_ref
        rows = pl.ds(pl.multiple_of(far + row, 16), count)
        return pltpu.make_async_copy(source, target.at[rows, columns[part]], sem.at[1 + part])

    columns = [pl.ds(0, D), pl.ds(D, D), pl.ds(2 * D, D), pl.ds(0, D)]
    targets = [w_ref, w_ref, w_ref, wo_ref]
    for part in range(4):
        near(part, targets[part], columns[part]).start()
        side = part % 2
        turn = z if side else x
        for held, core in ((mine_refs, co), (other_refs, 1 - co)):

            @pl.when(core == part // 2)
            def _(held=held, part=part, side=side, turn=turn):
                for slot, shift in enumerate((0, 3, 1)):
                    row = lax.rem(turn + shift, 4) * KR
                    distant(part, held[slot * 2 + side], row, KR).start()
                row = lax.rem(turn + 2, 4) * KR
                distant(part, held[6 + side], row, KR // 2).start()
                distant(part, held[8 + side], row + KR // 2, KR // 2).start()

    def arrived(part):
        near(part, targets[part], columns[part]).wait()
        for _ in range(4):
            distant(part, mine_refs[0], 0, KR).wait()

    if not edge:
        x_ref[LOCAL:, :] = jnp.zeros((x_ref.shape[0] - LOCAL, D), jnp.bfloat16)
    for copy in inputs:
        copy.wait()

    def mover(lag):
        out = lax.broadcasted_iota(jnp.int32, (QB, QB + SHIFT), 0)
        source = lax.broadcasted_iota(jnp.int32, (QB, QB + SHIFT), 1)
        return jnp.where(source == out + lag, 1.0, 0.0).astype(jnp.bfloat16)

    if edge:
        wide_ref[WIN:, :] = jnp.zeros((wide_ref.shape[0] - WIN, D), jnp.bfloat16)
        pick = mover(offset)

        def align(j, carry):
            rows = pl.ds(pl.multiple_of(first + j * QB, SHIFT), QB + SHIFT)
            taken = jnp.dot(pick, wide_ref[rows, :], preferred_element_type=jnp.float32)
            x_ref[pl.ds(pl.multiple_of(j * QB, QB), QB), :] = taken.astype(jnp.bfloat16)
            return carry

        lax.fori_loop(0, blocks, align, 0)

    def block_rows(j):
        row0 = pl.multiple_of(base + j * QB, 128)
        return row0, pl.ds(row0, QB)

    def normalize(j, carry):
        _, rows = block_rows(j)
        values = x_ref[rows, :].astype(jnp.float32)
        center = values - jnp.mean(values, axis=1, keepdims=True)
        spread = jnp.mean(center * center, axis=1, keepdims=True)
        normed = center * lax.rsqrt(spread + 1e-05) * gain_ref[...]
        n_ref[rows, :] = normed.astype(jnp.bfloat16)
        return carry

    lax.fori_loop(0, blocks, normalize, 0)
    k_ref[...] = jnp.zeros_like(k_ref)
    vt_ref[...] = jnp.zeros_like(vt_ref)
    hid_ref[...] = jnp.zeros_like(hid_ref)
    if edge:
        wide_ref[...] = jnp.zeros_like(wide_ref)

    def project_q(j, carry):
        _, rows = block_rows(j)
        q = jnp.dot(n_ref[rows, :], w_ref[:, 0:D], preferred_element_type=jnp.float32)
        q_ref[rows, :] = (q * (LOG2E * SIZE**-0.5)).astype(jnp.bfloat16)
        return carry

    def project_k(j, carry):
        _, rows = block_rows(j)
        k = jnp.dot(n_ref[rows, :], w_ref[:, D : 2 * D], preferred_element_type=jnp.float32)
        k_ref[rows, :] = k.astype(jnp.bfloat16)
        return carry

    def project_v(j, carry):
        _, rows = block_rows(j)
        v = jnp.dot(n_ref[rows, :], w_ref[:, 2 * D :], preferred_element_type=jnp.float32)
        vt = v.T.astype(jnp.bfloat16)
        for h in range(HEADS):
            vt_ref[pl.ds(h * VROWS, SIZE), rows] = vt[h * SIZE : (h + 1) * SIZE]
            vt_ref[pl.ds(h * VROWS + SIZE, VROWS - SIZE), rows] = jnp.ones(
                (VROWS - SIZE, QB), jnp.bfloat16
            )
        return carry

    for part, project in enumerate((project_q, project_k, project_v)):
        arrived(part)
        lax.fori_loop(0, blocks, project, 0)
    arrived(3)

    def attend(j, carry):
        row0, rows = block_rows(j)
        if edge:
            k0, need = 0, hi
            start, end = 0, hi
        else:
            least = ends_ref[0, jnp.maximum(row0, lo)]
            most = ends_ref[1, jnp.minimum(row0 + QB, hi) - 1]
            k0 = pl.multiple_of((least // 128) * 128, 128)
            need = most - k0
            start = spans_ref[0:1, rows]
            end = spans_ref[1:2, rows]
        for i, width in enumerate(WIDTHS):
            above = WIDTHS[i - 1] if i else 0

            @pl.when((need > above) & (need <= width))
            def _(width=width):
                keys = pl.ds(k0, width)
                at = lax.broadcasted_iota(jnp.int32, (width, QB), 0) + k0
                bias_ref[0:width, :] = jnp.where((at >= start) & (at < end), 0.0, -1e30)

                def scores(h, s_ref, top_ref):
                    w0 = pl.multiple_of(jnp.minimum((h * SIZE) // 128 * 128, D - 256), 128)
                    lanes = pl.ds(w0, 256)
                    lane = lax.broadcasted_iota(jnp.int32, (1, 256), 1) + (w0 - h * SIZE)
                    inside = jnp.where((lane >= 0) & (lane < SIZE), 1.0, 0.0)
                    q = q_ref[rows, lanes] * inside.astype(jnp.bfloat16)
                    s = lax.dot_general(
                        k_ref[keys, lanes], q, (((1,), (1,)), ((), ())),
                        preferred_element_type=jnp.float32,
                    )
                    s = s + bias_ref[0:width, :]
                    s_ref[0:width, :] = s
                    top_ref[...] = jnp.max(s, axis=0, keepdims=True)

                def weights(s_ref, top_ref, p_ref):
                    p_ref[0:width, :] = jnp.exp2(s_ref[0:width, :] - top_ref[...]).astype(
                        jnp.bfloat16
                    )

                def mix(h, p_ref):
                    features = pl.ds(pl.multiple_of(h * VROWS, 16), VROWS)
                    c = jnp.dot(
                        vt_ref[features, keys], p_ref[0:width, :],
                        preferred_element_type=jnp.float32,
                    )
                    ctx_ref[pl.ds(pl.multiple_of(h * SIZE, 16), SIZE), :] = (
                        c[0:SIZE] * (1.0 / c[SIZE : SIZE + 1])
                    ).astype(jnp.bfloat16)

                scores(0, s0_ref, top0_ref)

                def two_heads(i, inner):
                    h = i * 2
                    scores(h + 1, s1_ref, top1_ref)
                    weights(s0_ref, top0_ref, p0_ref)
                    mix(jnp.maximum(h - 1, 0), p1_ref)
                    scores(jnp.minimum(h + 2, HEADS - 1), s0_ref, top0_ref)
                    weights(s1_ref, top1_ref, p1_ref)
                    mix(h, p0_ref)
                    return inner

                lax.fori_loop(0, HEADS // 2, two_heads, 0)
                mix(HEADS - 1, p1_ref)

        mixed = lax.dot_general(
            ctx_ref[...], wo_ref[...], (((0,), (0,)), ((), ())),
            preferred_element_type=jnp.float32,
        )
        hidden = x_ref[rows, :].astype(jnp.float32) + mixed
        at = lax.broadcasted_iota(jnp.int32, (QB, D), 0) + row0
        inside = (at >= lo) & (at < hi)
        hidden = hidden.astype(jnp.bfloat16)
        if edge:
            hid_ref[pl.ds(pl.multiple_of(row0 + SHIFT, SHIFT), QB), :] = jnp.where(
                inside, hidden, jnp.zeros_like(hidden)
            )
        else:
            hid_ref[rows, :] = jnp.where(inside, hidden, hid_ref[rows, :])
        return carry

    lax.fori_loop(0, blocks, attend, 0)

    if edge:
        put = mover(SHIFT - offset)

        @pl.when(hi > 0)
        def _():
            for j in range(3):
                moved_rows = jnp.dot(
                    put, hid_ref[j * QB : (j + 1) * QB + SHIFT, :],
                    preferred_element_type=jnp.float32,
                )
                rows = pl.ds(pl.multiple_of(first + j * QB, SHIFT), QB)
                wide_ref[rows, :] = moved_rows.astype(jnp.bfloat16)

        hprev_ref[...] = wide_ref[0:LOCAL, :]
        hown_ref[...] = hin_ref[...] + wide_ref[LOCAL:WIN, :]
        extra = jnp.dot(
            jnp.ones((8, LOCAL + SHIFT), jnp.bfloat16), hid_ref[0 : LOCAL + SHIFT, :],
            preferred_element_type=jnp.float32,
        )
        label = lax.broadcasted_iota(jnp.int32, (IMAGES, D), 0)
        alone = jnp.where(label == place_ref[6], extra[0:1, :] / lens_ref[...], 0.0)
        pooled_ref[...] = sum_ref[...] + alone.astype(jnp.bfloat16)
        few_ref[...] = jnp.sum(alone, axis=0, keepdims=True).astype(jnp.bfloat16)
        return
    hown_ref[...] = hid_ref[0:LOCAL, :]
    label = lax.broadcasted_iota(jnp.int32, (IMAGES, LOCAL), 0)
    at = lax.broadcasted_iota(jnp.int32, (IMAGES, LOCAL), 1)
    member = (label == image_ref[...]) & (at >= lo) & (at < hi)
    sums = jnp.dot(
        jnp.where(member, 1.0, 0.0).astype(jnp.bfloat16), hid_ref[0:LOCAL, :],
        preferred_element_type=jnp.float32,
    )
    means = (sums / lens_ref[...]).astype(jnp.bfloat16)
    sum_ref[...] = means
    label = lax.broadcasted_iota(jnp.int32, (SLOTS, IMAGES), 0) + place_ref[6]
    pick = lax.broadcasted_iota(jnp.int32, (SLOTS, IMAGES), 1) == label
    few_ref[...] = jnp.dot(
        jnp.where(pick, 1.0, 0.0).astype(jnp.bfloat16), means, preferred_element_type=jnp.float32
    ).astype(jnp.bfloat16)


def unpack_kernel(near_ref, far_ref, near_edge_ref, far_edge_ref, slot_ref, out_ref):
    means = jnp.zeros((IMAGES, D), jnp.float32)
    for row, refs in ((0, (near_ref, far_ref)), (1, (near_edge_ref, far_edge_ref))):
        for i, ref in enumerate(refs):
            count = ref.shape[0]
            at = lax.broadcasted_iota(jnp.int32, (count, IMAGES), 0) + i * count
            pick = jnp.where(slot_ref[row : row + 1, :] == at, 1.0, 0.0).astype(jnp.bfloat16)
            means = means + lax.dot_general(
                pick, ref[...], (((0,), (0,)), ((), ())), preferred_element_type=jnp.float32
            )
    out_ref[...] = means


def unpack(near, far, near_edge, far_edge, slot):
    vmem = pl.BlockSpec(memory_space=pltpu.VMEM)
    return pl.pallas_call(
        unpack_kernel,
        out_shape=jax.ShapeDtypeStruct((IMAGES, D), jnp.float32),
        in_specs=[vmem] * 5,
        out_specs=vmem,
        compiler_params=pltpu.CompilerParams(vmem_limit_bytes=16 * 2**20),
        name="unpack",
    )(near, far, near_edge, far_edge, slot)


def attention(edge, place, spans, inputs, gain, weights, extra):
    hbm = pl.BlockSpec(memory_space=pltpu.HBM)
    vmem = pl.BlockSpec(memory_space=pltpu.VMEM)
    smem = pl.BlockSpec(memory_space=pltpu.SMEM)
    rows = LOCAL + 256
    width = WIDTHS[-1]
    hidden = jax.ShapeDtypeStruct((LOCAL, D), jnp.bfloat16)
    pooled = jax.ShapeDtypeStruct((IMAGES, D), jnp.bfloat16)
    if edge:
        outs = (hidden, hidden, pooled, jax.ShapeDtypeStruct((1, D), jnp.bfloat16))
        tail = [vmem, vmem, vmem]
    else:
        outs = (hidden, pooled, jax.ShapeDtypeStruct((SLOTS, D), jnp.bfloat16))
        tail = [vmem, vmem]
    return pl.pallas_call(
        functools.partial(attention_kernel, edge),
        out_shape=outs,
        in_specs=[smem, smem] + [hbm] * len(inputs) + [vmem] + [hbm] * 22 + [vmem] + tail,
        out_specs=(vmem,) * len(outs),
        scratch_shapes=([pltpu.VMEM((WIN + 3 * QB, D), jnp.bfloat16)] if edge else [])
        + [
            pltpu.VMEM((rows, D), jnp.bfloat16),
            pltpu.VMEM((rows, D), jnp.bfloat16),
            pltpu.VMEM((D, 3 * D), jnp.bfloat16),
            pltpu.VMEM((D, D), jnp.bfloat16),
            pltpu.VMEM((rows, D), jnp.bfloat16),
            pltpu.VMEM((rows, D), jnp.bfloat16),
            pltpu.VMEM((HEADS * VROWS, rows), jnp.bfloat16),
            pltpu.VMEM((D, QB), jnp.bfloat16),
            pltpu.VMEM((width, QB), jnp.float32),
            pltpu.VMEM((rows + 2 * SHIFT, D), jnp.bfloat16),
            pltpu.VMEM((width, QB), jnp.float32),
            pltpu.VMEM((width, QB), jnp.float32),
            pltpu.VMEM((width, QB), jnp.bfloat16),
            pltpu.VMEM((width, QB), jnp.bfloat16),
            pltpu.VMEM((1, QB), jnp.float32),
            pltpu.VMEM((1, QB), jnp.float32),
            pltpu.SemaphoreType.DMA((6,)),
        ],
        compiler_params=pltpu.CompilerParams(vmem_limit_bytes=50 * 2**20),
        cost_estimate=pl.CostEstimate(
            flops=15_000_000_000, bytes_accessed=20_000_000, transcendentals=5_000_000
        ),
        name="edge_attention" if edge else "own_attention",
    )(place, spans, *inputs, gain, *weights, spans, *extra)


def layer(tokens, lengths, ln_gain, w_qkv, w_out):
    x, co, z, yh, dp = (lax.axis_index(a) for a in ALL_AXES)
    shard = (x * 2 + co) * 8 + z * 2 + yh
    own = tokens[0]

    p0, p1 = first_pieces(w_qkv, w_out)
    r0 = moved(p0, Y_UP)
    r1 = moved(p1, Y_DOWN)
    ux, dx = moved(r0, X_UP), moved(r0, X_DOWN)
    uz, dz = moved(r1, Z_UP), moved(r1, Z_DOWN)
    half = KR // 2
    fx, fz = moved(ux[:half], X_UP), moved(uz[:half], Z_UP)
    gx, gz = moved(dx[half:], X_DOWN), moved(dz[half:], Z_DOWN)
    prev = lax.ppermute(own, TOKEN_AXES, [(i, i + 1) for i in range(63)])
    near = [moved(a, CORE) for a in (r0, r1, ux, uz, dx, dz)]
    last = [moved(a, CORE) for a in (fx, fz, gx, gz)]
    mine = [r0, r1, ux, uz, dx, dz, fx, fz, gx, gz]
    other = near + last

    lens = lengths[0]
    ends = jnp.cumsum(lens)
    offsets = ends - lens
    first = (shard - 1) * LOCAL
    at = first + jnp.arange(WIN + 256, dtype=jnp.int32)
    begun = offsets[:, None] <= at[None, :]
    image = jnp.sum(begun.astype(jnp.int32), axis=0) - 1
    start = jnp.max(jnp.where(begun, offsets[:, None], -WIN), axis=0) - first
    end = jnp.min(jnp.where(ends[:, None] > at[None, :], ends[:, None], 1 << 20), axis=0) - first
    spans = jnp.stack([start, end]).astype(jnp.int32)
    low = start[LOCAL]
    cut = jnp.where(low < LOCAL, end[LOCAL], LOCAL)
    limit = jnp.where(end[WIN - 1] == WIN, WIN, start[WIN - 1])
    places = [
        jnp.stack([x, co, dp, lo, hi, z, image[LOCAL]]).astype(jnp.int32)
        for lo, hi in ((low, cut), (cut - LOCAL, limit - LOCAL))
    ]
    owner = (ends - 1) // LOCAL
    leader = jnp.sum((offsets[None, :] <= owner[:, None] * LOCAL).astype(jnp.int32), axis=1) - 1
    rank = jnp.arange(IMAGES, dtype=jnp.int32) - leader
    group = owner // 16 * 8 + owner % 8
    slot = jnp.where(owner // 8 % 2 == co, 0, 32 * SLOTS) + group * SLOTS + rank
    edge_slot = jnp.where(owner // 8 % 2 == co, 0, 32) + group
    slot = jnp.stack([slot, jnp.where(rank == 0, edge_slot, -1)])
    crowded = jnp.full((8, 128), jnp.max(rank) >= SLOTS).astype(jnp.float32)
    elsewhere = lax.ppermute(crowded, "dp", SWAP)
    fits = crowded[0, 0] + elsewhere[0, 0] == 0.0

    gain = ln_gain[None]
    weights = [w_qkv, w_out, *mine, *other]

    column = lens.astype(jnp.float32)[:, None]
    hown, means, few = attention(
        False, places[1], spans[:, LOCAL:] - LOCAL, [own], gain, weights,
        [image[None, LOCAL:WIN], column],
    )
    near = lax.all_to_all(
        jnp.broadcast_to(few[None], (32, SLOTS, D)), GROUP, 0, 0, tiled=True
    ).reshape(32 * SLOTS, D)
    hprev, hown, part, alone = attention(
        True, places[0], spans, [prev, own], gain, weights, [column, hown, means]
    )
    back = lax.ppermute(hprev, TOKEN_AXES, [(i + 1, i) for i in range(63)])
    far = lax.ppermute(near, "co", SWAP)
    near_edge = lax.all_to_all(jnp.broadcast_to(alone, (32, D)), GROUP, 0, 0, tiled=True)
    far_edge = lax.ppermute(near_edge, "co", SWAP)

    def pooled_directly(part):
        return unpack(near, far, near_edge, far_edge, slot)

    def pooled_by_sums(part):
        part = part.reshape(2, IMAGES // 2, D)
        kept = lax.dynamic_index_in_dim(part, co, 0, keepdims=False)
        given = lax.dynamic_index_in_dim(part, 1 - co, 0, keepdims=False)
        given = lax.ppermute(given, "co", SWAP)
        kept = kept.astype(jnp.float32) + given.astype(jnp.float32)
        kept = kept.astype(jnp.bfloat16).reshape(32, 4, D)
        rows = lax.all_to_all(kept, GROUP, 0, 0, tiled=True).astype(jnp.float32)
        rows = jnp.sum(rows, axis=0).astype(jnp.bfloat16)
        half = lax.all_to_all(jnp.broadcast_to(rows[None], (32, 4, D)), GROUP, 0, 0, tiled=True)
        half = half.reshape(IMAGES // 2, D)
        rest = lax.ppermute(half, "co", SWAP)
        pooled = jnp.where(co == 0, jnp.stack([half, rest]), jnp.stack([rest, half]))
        return pooled.reshape(IMAGES, D).astype(jnp.float32)

    pooled = lax.cond(fits, pooled_directly, pooled_by_sums, part)[None]

    here = jnp.arange(LOCAL, dtype=jnp.int32)[:, None] < limit - LOCAL
    hidden = jnp.where(here, hown, back)[None]
    return hidden, pooled


def solution(mesh):
    fine = Mesh(mesh.devices.reshape(4, 2, 4, 2, 2), ALL_AXES)
    in_specs = (P("dp", TOKEN_AXES, None), P("dp", None), P(), P("dp", None), P("dp", None))
    out_specs = (P("dp", TOKEN_AXES, None), P("dp", None, None))
    return jax.shard_map(layer, mesh=fine, in_specs=in_specs, out_specs=out_specs, check_vma=False)
```

```python
import functools
import itertools

import jax
import jax.numpy as jnp
from jax import lax
from jax.experimental import pallas as pl
from jax.experimental.pallas import tpu as pltpu
from jax.sharding import Mesh
from jax.sharding import PartitionSpec as P


HEADS = 16
SIZE = 80
VROWS = 96
D = HEADS * SIZE
LOCAL = 512
WIN = 2 * LOCAL
QB = 256
IMAGES = 256
WIDTHS = (256, 384, 512)
SHIFT = 16
SLOTS = 16
HALF = D // 2
KR = 160
TOKEN_AXES = ("x", "co", "z", "yh")
ALL_AXES = TOKEN_AXES + ("dp",)
GROUP = ("x", "z", "yh")
SWAP = [(0, 1), (1, 0)]
LOG2E = 1.4426950408889634


def permutation(move):
    def index(x, co, z, y):
        return ((x * 2 + co) * 8 + (z * 2 + y // 2)) * 2 + y % 2

    places = itertools.product(range(4), range(2), range(4), range(4))
    return [(index(*place), index(*move(*place))) for place in places]


Y_UP = permutation(lambda x, co, z, y: (x, co, z, (y + 1) % 4))
Y_DOWN = permutation(lambda x, co, z, y: (x, co, z, (y - 1) % 4))
X_UP = permutation(lambda x, co, z, y: ((x + 1) % 4, co, z, y))
X_DOWN = permutation(lambda x, co, z, y: ((x - 1) % 4, co, z, y))
Z_UP = permutation(lambda x, co, z, y: (x, co, (z + 1) % 4, y))
Z_DOWN = permutation(lambda x, co, z, y: (x, co, (z - 1) % 4, y))
CORE = permutation(lambda x, co, z, y: (x, 1 - co, z, y))


WRAPS = [i for i in range(63) if i % 16 == 15]


def moved(piece, pairs):
    return lax.ppermute(piece, ALL_AXES, pairs)


def first_pieces(w_qkv, w_out):
    x, co = lax.axis_index("x"), lax.axis_index("co")
    pieces = []
    for side in range(2):
        part = co * 2 + side
        q = lax.dynamic_slice(w_qkv, (x * KR, jnp.minimum(part, 2) * D), (KR, D))
        o = lax.dynamic_slice(w_out, (x * KR, 0), (KR, D))
        pieces.append(q if side == 0 else jnp.where(co == 0, q, o))
    return pieces


def attention_kernel(edge, place_ref, ends_ref, *refs):
    if edge:
        prev_ref, late_ref, refs = refs[0], refs[1], refs[2:]
    own_ref, gain_ref, wqkv_ref, wout_ref, refs = *refs[:4], refs[4:]
    mine_refs, other_refs, spans_ref, refs = refs[:8], refs[8:16], refs[16], refs[17:]
    if edge:
        hprev_ref, hown_ref, sum_ref, refs = *refs[:3], refs[3:]
    else:
        image_ref, lens_ref, hedge_ref, sum_ref, hown_ref, pooled_ref, few_ref, refs = *refs[:7], refs[7:]
    if edge:
        wide_ref, refs = refs[0], refs[1:]
    (
        x_ref, n_ref, w_ref, wo_ref, q_ref, k_ref, vt_ref, ctx_ref, bias_ref, hid_ref,
        s0_ref, s1_ref, p0_ref, p1_ref, top0_ref, top1_ref, sem,
    ) = refs
    x, co, dp, lo, hi, wrap = (place_ref[i] for i in range(6))
    if edge:
        first = pl.multiple_of(lo // SHIFT * SHIFT, SHIFT)
        offset = lo - first
        base, lo, hi = 0, 0, hi - lo
    else:
        base = (lo // 128) * 128
    blocks = (hi - base + QB - 1) // QB

    far = (1 - dp) * HALF

    tokens_ref = wide_ref if edge else x_ref
    inputs = [
        pltpu.make_async_copy(
            own_ref, tokens_ref.at[pl.ds(LOCAL if edge else 0, LOCAL)], sem.at[0]
        )
    ]
    inputs[0].start()
    if edge:
        inputs.append(pltpu.make_async_copy(prev_ref, wide_ref.at[pl.ds(0, LOCAL)], sem.at[0]))

        @pl.when(wrap == 0)
        def _():
            inputs[1].start()

        @pl.when(wrap == 1)
        def _():
            pltpu.make_async_copy(late_ref, wide_ref.at[pl.ds(0, LOCAL)], sem.at[0]).start()
    else:
        inputs.append(pltpu.make_async_copy(hedge_ref, hid_ref.at[pl.ds(0, LOCAL)], sem.at[5]))
        inputs[1].start()

    def near(part, target, cols):
        return pltpu.make_async_copy(
            wout_ref if part == 3 else wqkv_ref.at[:, cols],
            target.at[pl.ds(pl.multiple_of(dp * HALF, 16), HALF), cols],
            sem.at[1 + part],
        )

    def distant(part, source, row):
        target = wo_ref if part == 3 else w_ref
        rows = pl.ds(pl.multiple_of(far + row * KR, 16), KR)
        return pltpu.make_async_copy(source, target.at[rows, columns[part]], sem.at[1 + part])

    columns = [pl.ds(0, D), pl.ds(D, D), pl.ds(2 * D, D), pl.ds(0, D)]
    targets = [w_ref, w_ref, w_ref, wo_ref]
    shift = (0, 3, 1, 2)
    for part in range(4):
        near(part, targets[part], columns[part]).start()
        for held, core in ((mine_refs, co), (other_refs, 1 - co)):

            @pl.when(core == part // 2)
            def _(held=held, part=part):
                for slot in range(4):
                    row = lax.rem(x + shift[slot], 4)
                    distant(part, held[slot * 2 + part % 2], row).start()

    def arrived(part):
        near(part, targets[part], columns[part]).wait()
        for _ in range(4):
            distant(part, mine_refs[0], 0).wait()

    if not edge:
        x_ref[LOCAL:, :] = jnp.zeros((x_ref.shape[0] - LOCAL, D), jnp.bfloat16)
    for copy in inputs:
        copy.wait()

    def mover(lag):
        out = lax.broadcasted_iota(jnp.int32, (QB, QB + SHIFT), 0)
        source = lax.broadcasted_iota(jnp.int32, (QB, QB + SHIFT), 1)
        return jnp.where(source == out + lag, 1.0, 0.0).astype(jnp.bfloat16)

    if edge:
        wide_ref[WIN:, :] = jnp.zeros((wide_ref.shape[0] - WIN, D), jnp.bfloat16)
        pick = mover(offset)

        def align(j, carry):
            rows = pl.ds(pl.multiple_of(first + j * QB, SHIFT), QB + SHIFT)
            taken = jnp.dot(pick, wide_ref[rows, :], preferred_element_type=jnp.float32)
            x_ref[pl.ds(pl.multiple_of(j * QB, QB), QB), :] = taken.astype(jnp.bfloat16)
            return carry

        lax.fori_loop(0, blocks, align, 0)

    def block_rows(j):
        row0 = pl.multiple_of(base + j * QB, 128)
        return row0, pl.ds(row0, QB)

    def normalize(j, carry):
        _, rows = block_rows(j)
        values = x_ref[rows, :].astype(jnp.float32)
        center = values - jnp.mean(values, axis=1, keepdims=True)
        spread = jnp.mean(center * center, axis=1, keepdims=True)
        normed = center * lax.rsqrt(spread + 1e-05) * gain_ref[...]
        n_ref[rows, :] = normed.astype(jnp.bfloat16)
        return carry

    lax.fori_loop(0, blocks, normalize, 0)
    k_ref[...] = jnp.zeros_like(k_ref)
    vt_ref[...] = jnp.zeros_like(vt_ref)
    if edge:
        hid_ref[...] = jnp.zeros_like(hid_ref)
        wide_ref[...] = jnp.zeros_like(wide_ref)

    def project_q(j, carry):
        _, rows = block_rows(j)
        q = jnp.dot(n_ref[rows, :], w_ref[:, 0:D], preferred_element_type=jnp.float32)
        q_ref[rows, :] = (q * (LOG2E * SIZE**-0.5)).astype(jnp.bfloat16)
        return carry

    def project_k(j, carry):
        _, rows = block_rows(j)
        k = jnp.dot(n_ref[rows, :], w_ref[:, D : 2 * D], preferred_element_type=jnp.float32)
        k_ref[rows, :] = k.astype(jnp.bfloat16)
        return carry

    def project_v(j, carry):
        _, rows = block_rows(j)
        v = jnp.dot(n_ref[rows, :], w_ref[:, 2 * D :], preferred_element_type=jnp.float32)
        vt = v.T.astype(jnp.bfloat16)
        for h in range(HEADS):
            vt_ref[pl.ds(h * VROWS, SIZE), rows] = vt[h * SIZE : (h + 1) * SIZE]
            vt_ref[pl.ds(h * VROWS + SIZE, VROWS - SIZE), rows] = jnp.ones(
                (VROWS - SIZE, QB), jnp.bfloat16
            )
        return carry

    for part, project in enumerate((project_q, project_k, project_v)):
        arrived(part)
        lax.fori_loop(0, blocks, project, 0)
    arrived(3)

    def attend(j, carry):
        row0, rows = block_rows(j)
        if edge:
            k0, need = 0, hi
            start, end = 0, hi
        else:
            least = ends_ref[0, jnp.maximum(row0, lo)]
            most = ends_ref[1, jnp.minimum(row0 + QB, hi) - 1]
            k0 = pl.multiple_of((least // 128) * 128, 128)
            need = most - k0
            start = spans_ref[0:1, rows]
            end = spans_ref[1:2, rows]
        for i, width in enumerate(WIDTHS):
            above = WIDTHS[i - 1] if i else 0

            @pl.when((need > above) & (need <= width))
            def _(width=width):
                keys = pl.ds(k0, width)
                at = lax.broadcasted_iota(jnp.int32, (width, QB), 0) + k0
                bias_ref[0:width, :] = jnp.where((at >= start) & (at < end), 0.0, -1e30)

                def scores(h, s_ref, top_ref):
                    w0 = pl.multiple_of(jnp.minimum((h * SIZE) // 128 * 128, D - 256), 128)
                    lanes = pl.ds(w0, 256)
                    lane = lax.broadcasted_iota(jnp.int32, (1, 256), 1) + (w0 - h * SIZE)
                    inside = jnp.where((lane >= 0) & (lane < SIZE), 1.0, 0.0)
                    q = q_ref[rows, lanes] * inside.astype(jnp.bfloat16)
                    s = lax.dot_general(
                        k_ref[keys, lanes], q, (((1,), (1,)), ((), ())),
                        preferred_element_type=jnp.float32,
                    )
                    s = s + bias_ref[0:width, :]
                    s_ref[0:width, :] = s
                    top_ref[...] = jnp.max(s, axis=0, keepdims=True)

                def weights(s_ref, top_ref, p_ref):
                    p_ref[0:width, :] = jnp.exp2(s_ref[0:width, :] - top_ref[...]).astype(
                        jnp.bfloat16
                    )

                def mix(h, p_ref):
                    features = pl.ds(pl.multiple_of(h * VROWS, 16), VROWS)
                    c = jnp.dot(
                        vt_ref[features, keys], p_ref[0:width, :],
                        preferred_element_type=jnp.float32,
                    )
                    ctx_ref[pl.ds(pl.multiple_of(h * SIZE, 16), SIZE), :] = (
                        c[0:SIZE] * (1.0 / c[SIZE : SIZE + 1])
                    ).astype(jnp.bfloat16)

                scores(0, s0_ref, top0_ref)

                def two_heads(i, inner):
                    h = i * 2
                    scores(h + 1, s1_ref, top1_ref)
                    weights(s0_ref, top0_ref, p0_ref)
                    mix(jnp.maximum(h - 1, 0), p1_ref)
                    scores(jnp.minimum(h + 2, HEADS - 1), s0_ref, top0_ref)
                    weights(s1_ref, top1_ref, p1_ref)
                    mix(h, p0_ref)
                    return inner

                lax.fori_loop(0, HEADS // 2, two_heads, 0)
                mix(HEADS - 1, p1_ref)

        mixed = lax.dot_general(
            ctx_ref[...], wo_ref[...], (((0,), (0,)), ((), ())),
            preferred_element_type=jnp.float32,
        )
        hidden = x_ref[rows, :].astype(jnp.float32) + mixed
        at = lax.broadcasted_iota(jnp.int32, (QB, D), 0) + row0
        inside = (at >= lo) & (at < hi)
        hidden = hidden.astype(jnp.bfloat16)
        if edge:
            hid_ref[pl.ds(pl.multiple_of(row0 + SHIFT, SHIFT), QB), :] = jnp.where(
                inside, hidden, jnp.zeros_like(hidden)
            )
        else:
            hid_ref[rows, :] = jnp.where(inside, hidden, hid_ref[rows, :])
        return carry

    lax.fori_loop(0, blocks, attend, 0)

    if edge:
        put = mover(SHIFT - offset)

        @pl.when(hi > 0)
        def _():
            for j in range(3):
                moved_rows = jnp.dot(
                    put, hid_ref[j * QB : (j + 1) * QB + SHIFT, :],
                    preferred_element_type=jnp.float32,
                )
                rows = pl.ds(pl.multiple_of(first + j * QB, SHIFT), QB)
                wide_ref[rows, :] = moved_rows.astype(jnp.bfloat16)

        hprev_ref[...] = wide_ref[0:LOCAL, :]
        hown_ref[...] = wide_ref[LOCAL:WIN, :]
        sum_ref[...] = jnp.dot(
            jnp.ones((8, LOCAL + SHIFT), jnp.bfloat16), hid_ref[0 : LOCAL + SHIFT, :],
            preferred_element_type=jnp.float32,
        )
        return
    hown_ref[...] = hid_ref[0:LOCAL, :]
    label = lax.broadcasted_iota(jnp.int32, (IMAGES, LOCAL), 0)
    at = lax.broadcasted_iota(jnp.int32, (IMAGES, LOCAL), 1)
    member = (label == image_ref[...]) & (at >= lo) & (at < hi)
    sums = jnp.dot(
        jnp.where(member, 1.0, 0.0).astype(jnp.bfloat16), hid_ref[0:LOCAL, :],
        preferred_element_type=jnp.float32,
    )
    label = lax.broadcasted_iota(jnp.int32, (IMAGES, D), 0)
    sums = sums + jnp.where(label == place_ref[6], sum_ref[0:1, :], 0.0)
    means = (sums / lens_ref[...]).astype(jnp.bfloat16)
    pooled_ref[...] = means
    label = lax.broadcasted_iota(jnp.int32, (SLOTS, IMAGES), 0) + place_ref[6]
    pick = lax.broadcasted_iota(jnp.int32, (SLOTS, IMAGES), 1) == label
    few_ref[...] = jnp.dot(
        jnp.where(pick, 1.0, 0.0).astype(jnp.bfloat16), means, preferred_element_type=jnp.float32
    ).astype(jnp.bfloat16)


def unpack_kernel(near_ref, far_ref, slot_ref, out_ref):
    at = lax.broadcasted_iota(jnp.int32, (32 * SLOTS, IMAGES), 0)
    means = jnp.zeros((IMAGES, D), jnp.float32)
    for i, ref in enumerate((near_ref, far_ref)):
        pick = jnp.where(slot_ref[...] == at + i * 32 * SLOTS, 1.0, 0.0).astype(jnp.bfloat16)
        means = means + lax.dot_general(
            pick, ref[...], (((0,), (0,)), ((), ())), preferred_element_type=jnp.float32
        )
    out_ref[...] = means


def unpack(near, far, slot):
    vmem = pl.BlockSpec(memory_space=pltpu.VMEM)
    return pl.pallas_call(
        unpack_kernel,
        out_shape=jax.ShapeDtypeStruct((IMAGES, D), jnp.float32),
        in_specs=[vmem] * 3,
        out_specs=vmem,
        compiler_params=pltpu.CompilerParams(vmem_limit_bytes=16 * 2**20),
        name="unpack",
    )(near, far, slot)


def attention(edge, place, spans, inputs, gain, weights, extra):
    hbm = pl.BlockSpec(memory_space=pltpu.HBM)
    vmem = pl.BlockSpec(memory_space=pltpu.VMEM)
    smem = pl.BlockSpec(memory_space=pltpu.SMEM)
    rows = LOCAL + 256
    width = WIDTHS[-1]
    hidden = jax.ShapeDtypeStruct((LOCAL, D), jnp.bfloat16)
    if edge:
        outs = (hidden, hidden, jax.ShapeDtypeStruct((8, D), jnp.float32))
        tail = []
    else:
        outs = (
            hidden,
            jax.ShapeDtypeStruct((IMAGES, D), jnp.bfloat16),
            jax.ShapeDtypeStruct((SLOTS, D), jnp.bfloat16),
        )
        tail = [vmem, vmem, hbm, vmem]
    return pl.pallas_call(
        functools.partial(attention_kernel, edge),
        out_shape=outs,
        in_specs=[smem, smem] + [hbm] * len(inputs) + [vmem] + [hbm] * 18 + [vmem] + tail,
        out_specs=(vmem,) * len(outs),
        scratch_shapes=([pltpu.VMEM((WIN + 3 * QB, D), jnp.bfloat16)] if edge else [])
        + [
            pltpu.VMEM((rows, D), jnp.bfloat16),
            pltpu.VMEM((rows, D), jnp.bfloat16),
            pltpu.VMEM((D, 3 * D), jnp.bfloat16),
            pltpu.VMEM((D, D), jnp.bfloat16),
            pltpu.VMEM((rows, D), jnp.bfloat16),
            pltpu.VMEM((rows, D), jnp.bfloat16),
            pltpu.VMEM((HEADS * VROWS, rows), jnp.bfloat16),
            pltpu.VMEM((D, QB), jnp.bfloat16),
            pltpu.VMEM((width, QB), jnp.float32),
            pltpu.VMEM((rows + 2 * SHIFT, D), jnp.bfloat16),
            pltpu.VMEM((width, QB), jnp.float32),
            pltpu.VMEM((width, QB), jnp.float32),
            pltpu.VMEM((width, QB), jnp.bfloat16),
            pltpu.VMEM((width, QB), jnp.bfloat16),
            pltpu.VMEM((1, QB), jnp.float32),
            pltpu.VMEM((1, QB), jnp.float32),
            pltpu.SemaphoreType.DMA((6,)),
        ],
        compiler_params=pltpu.CompilerParams(vmem_limit_bytes=50 * 2**20),
        cost_estimate=pl.CostEstimate(
            flops=15_000_000_000, bytes_accessed=20_000_000, transcendentals=5_000_000
        ),
        name="edge_attention" if edge else "own_attention",
    )(place, spans, *inputs, gain, *weights, spans, *extra)


def layer(tokens, lengths, ln_gain, w_qkv, w_out):
    x, co, z, yh, dp = (lax.axis_index(a) for a in ALL_AXES)
    shard = (x * 2 + co) * 8 + z * 2 + yh
    own = tokens[0]

    p0, p1 = first_pieces(w_qkv, w_out)
    lent = lax.ppermute(own, TOKEN_AXES, [(i, i + 8) for i in WRAPS])
    r0 = moved(p0, Y_UP)
    r1 = moved(p1, Y_DOWN)
    prev = lax.ppermute(own, TOKEN_AXES, [(i, i + 1) for i in range(63) if i not in WRAPS])
    u0 = moved(r0, X_UP)
    d1 = moved(r1, X_DOWN)
    late = lax.ppermute(lent, TOKEN_AXES, [(i + 8, i + 1) for i in WRAPS])
    u1 = moved(r1, X_UP)
    d0 = moved(r0, X_DOWN)
    f0 = moved(u0, X_UP)
    f1 = moved(d1, X_DOWN)
    near = [moved(a, CORE) for a in (r0, r1)]
    ring = [moved(a, CORE) for a in (u0, u1, d0, d1)]
    last = [moved(a, CORE) for a in (f0, f1)]
    mine = [r0, r1, u0, u1, d0, d1, f0, f1]
    other = near + ring + last

    lens = lengths[0]
    ends = jnp.cumsum(lens)
    offsets = ends - lens
    first = (shard - 1) * LOCAL
    at = first + jnp.arange(WIN + 256, dtype=jnp.int32)
    begun = offsets[:, None] <= at[None, :]
    image = jnp.sum(begun.astype(jnp.int32), axis=0) - 1
    start = jnp.max(jnp.where(begun, offsets[:, None], -WIN), axis=0) - first
    end = jnp.min(jnp.where(ends[:, None] > at[None, :], ends[:, None], 1 << 20), axis=0) - first
    spans = jnp.stack([start, end]).astype(jnp.int32)
    low = start[LOCAL]
    cut = jnp.where(low < LOCAL, end[LOCAL], LOCAL)
    limit = jnp.where(end[WIN - 1] == WIN, WIN, start[WIN - 1])
    wrap = (co + z + yh == 0) & (x > 0)
    places = [
        jnp.stack([x, co, dp, lo, hi, wrap, image[LOCAL]]).astype(jnp.int32)
        for lo, hi in ((low, cut), (cut - LOCAL, limit - LOCAL))
    ]
    owner = (ends - 1) // LOCAL
    leader = jnp.sum((offsets[None, :] <= owner[:, None] * LOCAL).astype(jnp.int32), axis=1) - 1
    rank = jnp.arange(IMAGES, dtype=jnp.int32) - leader
    group = owner // 16 * 8 + owner % 8
    slot = jnp.where(owner // 8 % 2 == co, 0, 32 * SLOTS) + group * SLOTS + rank
    slot = slot[None]
    crowded = jnp.full((8, 128), jnp.max(rank) >= SLOTS).astype(jnp.float32)
    elsewhere = lax.ppermute(crowded, "dp", SWAP)
    fits = crowded[0, 0] + elsewhere[0, 0] == 0.0

    gain = ln_gain[None]
    weights = [w_qkv, w_out, *mine, *other]

    hprev, hedge, total = attention(True, places[0], spans, [prev, late, own], gain, weights, [])
    back = lax.ppermute(hprev, TOKEN_AXES, [(i + 1, i) for i in range(63)])
    hown, part, few = attention(
        False, places[1], spans[:, LOCAL:] - LOCAL, [own], gain, weights,
        [image[None, LOCAL:WIN], lens.astype(jnp.float32)[:, None], hedge, total],
    )

    def pooled_directly(few, part):
        near = lax.all_to_all(
            jnp.broadcast_to(few[None], (32, SLOTS, D)), GROUP, 0, 0, tiled=True
        ).reshape(32 * SLOTS, D)
        far = lax.ppermute(near, "co", SWAP)
        return unpack(near, far, slot)

    def pooled_by_sums(few, part):
        part = part.reshape(2, IMAGES // 2, D)
        kept = lax.dynamic_index_in_dim(part, co, 0, keepdims=False)
        given = lax.dynamic_index_in_dim(part, 1 - co, 0, keepdims=False)
        given = lax.ppermute(given, "co", SWAP)
        kept = kept.astype(jnp.float32) + given.astype(jnp.float32)
        kept = kept.astype(jnp.bfloat16).reshape(32, 4, D)
        rows = lax.all_to_all(kept, GROUP, 0, 0, tiled=True).astype(jnp.float32)
        rows = jnp.sum(rows, axis=0).astype(jnp.bfloat16)
        half = lax.all_to_all(jnp.broadcast_to(rows[None], (32, 4, D)), GROUP, 0, 0, tiled=True)
        half = half.reshape(IMAGES // 2, D)
        rest = lax.ppermute(half, "co", SWAP)
        pooled = jnp.where(co == 0, jnp.stack([half, rest]), jnp.stack([rest, half]))
        return pooled.reshape(IMAGES, D).astype(jnp.float32)

    pooled = lax.cond(fits, pooled_directly, pooled_by_sums, few, part)[None]

    here = jnp.arange(LOCAL, dtype=jnp.int32)[:, None] < limit - LOCAL
    hidden = jnp.where(here, hown, back)[None]
    return hidden, pooled


def solution(mesh):
    fine = Mesh(mesh.devices.reshape(4, 2, 4, 2, 2), ALL_AXES)
    in_specs = (P("dp", TOKEN_AXES, None), P("dp", None), P(), P("dp", None), P("dp", None))
    out_specs = (P("dp", TOKEN_AXES, None), P("dp", None, None))
    return jax.shard_map(layer, mesh=fine, in_specs=in_specs, out_specs=out_specs, check_vma=False)
```

```python
import functools
import itertools

import jax
import jax.numpy as jnp
from jax import lax
from jax.experimental import pallas as pl
from jax.experimental.pallas import tpu as pltpu
from jax.sharding import Mesh
from jax.sharding import PartitionSpec as P


HEADS = 16
SIZE = 80
VROWS = 96
D = HEADS * SIZE
LOCAL = 512
WIN = 2 * LOCAL
QB = 256
IMAGES = 256
WIDTHS = (256, 384, 512)
SHIFT = 16
SLOTS = 16
HALF = D // 2
KR = 160
TOKEN_AXES = ("x", "co", "z", "yh")
ALL_AXES = TOKEN_AXES + ("dp",)
GROUP = ("x", "z", "yh")
SWAP = [(0, 1), (1, 0)]
LOG2E = 1.4426950408889634


def permutation(move):
    def index(x, co, z, y):
        return ((x * 2 + co) * 8 + (z * 2 + y // 2)) * 2 + y % 2

    places = itertools.product(range(4), range(2), range(4), range(4))
    return [(index(*place), index(*move(*place))) for place in places]


Y_UP = permutation(lambda x, co, z, y: (x, co, z, (y + 1) % 4))
Y_DOWN = permutation(lambda x, co, z, y: (x, co, z, (y - 1) % 4))
X_UP = permutation(lambda x, co, z, y: ((x + 1) % 4, co, z, y))
X_DOWN = permutation(lambda x, co, z, y: ((x - 1) % 4, co, z, y))
Z_UP = permutation(lambda x, co, z, y: (x, co, (z + 1) % 4, y))
Z_DOWN = permutation(lambda x, co, z, y: (x, co, (z - 1) % 4, y))
CORE = permutation(lambda x, co, z, y: (x, 1 - co, z, y))


WRAPS = [i for i in range(63) if i % 16 == 15]


def moved(piece, pairs):
    return lax.ppermute(piece, ALL_AXES, pairs)


def first_pieces(w_qkv, w_out):
    x, co = lax.axis_index("x"), lax.axis_index("co")
    pieces = []
    for side in range(2):
        part = co * 2 + side
        q = lax.dynamic_slice(w_qkv, (x * KR, jnp.minimum(part, 2) * D), (KR, D))
        o = lax.dynamic_slice(w_out, (x * KR, 0), (KR, D))
        pieces.append(q if side == 0 else jnp.where(co == 0, q, o))
    return pieces


def attention_kernel(edge, place_ref, ends_ref, *refs):
    if edge:
        prev_ref, late_ref, refs = refs[0], refs[1], refs[2:]
    own_ref, gain_ref, wqkv_ref, wout_ref, refs = *refs[:4], refs[4:]
    mine_refs, other_refs, spans_ref, refs = refs[:8], refs[8:16], refs[16], refs[17:]
    if edge:
        hprev_ref, hown_ref, sum_ref, refs = *refs[:3], refs[3:]
    else:
        image_ref, lens_ref, hedge_ref, sum_ref, hown_ref, pooled_ref, few_ref, refs = *refs[:7], refs[7:]
    if edge:
        wide_ref, refs = refs[0], refs[1:]
    (
        x_ref, n_ref, w_ref, wo_ref, q_ref, k_ref, vt_ref, ctx_ref, bias_ref, hid_ref,
        s0_ref, s1_ref, p0_ref, p1_ref, top0_ref, top1_ref, sem,
    ) = refs
    x, co, dp, lo, hi, wrap = (place_ref[i] for i in range(6))
    if edge:
        first = pl.multiple_of(lo // SHIFT * SHIFT, SHIFT)
        offset = lo - first
        base, lo, hi = 0, 0, hi - lo
    else:
        base = (lo // 128) * 128
    blocks = (hi - base + QB - 1) // QB

    far = (1 - dp) * HALF

    tokens_ref = wide_ref if edge else x_ref
    inputs = [
        pltpu.make_async_copy(
            own_ref, tokens_ref.at[pl.ds(LOCAL if edge else 0, LOCAL)], sem.at[0]
        )
    ]
    inputs[0].start()
    if edge:
        inputs.append(pltpu.make_async_copy(prev_ref, wide_ref.at[pl.ds(0, LOCAL)], sem.at[0]))

        @pl.when(wrap == 0)
        def _():
            inputs[1].start()

        @pl.when(wrap == 1)
        def _():
            pltpu.make_async_copy(late_ref, wide_ref.at[pl.ds(0, LOCAL)], sem.at[0]).start()
    else:
        edge_rows = pltpu.make_async_copy(hedge_ref, hid_ref.at[pl.ds(0, LOCAL)], sem.at[5])

    def near(part, target, cols):
        return pltpu.make_async_copy(
            wout_ref if part == 3 else wqkv_ref.at[:, cols],
            target.at[pl.ds(pl.multiple_of(dp * HALF, 16), HALF), cols],
            sem.at[1 + part],
        )

    def distant(part, source, row):
        target = wo_ref if part == 3 else w_ref
        rows = pl.ds(pl.multiple_of(far + row * KR, 16), KR)
        return pltpu.make_async_copy(source, target.at[rows, columns[part]], sem.at[1 + part])

    columns = [pl.ds(0, D), pl.ds(D, D), pl.ds(2 * D, D), pl.ds(0, D)]
    targets = [w_ref, w_ref, w_ref, wo_ref]
    shift = (0, 3, 1, 2)
    for part in range(4):
        near(part, targets[part], columns[part]).start()
        for held, core in ((mine_refs, co), (other_refs, 1 - co)):

            @pl.when(core == part // 2)
            def _(held=held, part=part):
                for slot in range(4):
                    row = lax.rem(x + shift[slot], 4)
                    distant(part, held[slot * 2 + part % 2], row).start()

    if not edge:
        edge_rows.start()

    def arrived(part):
        near(part, targets[part], columns[part]).wait()
        for _ in range(4):
            distant(part, mine_refs[0], 0).wait()

    if not edge:
        x_ref[LOCAL:, :] = jnp.zeros((x_ref.shape[0] - LOCAL, D), jnp.bfloat16)
    for copy in inputs:
        copy.wait()

    def mover(lag):
        out = lax.broadcasted_iota(jnp.int32, (QB, QB + SHIFT), 0)
        source = lax.broadcasted_iota(jnp.int32, (QB, QB + SHIFT), 1)
        return jnp.where(source == out + lag, 1.0, 0.0).astype(jnp.bfloat16)

    if edge:
        wide_ref[WIN : WIN + QB, :] = jnp.zeros((QB, D), jnp.bfloat16)
        pick = mover(offset)

        def align(j, carry):
            rows = pl.ds(pl.multiple_of(first + j * QB, SHIFT), QB + SHIFT)
            taken = jnp.dot(pick, wide_ref[rows, :], preferred_element_type=jnp.float32)
            x_ref[pl.ds(pl.multiple_of(j * QB, QB), QB), :] = taken.astype(jnp.bfloat16)
            return carry

        lax.fori_loop(0, blocks, align, 0)

    def block_rows(j):
        row0 = pl.multiple_of(base + j * QB, 128)
        return row0, pl.ds(row0, QB)

    def normalize(j, carry):
        _, rows = block_rows(j)
        values = x_ref[rows, :].astype(jnp.float32)
        center = values - jnp.mean(values, axis=1, keepdims=True)
        spread = jnp.mean(center * center, axis=1, keepdims=True)
        normed = center * lax.rsqrt(spread + 1e-05) * gain_ref[...]
        n_ref[rows, :] = normed.astype(jnp.bfloat16)
        return carry

    lax.fori_loop(0, blocks, normalize, 0)
    past = pl.ds(pl.multiple_of(jnp.minimum(base + blocks * QB, LOCAL), 128), QB)
    k_ref[past, :] = jnp.zeros((QB, D), jnp.bfloat16)
    vt_ref[:, past] = jnp.zeros((HEADS * VROWS, QB), jnp.bfloat16)
    if edge:
        hid_ref[...] = jnp.zeros_like(hid_ref)
        wide_ref[0:WIN, :] = jnp.zeros((WIN, D), jnp.bfloat16)

    def project_q(j, carry):
        _, rows = block_rows(j)
        q = jnp.dot(n_ref[rows, :], w_ref[:, 0:D], preferred_element_type=jnp.float32)
        q_ref[rows, :] = (q * (LOG2E * SIZE**-0.5)).astype(jnp.bfloat16)
        return carry

    def project_k(j, carry):
        _, rows = block_rows(j)
        k = jnp.dot(n_ref[rows, :], w_ref[:, D : 2 * D], preferred_element_type=jnp.float32)
        k_ref[rows, :] = k.astype(jnp.bfloat16)
        return carry

    def project_v(j, carry):
        _, rows = block_rows(j)
        v = jnp.dot(n_ref[rows, :], w_ref[:, 2 * D :], preferred_element_type=jnp.float32)
        vt = v.T.astype(jnp.bfloat16)
        for h in range(HEADS):
            vt_ref[pl.ds(h * VROWS, SIZE), rows] = vt[h * SIZE : (h + 1) * SIZE]
            vt_ref[pl.ds(h * VROWS + SIZE, VROWS - SIZE), rows] = jnp.ones(
                (VROWS - SIZE, QB), jnp.bfloat16
            )
        return carry

    for part, project in enumerate((project_q, project_k, project_v)):
        arrived(part)
        lax.fori_loop(0, blocks, project, 0)
    arrived(3)
    if not edge:
        edge_rows.wait()

    def attend(j, carry):
        row0, rows = block_rows(j)
        if edge:
            k0, need = 0, hi
            start, end = 0, hi
        else:
            least = ends_ref[0, jnp.maximum(row0, lo)]
            most = ends_ref[1, jnp.minimum(row0 + QB, hi) - 1]
            k0 = pl.multiple_of((least // 128) * 128, 128)
            need = most - k0
            start = spans_ref[0:1, rows]
            end = spans_ref[1:2, rows]
        for i, width in enumerate(WIDTHS):
            above = WIDTHS[i - 1] if i else 0

            @pl.when((need > above) & (need <= width))
            def _(width=width):
                keys = pl.ds(k0, width)
                at = lax.broadcasted_iota(jnp.int32, (width, QB), 0) + k0
                bias_ref[0:width, :] = jnp.where((at >= start) & (at < end), 0.0, -1e30)

                def scores(h, s_ref, top_ref):
                    w0 = pl.multiple_of(jnp.minimum((h * SIZE) // 128 * 128, D - 256), 128)
                    lanes = pl.ds(w0, 256)
                    lane = lax.broadcasted_iota(jnp.int32, (1, 256), 1) + (w0 - h * SIZE)
                    inside = jnp.where((lane >= 0) & (lane < SIZE), 1.0, 0.0)
                    q = q_ref[rows, lanes] * inside.astype(jnp.bfloat16)
                    s = lax.dot_general(
                        k_ref[keys, lanes], q, (((1,), (1,)), ((), ())),
                        preferred_element_type=jnp.float32,
                    )
                    s = s + bias_ref[0:width, :]
                    s_ref[0:width, :] = s
                    top_ref[...] = jnp.max(s, axis=0, keepdims=True)

                def weights(s_ref, top_ref, p_ref):
                    p_ref[0:width, :] = jnp.exp2(s_ref[0:width, :] - top_ref[...]).astype(
                        jnp.bfloat16
                    )

                def mix(h, p_ref):
                    features = pl.ds(pl.multiple_of(h * VROWS, 16), VROWS)
                    c = jnp.dot(
                        vt_ref[features, keys], p_ref[0:width, :],
                        preferred_element_type=jnp.float32,
                    )
                    ctx_ref[pl.ds(pl.multiple_of(h * SIZE, 16), SIZE), :] = (
                        c[0:SIZE] * (1.0 / c[SIZE : SIZE + 1])
                    ).astype(jnp.bfloat16)

                scores(0, s0_ref, top0_ref)

                def two_heads(i, inner):
                    h = i * 2
                    scores(h + 1, s1_ref, top1_ref)
                    weights(s0_ref, top0_ref, p0_ref)
                    mix(jnp.maximum(h - 1, 0), p1_ref)
                    scores(jnp.minimum(h + 2, HEADS - 1), s0_ref, top0_ref)
                    weights(s1_ref, top1_ref, p1_ref)
                    mix(h, p0_ref)
                    return inner

                lax.fori_loop(0, HEADS // 2, two_heads, 0, unroll=4)
                mix(HEADS - 1, p1_ref)

        mixed = lax.dot_general(
            ctx_ref[...], wo_ref[...], (((0,), (0,)), ((), ())),
            preferred_element_type=jnp.float32,
        )
        hidden = x_ref[rows, :].astype(jnp.float32) + mixed
        at = lax.broadcasted_iota(jnp.int32, (QB, D), 0) + row0
        inside = (at >= lo) & (at < hi)
        hidden = hidden.astype(jnp.bfloat16)
        if edge:
            hid_ref[pl.ds(pl.multiple_of(row0 + SHIFT, SHIFT), QB), :] = jnp.where(
                inside, hidden, jnp.zeros_like(hidden)
            )
        else:
            hid_ref[rows, :] = jnp.where(inside, hidden, hid_ref[rows, :])
        return carry

    lax.fori_loop(0, blocks, attend, 0)

    if edge:
        put = mover(SHIFT - offset)

        @pl.when(hi > 0)
        def _():
            for j in range(3):
                moved_rows = jnp.dot(
                    put, hid_ref[j * QB : (j + 1) * QB + SHIFT, :],
                    preferred_element_type=jnp.float32,
                )
                rows = pl.ds(pl.multiple_of(first + j * QB, SHIFT), QB)
                wide_ref[rows, :] = moved_rows.astype(jnp.bfloat16)

        hprev_ref[...] = wide_ref[0:LOCAL, :]
        hown_ref[...] = wide_ref[LOCAL:WIN, :]
        sum_ref[...] = jnp.dot(
            jnp.ones((8, LOCAL + SHIFT), jnp.bfloat16), hid_ref[0 : LOCAL + SHIFT, :],
            preferred_element_type=jnp.float32,
        )
        return
    hown_ref[...] = hid_ref[0:LOCAL, :]
    label = lax.broadcasted_iota(jnp.int32, (IMAGES, LOCAL), 0)
    at = lax.broadcasted_iota(jnp.int32, (IMAGES, LOCAL), 1)
    member = (label == image_ref[...]) & (at >= lo) & (at < hi)
    sums = jnp.dot(
        jnp.where(member, 1.0, 0.0).astype(jnp.bfloat16), hid_ref[0:LOCAL, :],
        preferred_element_type=jnp.float32,
    )
    label = lax.broadcasted_iota(jnp.int32, (IMAGES, D), 0)
    sums = sums + jnp.where(label == place_ref[6], sum_ref[0:1, :], 0.0)
    means = (sums / lens_ref[...]).astype(jnp.bfloat16)
    pooled_ref[...] = means
    label = lax.broadcasted_iota(jnp.int32, (SLOTS, IMAGES), 0) + place_ref[6]
    pick = lax.broadcasted_iota(jnp.int32, (SLOTS, IMAGES), 1) == label
    few_ref[...] = jnp.dot(
        jnp.where(pick, 1.0, 0.0).astype(jnp.bfloat16), means, preferred_element_type=jnp.float32
    ).astype(jnp.bfloat16)


def unpack_kernel(near_ref, far_ref, slot_ref, out_ref):
    at = lax.broadcasted_iota(jnp.int32, (32 * SLOTS, IMAGES), 0)
    means = jnp.zeros((IMAGES, D), jnp.float32)
    for i, ref in enumerate((near_ref, far_ref)):
        pick = jnp.where(slot_ref[...] == at + i * 32 * SLOTS, 1.0, 0.0).astype(jnp.bfloat16)
        means = means + lax.dot_general(
            pick, ref[...], (((0,), (0,)), ((), ())), preferred_element_type=jnp.float32
        )
    out_ref[...] = means


def unpack(near, far, slot):
    vmem = pl.BlockSpec(memory_space=pltpu.VMEM)
    return pl.pallas_call(
        unpack_kernel,
        out_shape=jax.ShapeDtypeStruct((IMAGES, D), jnp.float32),
        in_specs=[vmem] * 3,
        out_specs=vmem,
        compiler_params=pltpu.CompilerParams(vmem_limit_bytes=16 * 2**20),
        name="unpack",
    )(near, far, slot)


def attention(edge, place, spans, inputs, gain, weights, extra):
    hbm = pl.BlockSpec(memory_space=pltpu.HBM)
    vmem = pl.BlockSpec(memory_space=pltpu.VMEM)
    smem = pl.BlockSpec(memory_space=pltpu.SMEM)
    rows = LOCAL + 256
    width = WIDTHS[-1]
    hidden = jax.ShapeDtypeStruct((LOCAL, D), jnp.bfloat16)
    if edge:
        outs = (hidden, hidden, jax.ShapeDtypeStruct((8, D), jnp.float32))
        tail = []
    else:
        outs = (
            hidden,
            jax.ShapeDtypeStruct((IMAGES, D), jnp.bfloat16),
            jax.ShapeDtypeStruct((SLOTS, D), jnp.bfloat16),
        )
        tail = [vmem, vmem, hbm, vmem]
    return pl.pallas_call(
        functools.partial(attention_kernel, edge),
        out_shape=outs,
        in_specs=[smem, smem] + [hbm] * len(inputs) + [vmem] + [hbm] * 18 + [vmem] + tail,
        out_specs=(vmem,) * len(outs),
        scratch_shapes=([pltpu.VMEM((WIN + 3 * QB, D), jnp.bfloat16)] if edge else [])
        + [
            pltpu.VMEM((rows, D), jnp.bfloat16),
            pltpu.VMEM((rows, D), jnp.bfloat16),
            pltpu.VMEM((D, 3 * D), jnp.bfloat16),
            pltpu.VMEM((D, D), jnp.bfloat16),
            pltpu.VMEM((rows, D), jnp.bfloat16),
            pltpu.VMEM((rows, D), jnp.bfloat16),
            pltpu.VMEM((HEADS * VROWS, rows), jnp.bfloat16),
            pltpu.VMEM((D, QB), jnp.bfloat16),
            pltpu.VMEM((width, QB), jnp.float32),
            pltpu.VMEM((rows + 2 * SHIFT, D), jnp.bfloat16),
            pltpu.VMEM((width, QB), jnp.float32),
            pltpu.VMEM((width, QB), jnp.float32),
            pltpu.VMEM((width, QB), jnp.bfloat16),
            pltpu.VMEM((width, QB), jnp.bfloat16),
            pltpu.VMEM((1, QB), jnp.float32),
            pltpu.VMEM((1, QB), jnp.float32),
            pltpu.SemaphoreType.DMA((6,)),
        ],
        compiler_params=pltpu.CompilerParams(vmem_limit_bytes=50 * 2**20),
        cost_estimate=pl.CostEstimate(
            flops=15_000_000_000, bytes_accessed=20_000_000, transcendentals=5_000_000
        ),
        name="edge_attention" if edge else "own_attention",
    )(place, spans, *inputs, gain, *weights, spans, *extra)


def layer(tokens, lengths, ln_gain, w_qkv, w_out):
    x, co, z, yh, dp = (lax.axis_index(a) for a in ALL_AXES)
    shard = (x * 2 + co) * 8 + z * 2 + yh
    own = tokens[0]

    p0, p1 = first_pieces(w_qkv, w_out)
    lent = lax.ppermute(own, TOKEN_AXES, [(i, i + 8) for i in WRAPS])
    r0 = moved(p0, Y_UP)
    r1 = moved(p1, Y_DOWN)
    prev = lax.ppermute(own, TOKEN_AXES, [(i, i + 1) for i in range(63) if i not in WRAPS])
    u0 = moved(r0, X_UP)
    d1 = moved(r1, X_DOWN)
    late = lax.ppermute(lent, TOKEN_AXES, [(i + 8, i + 1) for i in WRAPS])
    u1 = moved(r1, X_UP)
    d0 = moved(r0, X_DOWN)
    f0 = moved(u0, X_UP)
    f1 = moved(d1, X_DOWN)
    near = [moved(a, CORE) for a in (r0, r1)]
    ring = [moved(a, CORE) for a in (u0, u1, d0, d1)]
    last = [moved(a, CORE) for a in (f0, f1)]
    mine = [r0, r1, u0, u1, d0, d1, f0, f1]
    other = near + ring + last

    lens = lengths[0]
    ends = jnp.cumsum(lens)
    offsets = ends - lens
    first = (shard - 1) * LOCAL
    at = first + jnp.arange(WIN + 256, dtype=jnp.int32)
    begun = offsets[:, None] <= at[None, :]
    image = jnp.sum(begun.astype(jnp.int32), axis=0) - 1
    start = jnp.max(jnp.where(begun, offsets[:, None], -WIN), axis=0) - first
    end = jnp.min(jnp.where(ends[:, None] > at[None, :], ends[:, None], 1 << 20), axis=0) - first
    spans = jnp.stack([start, end]).astype(jnp.int32)
    low = start[LOCAL]
    cut = jnp.where(low < LOCAL, end[LOCAL], LOCAL)
    limit = jnp.where(end[WIN - 1] == WIN, WIN, start[WIN - 1])
    wrap = (co + z + yh == 0) & (x > 0)
    places = [
        jnp.stack([x, co, dp, lo, hi, wrap, image[LOCAL]]).astype(jnp.int32)
        for lo, hi in ((low, cut), (cut - LOCAL, limit - LOCAL))
    ]
    owner = (ends - 1) // LOCAL
    leader = jnp.sum((offsets[None, :] <= owner[:, None] * LOCAL).astype(jnp.int32), axis=1) - 1
    rank = jnp.arange(IMAGES, dtype=jnp.int32) - leader
    group = owner // 16 * 8 + owner % 8
    slot = jnp.where(owner // 8 % 2 == co, 0, 32 * SLOTS) + group * SLOTS + rank
    slot = slot[None]
    crowded = jnp.full((8, 128), jnp.max(rank) >= SLOTS).astype(jnp.float32)
    elsewhere = lax.ppermute(crowded, "dp", SWAP)
    fits = crowded[0, 0] + elsewhere[0, 0] == 0.0

    gain = ln_gain[None]
    weights = [w_qkv, w_out, *mine, *other]

    hprev, hedge, total = attention(True, places[0], spans, [prev, late, own], gain, weights, [])
    back = lax.ppermute(hprev, TOKEN_AXES, [(i + 1, i) for i in range(63)])
    hown, part, few = attention(
        False, places[1], spans[:, LOCAL:] - LOCAL, [own], gain, weights,
        [image[None, LOCAL:WIN], lens.astype(jnp.float32)[:, None], hedge, total],
    )

    def pooled_directly(few, part):
        near = lax.all_to_all(
            jnp.broadcast_to(few[None], (32, SLOTS, D)), GROUP, 0, 0, tiled=True
        ).reshape(32 * SLOTS, D)
        far = lax.ppermute(near, "co", SWAP)
        return unpack(near, far, slot)

    def pooled_by_sums(few, part):
        part = part.reshape(2, IMAGES // 2, D)
        kept = lax.dynamic_index_in_dim(part, co, 0, keepdims=False)
        given = lax.dynamic_index_in_dim(part, 1 - co, 0, keepdims=False)
        given = lax.ppermute(given, "co", SWAP)
        kept = kept.astype(jnp.float32) + given.astype(jnp.float32)
        kept = kept.astype(jnp.bfloat16).reshape(32, 4, D)
        rows = lax.all_to_all(kept, GROUP, 0, 0, tiled=True).astype(jnp.float32)
        rows = jnp.sum(rows, axis=0).astype(jnp.bfloat16)
        half = lax.all_to_all(jnp.broadcast_to(rows[None], (32, 4, D)), GROUP, 0, 0, tiled=True)
        half = half.reshape(IMAGES // 2, D)
        rest = lax.ppermute(half, "co", SWAP)
        pooled = jnp.where(co == 0, jnp.stack([half, rest]), jnp.stack([rest, half]))
        return pooled.reshape(IMAGES, D).astype(jnp.float32)

    pooled = lax.cond(fits, pooled_directly, pooled_by_sums, few, part)[None]

    here = jnp.arange(LOCAL, dtype=jnp.int32)[:, None] < limit - LOCAL
    hidden = jnp.where(here, hown, back)[None]
    return hidden, pooled


def solution(mesh):
    fine = Mesh(mesh.devices.reshape(4, 2, 4, 2, 2), ALL_AXES)
    in_specs = (P("dp", TOKEN_AXES, None), P("dp", None), P(), P("dp", None), P("dp", None))
    out_specs = (P("dp", TOKEN_AXES, None), P("dp", None, None))
    return jax.shard_map(layer, mesh=fine, in_specs=in_specs, out_specs=out_specs, check_vma=False)
```
